128 devices in a mesh: px: 16 (over z, y), py: 8 (over x, core).
Axes of the slice: x: 4, y: 4, z: 4, core: 2. Of those that a mesh axis runs over, the one named last changes fastest.
Arguments:
- point_channel_values: bfloat16 [16384, 64, 128], P(('px', 'py')), may hold values from -6 to 6
- point_offsets: bfloat16 [16384, 3, 128], P(('px', 'py')), may hold values from -1 to 17
- point_counts: int32 [16384], P(('px', 'py')), may hold values from 1 to 128
- block_bricks: int32 [16384, 4], P(('px', 'py')), may hold values from 0 to 16383, as said below
- spectral_weights: bfloat16 [2, 32, 32, 32, 64, 128], P(None, None, 'px', 'py'), may hold values from -0.5 to 0.5
- skip_weights: bfloat16 [2, 64, 64], replicated, may hold values from -0.75 to 0.75
- skip_bias: float32 [2, 64], replicated, may hold values from -3 to 3
Outputs:
- decoded: bfloat16 [16384, 64, 128], P(('px', 'py'))
The draws below stay inside these ranges and needn't reach their ends.
Inputs may be any that keep to these rules, and one draw needn't show every extreme that they name: `block_bricks`: the 4 bricks of a block are distinct and lie on one device. Among the 128 blocks of one device at most 2 have their bricks on any one device, and in every draw some device receives exactly 2 blocks from every device.
All inputs are finite; a program needn't handle non-finite values.
Results may differ from the reference program's by a relative error of at most 0.0075.
Values may be sent and summed in bfloat16 or wider, within the bound.
No kernel may reach another device: no remote copies, remote signals or barrier semaphores. Data moves between devices by JAX's collectives and lax.ppermute only.
A program may use at most 256 MiB of HBM per device.

```python
import math
import jax
import jax.numpy as jnp
from jax import lax

CH = 64
MODES = 32
NX = 128
NY = 128
NZ = 128
LAYERS = 2
BLOCK = 128
HALO = 4
BLK_DEV = 128
CAPB = 2
NBLK = 16384
BY = 4
BZ = 8
BRK_DEV = 128
N_PX = 16
N_PY = 8
DEVICES = 128


def draw_block_bricks(key, part):
    hot_key, device_key = jax.random.split(key)
    hottest = jax.random.randint(hot_key, (), 0, DEVICES)

    def per_source(source_point):
        source_key = jax.random.fold_in(device_key, source_point)
        pick_key, shuffle_key, brick_key = jax.random.split(source_key, 3)
        chosen = jax.random.permutation(pick_key, (DEVICES - 1) * CAPB)[:BLK_DEV - CAPB]
        others = chosen // CAPB
        others = others + (others >= hottest).astype(others.dtype)
        owners = jnp.concatenate([jnp.full((CAPB,), hottest, jnp.int32), others.astype(jnp.int32)])
        owners = jax.random.permutation(shuffle_key, owners)
        home_bricks = jax.random.randint(brick_key, (BLK_DEV,), 0, BRK_DEV)
        return (owners, home_bricks)
    owners, home_bricks = jax.vmap(per_source)(jnp.arange(DEVICES, dtype=jnp.int32))
    first_coord = home_bricks // (BY * BZ)
    second_coord = home_bricks // BZ % BY
    third_coord = home_bricks % BZ
    flip_first = (jnp.bitwise_xor(first_coord, 1) * BY + second_coord) * BZ + third_coord
    flip_second = (first_coord * BY + jnp.bitwise_xor(second_coord, 1)) * BZ + third_coord
    flip_third = (first_coord * BY + second_coord) * BZ + jnp.bitwise_xor(third_coord, 1)
    listed = jnp.stack([home_bricks, flip_first, flip_second, flip_third], axis=-1)
    return (owners[..., None] * BRK_DEV + listed).reshape(NBLK, HALO).astype(jnp.int32)


def draw_point_offsets(key, part):
    uniform_draw = jax.random.uniform(key, (NBLK, 3, BLOCK), jnp.float32)
    extent = jnp.array([2.0, 4.0, 16.0], jnp.float32)[None, :, None]
    return (-1.0 + uniform_draw * (extent + 2.0)).astype(jnp.bfloat16)


def touch_ends(result, stream_key, smallest, largest):
    longest = result.shape.index(max(result.shape))
    spots = []
    for shift in (0, 1):
        where = [jax.random.randint(jax.random.fold_in(stream_key, axis), (), 0, length) for axis, length in enumerate(result.shape)]
        where[longest] = (where[longest] + shift) % result.shape[longest]
        spots.append(tuple(where))
    return result.at[spots[0]].set(smallest).at[spots[1]].set(largest)


def levels(stream_key, dims, cuts, smallest, top_value):
    factor_of = 1.0
    for axis_at, shards_of in cuts:
        steps = jax.random.uniform(jax.random.fold_in(jax.random.fold_in(stream_key, 6), axis_at), (shards_of,), jnp.float32, smallest / len(cuts), top_value / len(cuts))
        factor_of = factor_of * jnp.repeat(jnp.exp(steps), dims[axis_at] // shards_of).reshape((-1,) + (1,) * (len(dims) - 1 - axis_at))
    return factor_of


def gaussian(rng, shape, scale, limit, pieces=(), kind=jnp.bfloat16):
    entries = jax.random.normal(rng, shape, jnp.float32) * scale
    if len(pieces) > 0:
        entries = levels(rng, shape, pieces, -0.22, 0.18) * entries
    return jnp.clip(entries, min=-limit, max=limit).astype(kind)


def setup_inputs(seed: int = 0) -> dict:
    key_of = jax.random.split(jax.random.key(seed), 8)
    return {
        "point_channel_values": gaussian(key_of[0], (NBLK, CH, BLOCK), 1.0, 6.0, ((0, 128),)),
        "point_offsets": draw_point_offsets(jax.random.fold_in(key_of[7], 71), 0),
        "point_counts": touch_ends(jax.random.randint(key_of[2], (NBLK,), 1, BLOCK + 1), jax.random.fold_in(key_of[2], 1), 1, BLOCK).astype(jnp.int32),
        "block_bricks": draw_block_bricks(jax.random.fold_in(key_of[7], 71), 0),
        "spectral_weights": gaussian(key_of[4], (LAYERS, MODES, MODES, MODES, CH, 2 * CH), (2 * CH) ** -0.5, 0.5, ((2, 16), (3, 8))),
        "skip_weights": gaussian(key_of[5], (LAYERS, CH, CH), CH ** -0.5, 0.75),
        "skip_bias": gaussian(key_of[6], (LAYERS, CH), 0.5, 3.0, (), jnp.float32),
    }


AMPLITUDE = 0.25
SPREAD = 4.5
DECODE_SCALE = 0.1


def cell_centers():
    cell_index = jnp.arange(128, dtype=jnp.int32)
    return jnp.stack([cell_index // 64, (cell_index // 16) % 4, cell_index % 16]).astype(jnp.float32) + 0.5


def brick_anchor(local_ids, bricks_y, bricks_z):
    clamped_weights = jnp.maximum(local_ids, 0)
    return jnp.stack([2 * (clamped_weights // (bricks_y * bricks_z)), 4 * ((clamped_weights // bricks_z) % bricks_y), 16 * (clamped_weights % bricks_z)], axis=-1).astype(jnp.float32)


def block_work(features, offsets, counts, local_ids, bricks_y, bricks_z):
    total_items, channels, points = features.shape
    group_size = math.gcd(total_items, 16)
    centers = cell_centers()

    def one_group(items):
        feature_share, offset_part, count_part, id_part = items
        validity = (jnp.arange(points, dtype=jnp.int32)[None, :] < count_part[:, None]).astype(jnp.float32)
        anchors = brick_anchor(id_part, bricks_y, bricks_z)
        relative_position = anchors - anchors[:, :1, :]
        placed = offset_part.astype(jnp.float32)[:, None, :, :] - relative_position[:, :, :, None]
        apart = placed[..., None] - centers[None, None, :, None, :]
        distance = jnp.sum(apart * apart, axis=2)
        kernel_weight_value = (AMPLITUDE * jnp.exp(-distance / SPREAD) * validity[:, None, :, None]).astype(jnp.bfloat16)
        brick_tile_grid = jnp.einsum('dqw,dewn->deqn', feature_share.astype(jnp.float32), kernel_weight_value.astype(jnp.float32)).astype(jnp.bfloat16)
        return kernel_weight_value, brick_tile_grid

    grouped = tuple(member.reshape((total_items // group_size, group_size) + member.shape[1:]) for member in (features, offsets, counts, local_ids))
    kernel_weight_value, brick_tile_grid = lax.map(one_group, grouped)
    return kernel_weight_value.reshape((total_items,) + kernel_weight_value.shape[2:]), brick_tile_grid.reshape((total_items,) + brick_tile_grid.shape[2:])


def decode_points(brick_values, kernel_weight_value):
    summed = jnp.einsum('nhcx,nhpx->ncp', brick_values.astype(jnp.float32), kernel_weight_value.astype(jnp.float32))
    return (DECODE_SCALE * summed).astype(jnp.bfloat16)


def round_half(values):
    lowered = values.astype(jnp.bfloat16)
    lowered = lax.optimization_barrier(lowered)
    return lowered.astype(values.dtype)


def round_complex(values):
    return lax.complex(round_half(jnp.real(values)), round_half(jnp.imag(values)))


def keep_index(length, kept_modes):
    half_modes = kept_modes // 2
    return jnp.concatenate([jnp.arange(half_modes, dtype=jnp.int32), jnp.arange(length - half_modes, length, dtype=jnp.int32)]).astype(jnp.int32)


def spectral_reference(grid, weights):
    third_modes = round_complex(jnp.fft.rfft(grid, axis=3, norm="ortho")[..., :MODES])
    second_modes = round_complex(jnp.take(jnp.fft.fft(third_modes, axis=2, norm="ortho"), keep_index(NY, MODES), axis=2))
    first_modes = round_complex(jnp.take(jnp.fft.fft(second_modes, axis=1, norm="ortho"), keep_index(NX, MODES), axis=1))
    real_part = jnp.real(first_modes).transpose(1, 2, 3, 0)
    imag_part = jnp.imag(first_modes).transpose(1, 2, 3, 0)

    def mix_slice(items):
        left_real, left_imag, weight_slice = items
        weight_full = weight_slice.astype(real_part.dtype)
        from_real = jnp.einsum('kzc,kzcr->kzr', left_real, weight_full, precision=lax.Precision.HIGHEST)
        from_imag = jnp.einsum('kzc,kzcr->kzr', left_imag, weight_full, precision=lax.Precision.HIGHEST)
        return from_real[..., :CH] - from_imag[..., CH:], from_real[..., CH:] + from_imag[..., :CH]

    mixed_real, mixed_imag = lax.map(mix_slice, (real_part, imag_part, weights))
    mixed = lax.complex(mixed_real, mixed_imag).transpose(3, 0, 1, 2)
    widened = jnp.zeros((CH, NX, MODES, MODES), mixed.dtype).at[:, keep_index(NX, MODES)].set(mixed)
    first_back = round_complex(jnp.fft.ifft(widened, axis=1, norm="ortho"))
    widened = jnp.zeros((CH, NX, NY, MODES), first_back.dtype).at[:, :, keep_index(NY, MODES)].set(first_back)
    second_back = round_complex(jnp.fft.ifft(widened, axis=2, norm="ortho"))
    return jnp.fft.irfft(second_back, n=NZ, axis=3, norm="ortho")


def global_grid(bricks, bricks_along_first, bricks_y, bricks_z):
    shaped = bricks.reshape(N_PX, N_PY, bricks_along_first, bricks_y, bricks_z, CH, 2, 4, 16)
    return shaped.transpose(5, 0, 2, 6, 1, 3, 7, 4, 8).reshape(CH, NX, NY, NZ)


def global_bricks(grid, bricks_along_first, bricks_y, bricks_z):
    shaped = grid.reshape(CH, N_PX, bricks_along_first, 2, N_PY, bricks_y, 4, bricks_z, 16)
    return shaped.transpose(1, 4, 2, 5, 7, 0, 3, 6, 8).reshape(N_PX * N_PY * bricks_along_first * bricks_y * bricks_z, CH, 128)


def reference(point_channel_values, point_offsets, point_counts, block_bricks, spectral_weights, skip_weights, skip_bias):
    bricks_along_first = NX // N_PX // 2
    bricks_y = NY // N_PY // 4
    bricks_z = NZ // 16
    bricks_device = bricks_along_first * bricks_y * bricks_z
    total_bricks = bricks_device * N_PX * N_PY
    block_total = point_channel_values.shape[0]
    group_size = math.gcd(block_total, 256)
    local_ids = block_bricks % bricks_device
    stacked = tuple(member.reshape((block_total // group_size, group_size) + member.shape[1:]) for member in (point_channel_values, point_offsets, point_counts, local_ids, block_bricks))

    def add_group(brick_sums, items):
        features, offsets, counts, local_part, global_part = items
        unused, brick_tile_grid = block_work(features, offsets, counts, local_part, bricks_y, bricks_z)
        flat_tiles = brick_tile_grid.reshape((-1,) + brick_tile_grid.shape[2:]).astype(jnp.float32)
        return brick_sums.at[global_part.reshape(-1)].add(flat_tiles), None

    brick_sums, unused = lax.scan(add_group, jnp.zeros((total_bricks, CH, 128), jnp.float32), stacked)
    grid = global_grid(brick_sums.astype(jnp.bfloat16), bricks_along_first, bricks_y, bricks_z)
    for depth_index in range(LAYERS):
        spectral = spectral_reference(grid.astype(jnp.float32), spectral_weights[depth_index])
        skipped = jnp.einsum('io,ixyz->oxyz', skip_weights[depth_index].astype(jnp.float32), grid.astype(jnp.float32), precision=lax.Precision.HIGHEST)
        grid = jax.nn.gelu(spectral + skipped + skip_bias[depth_index][:, None, None, None], approximate=False).astype(jnp.bfloat16)
    final_bricks = global_bricks(grid, bricks_along_first, bricks_y, bricks_z)

    def decode_group(items):
        features, offsets, counts, local_part, global_part = items
        kernel_weight_value, unused_tiles = block_work(features, offsets, counts, local_part, bricks_y, bricks_z)
        return decode_points(jnp.take(final_bricks, global_part, axis=0), kernel_weight_value)

    decoded = lax.map(decode_group, stacked)
    return decoded.reshape((block_total,) + decoded.shape[2:])
```

```python
import functools
import math

import jax
import jax.numpy as jnp
import numpy as np
from jax import lax
from jax.experimental import pallas as pl
from jax.experimental.pallas import tpu as pltpu
from jax.sharding import PartitionSpec as P

CH = 64
MODES = 32
LAYERS = 2
DEV = 128
AMPLITUDE = 0.25
SPREAD = 4.5
DECODE_SCALE = 0.1
BF = jnp.bfloat16
F32 = jnp.float32
MIB = 1024 * 1024
NT = (((1,), (1,)), ((), ()))


def halves(table):
    high = np.asarray(table, np.float32).astype(BF)
    low = (np.asarray(table, np.float64) - high.astype(np.float64)).astype(np.float32).astype(BF)
    return high, low


def waves():
    j = np.arange(MODES)
    return np.where(j < MODES // 2, j, j - MODES)


def turn(frequency, place):
    return 2.0 * math.pi / 128 * ((frequency * place) % 128)


def forward_pair(angle):
    c, s = np.cos(angle) / math.sqrt(128), np.sin(angle) / math.sqrt(128)
    return np.array([[c, s], [-s, c]])


def backward_pair(angle):
    c, s = np.cos(angle) / math.sqrt(128), np.sin(angle) / math.sqrt(128)
    return np.array([[c, -s], [s, c]])


@functools.lru_cache(None)
def tables():
    k = np.arange(MODES)
    z = np.arange(128)
    angle = turn(k[:, None], z[None, :])
    mz = np.stack([np.cos(angle), -np.sin(angle)], 1).reshape(64, 128) / math.sqrt(128)
    mz_high, mz_low = halves(mz)
    z_forward = np.concatenate([mz_high, mz_low], 0)
    weight = np.where(k == 0, 1.0, 2.0)[:, None, None]
    inv = np.stack([np.cos(angle), -np.sin(angle)], 1) / math.sqrt(128) * weight
    inv = inv.reshape(8, 8, 128)
    zi = np.zeros((2, 128, 8, 2, 8))
    for y2 in range(2):
        zi[y2, :, :, y2, :] = inv.transpose(2, 0, 1)
    z_back = np.concatenate(halves(zi.reshape(256, 128)), 1)
    f = waves()
    y = np.arange(128)
    pair = forward_pair(turn(f[:, None], y[None, :])).reshape(2, 2, 16, 2, 32, 4)
    ty = np.zeros((4, 16, 2, 2, 32, 4, 4, 2))
    for k4 in range(4):
        ty[k4, :, :, :, :, :, k4, :] = pair.transpose(2, 3, 0, 4, 5, 1)
    y_forward = np.concatenate(halves(ty.reshape(256, 1024)), 0)
    pair = backward_pair(turn(f[:, None], y[None, :])).reshape(2, 2, 16, 2, 32, 4)
    ti = np.zeros((32, 4, 4, 2, 4, 16, 2, 2))
    for k4 in range(4):
        ti[:, :, k4, :, k4, :, :, :] = pair.transpose(4, 5, 0, 2, 3, 1)
    y_back = np.concatenate(halves(ti.reshape(1024, 256)), 1)
    x = np.arange(128)
    pair = forward_pair(turn(f[:, None], x[None, :])).reshape(2, 2, 32, 16, 4, 2)
    tx = np.zeros((32, 2, 2, 16, 2, 4, 2, 2))
    for ky in range(2):
        tx[:, ky, :, :, :, :, ky, :] = pair.transpose(2, 0, 3, 5, 4, 1)
    x_forward = np.concatenate(halves(tx.reshape(128, 512)), 0)
    pair = backward_pair(turn(f[:, None], x[None, :])).reshape(2, 2, 32, 16, 4, 2)
    txi = np.zeros((16, 2, 4, 2, 2, 2, 32, 2))
    for ky in range(2):
        txi[:, :, :, ky, :, :, :, ky] = pair.transpose(3, 5, 4, 0, 1, 2)
    high, low = halves(txi.reshape(512, 128))
    x_back = np.concatenate([high, low, high], 1)
    order = np.arange(512).reshape(8, 16, 4).transpose(1, 0, 2).reshape(-1)
    to_send = np.eye(512)[order].astype(BF)
    from_send = np.ascontiguousarray(np.eye(512)[order].T).astype(BF)
    row = np.arange(512)
    repeat = np.eye(128)[(row // 8) * 2 + row % 2].astype(BF)
    return dict(
        z_forward=z_forward, z_back=z_back, y_forward=y_forward, y_back=y_back,
        x_forward=x_forward, x_back=x_back, to_send=to_send, from_send=from_send,
        repeat=repeat, eye=np.eye(256).astype(BF),
    )


def dot(a, b):
    return jnp.dot(a, b, preferred_element_type=F32)


def dot_nt(a, b):
    return lax.dot_general(a, b, NT, preferred_element_type=F32)


def call(body, out_shape, *args, scratch=(), specs=None, out_specs=None, limit=40):
    vm = pl.BlockSpec(memory_space=pltpu.VMEM)
    single = not isinstance(out_shape, (tuple, list))
    if specs is None:
        specs = [vm] * len(args)
    if out_specs is None:
        out_specs = vm if single else [vm] * len(out_shape)
    return pl.pallas_call(
        body,
        out_shape=out_shape,
        in_specs=specs,
        out_specs=out_specs,
        scratch_shapes=list(scratch),
        compiler_params=pltpu.CompilerParams(vmem_limit_bytes=limit * MIB),
    )(*args)


VM = pl.BlockSpec(memory_space=pltpu.VMEM)
SM = pl.BlockSpec(memory_space=pltpu.SMEM)


def shaped(shape, dtype=BF):
    return jax.ShapeDtypeStruct(shape, dtype)


def pack_body(bricks, counts, values, offsets, send, slots, seen, aux):
    def clear(d, _):
        send[d] = jnp.zeros((136, 128), BF)
        aux[d] = jnp.zeros((8, 128), F32)
        seen[d] = 0
        return 0

    lax.fori_loop(0, DEV, clear, 0, unroll=4)
    lane = lax.broadcasted_iota(jnp.int32, (1, 128), 1)
    half = lax.broadcasted_iota(jnp.int32, (8, 128), 0) // 4

    def one(b, _):
        first = bricks[4 * b]
        owner = first // 128
        rank = seen[owner]
        seen[owner] = rank + 1
        slots[b] = owner * 2 + rank
        base = owner * 128
        send[owner, pl.ds(pl.multiple_of(rank * 64, 64), 64), :] = values[b]
        meta = jnp.where(lane == 0, counts[b], 0)
        for h in range(4):
            meta = jnp.where(lane == 1 + h, bricks[4 * b + h] - base, meta)
        rows = jnp.concatenate([offsets[b].astype(F32), meta.astype(F32)], 0)
        both = jnp.concatenate([rows, rows], 0)
        aux[owner] = aux[owner] + jnp.where(half == rank, both, 0.0)
        return 0

    lax.fori_loop(0, DEV, one, 0, unroll=2)

    def finish(d, _):
        send[d, 128:136, :] = aux[d].astype(BF)
        return 0

    lax.fori_loop(0, DEV, finish, 0, unroll=4)


def pack(values, offsets, counts, bricks):
    return call(
        pack_body,
        (shaped((DEV, 136, 128)), shaped((DEV,), jnp.int32)),
        bricks.reshape(-1), counts, values, offsets,
        scratch=(pltpu.SMEM((DEV,), jnp.int32), pltpu.VMEM((DEV, 8, 128), F32)),
        specs=[SM, SM, VM, VM],
        out_specs=[VM, SM],
        limit=32,
    )


def anchor(local):
    return (
        (2 * (local // 32)).astype(F32),
        (4 * ((local // 8) % 4)).astype(F32),
        (16 * (local % 8)).astype(F32),
    )


def spread_weights(place, count, ids):
    lane = lax.broadcasted_iota(jnp.int32, (1, 128), 1)
    sub = lax.broadcasted_iota(jnp.int32, (8, 128), 0)
    xs = (sub // 4).astype(F32) + 0.5
    ys = (sub % 4).astype(F32) + 0.5
    zs = lax.broadcasted_iota(jnp.int32, (16, 128), 0).astype(F32) + 0.5
    qx = jnp.where(lane < count, place[0:1], 1.0e4)
    qy = place[1:2]
    qz = place[2:3]
    x0, y0, z0 = anchor(ids[0])
    parts = []
    for h in range(4):
        xh, yh, zh = anchor(ids[h])
        dx = (qx - (xh - x0)) - xs
        dy = (qy - (yh - y0)) - ys
        dz = (qz - (zh - z0)) - zs
        xy = AMPLITUDE * jnp.exp(-(dx * dx + dy * dy) / SPREAD)
        zz = jnp.exp(-(dz * dz) / SPREAD)
        for i in range(8):
            parts.append((xy[i : i + 1] * zz).astype(BF))
    return jnp.concatenate(parts, 0)


def third_forward(grid_at, table, out):
    for by in range(4):
        for j in range(4):
            modes = []
            for half in range(2):
                both = dot(table, grid_at(by, 2 * j + half))
                modes.append(both[:64] + both[64:])
            for kg in range(8):
                piece = jnp.concatenate([m[8 * kg : 8 * kg + 8] for m in modes], 0)
                at = by * 64 + j * 16
                out[kg, at : at + 16, :] = piece.astype(BF)


def encode_body(meta, got, eye, z_table, grid, modes, acc):
    def clear(b, _):
        acc[b] = jnp.zeros((64, 128), F32)
        return 0

    lax.fori_loop(0, 128, clear, 0, unroll=4)

    def one(d, _):
        rows = got[d, 128:136, :].astype(F32)
        for r in range(2):
            at = d * 10 + r * 5
            ids = [meta[at + 1 + h] for h in range(4)]
            weights = spread_weights(rows[4 * r : 4 * r + 3], meta[at], ids)
            tile = dot_nt(got[d, 64 * r : 64 * r + 64, :], weights)
            for h in range(4):
                acc[ids[h]] = acc[ids[h]] + tile[:, 128 * h : 128 * h + 128]
        return 0

    lax.fori_loop(0, DEV, one, 0, unroll=2)
    eye128 = eye[0:128, 0:128]
    for by in range(4):
        for bz in range(8):
            bricks = jnp.concatenate([acc[(bx * 4 + by) * 8 + bz] for bx in range(4)], 0)
            cells = dot_nt(eye128, bricks.astype(BF)).astype(BF)
            for xy in range(8):
                grid[by, xy, 16 * bz : 16 * bz + 16, :] = cells[16 * xy : 16 * xy + 16]
    third_forward(lambda by, xy: grid[by, xy], z_table[...], modes)


def encode(meta, got, t):
    return call(
        encode_body,
        (shaped((4, 8, 128, 256)), shaped((8, 256, 256))),
        meta, got, t["eye"], t["z_forward"],
        scratch=(pltpu.VMEM((128, 64, 128), F32),),
        specs=[SM, VM, VM, VM],
        limit=40,
    )


def second_body(got, table, order, send):
    rows = []
    for x2 in range(2):
        data = jnp.concatenate(
            [
                got[py, by * 64 + x2 * 32 : by * 64 + x2 * 32 + 32, :]
                for py in range(8)
                for by in range(4)
            ],
            0,
        )
        both = dot(table[...], data)
        out = both[:256] + both[256:]
        for bx in range(4):
            rows.append(
                jnp.concatenate(
                    [out[64 * k : 64 * k + 64, 64 * bx : 64 * bx + 64] for k in range(4)], 1
                ).astype(BF)
            )
    send[...] = dot(order[...], jnp.concatenate(rows, 0)).astype(BF)


def mix_body(got, weights, forward, back, repeat, send, product):
    both = dot(forward[...], got[...])
    modes = (both[:128] + both[128:]).astype(BF)
    spread = dot(repeat[...], modes)
    row = lax.broadcasted_iota(jnp.int32, (512, 256), 0)
    col = lax.broadcasted_iota(jnp.int32, (512, 256), 1)
    spread = jnp.where(col // 64 == (row % 8) // 2, spread, 0.0)
    for m in range(64):
        product[8 * m : 8 * m + 8, :] = dot(spread[8 * m : 8 * m + 8].astype(BF), weights[m])
    real, imag = [], []
    for kz in range(4):
        from_real = product[pl.ds(2 * kz, 64, stride=8), :]
        from_imag = product[pl.ds(2 * kz + 1, 64, stride=8), :]
        real.append(from_real[:, :64] - from_imag[:, 64:])
        imag.append(from_real[:, 64:] + from_imag[:, :64])
    mixed = jnp.concatenate([jnp.concatenate(real, 1), jnp.concatenate(imag, 1)], 0)
    high = mixed.astype(BF)
    low = (mixed - high.astype(F32)).astype(BF)
    send[...] = dot(back[...], jnp.concatenate([high, high, low], 0)).astype(BF)


def second_back_body(got, table, order, send):
    ordered = dot(order[...], got[...])
    for x2 in range(2):
        parts = []
        for k in range(4):
            parts.append(
                jnp.concatenate(
                    [
                        ordered[
                            (x2 * 4 + bx) * 64 : (x2 * 4 + bx) * 64 + 64, 64 * k : 64 * k + 64
                        ]
                        for bx in range(4)
                    ],
                    1,
                ).astype(BF)
            )
        data = jnp.concatenate(parts, 0)
        out = dot(table[...], jnp.concatenate([data, data], 0)).astype(BF)
        for py in range(8):
            for by in range(4):
                at = py * 128 + by * 32
                send[py, by * 64 + x2 * 32 : by * 64 + x2 * 32 + 32, :] = out[at : at + 32]


def layer_values(by, j, got, grid, z_back, skip, bias):
    at = by * 64 + j * 16
    data = jnp.concatenate([got[kg, at : at + 16, :] for kg in range(8)], 0)
    total = dot(z_back, jnp.concatenate([data, data], 0))
    total = total + dot(grid[by, 2 * j : 2 * j + 2].reshape(256, 256), skip)
    total = total + bias
    result = 0.5 * total * (1.0 + lax.erf(total * math.sqrt(0.5)))
    return result.astype(BF)


def inner_layer_body(got, grid, z_back, skip, bias, z_table, new_grid, modes):
    for by in range(4):
        for j in range(4):
            values = layer_values(by, j, got, grid, z_back[...], skip[...], bias[...])
            new_grid[by, 2 * j] = values[:128]
            new_grid[by, 2 * j + 1] = values[128:]
    third_forward(lambda by, xy: new_grid[by, xy], z_table[...], modes)


def last_layer_body(got, grid, z_back, skip, bias, eye, bricks):
    for by in range(4):
        values = [
            layer_values(by, j, got, grid, z_back[...], skip[...], bias[...]) for j in range(4)
        ]
        for bz in range(8):
            cells = jnp.concatenate(
                [
                    values[xy // 2][(xy % 2) * 128 + 16 * bz : (xy % 2) * 128 + 16 * bz + 16]
                    for xy in range(8)
                ],
                0,
            )
            turned = dot_nt(eye[...], cells).astype(BF)
            for bx in range(4):
                bricks[(bx * 4 + by) * 8 + bz] = turned[64 * bx : 64 * bx + 64]


def decode_body(meta, got, bricks, reply):
    def one(d, _):
        rows = got[d, 128:136, :].astype(F32)
        for r in range(2):
            at = d * 10 + r * 5
            ids = [meta[at + 1 + h] for h in range(4)]
            weights = spread_weights(rows[4 * r : 4 * r + 3], meta[at], ids)
            near = jnp.concatenate([bricks[ids[h]] for h in range(4)], 1)
            reply[d, 64 * r : 64 * r + 64, :] = (DECODE_SCALE * dot(near, weights)).astype(BF)
        return 0

    lax.fori_loop(0, DEV, one, 0, unroll=2)


def pick_body(slots, got, out):
    def one(b, _):
        out[b] = got[slots[b]]
        return 0

    lax.fori_loop(0, DEV, one, 0, unroll=4)


def exchange(x, axis):
    return lax.all_to_all(x, axis, split_axis=0, concat_axis=0, tiled=True)


def per_device(values, offsets, counts, bricks, spectral_weights, skip_weights, skip_bias):
    t = tables()
    t = {name: jnp.asarray(table) for name, table in t.items()}
    send, slots = pack(values, offsets, counts, bricks)
    got = exchange(send, ("px", "py"))
    meta = got[:, 128:, :5].reshape(DEV, 2, 4, 5)[:, :, 3].astype(jnp.int32).reshape(-1)
    grid, modes = encode(meta, got, t)
    for layer in range(LAYERS):
        columns = exchange(modes, "py")
        second = call(
            second_body, shaped((512, 256)), columns, t["y_forward"], t["to_send"], limit=24
        )
        lines = exchange(second.reshape(16, 32, 256), "px").reshape(512, 256)
        back = call(
            mix_body,
            shaped((512, 256)),
            lines,
            spectral_weights[layer].reshape(64, 256, 128),
            t["x_forward"],
            t["x_back"],
            t["repeat"],
            scratch=(pltpu.VMEM((512, 128), F32),),
            limit=24,
        )
        lines = exchange(back.reshape(16, 32, 256), "px").reshape(512, 256)
        columns = call(
            second_back_body,
            shaped((8, 256, 256)),
            lines,
            t["y_back"],
            t["from_send"],
            limit=24,
        )
        columns = exchange(columns, "py")
        skip = jnp.kron(jnp.eye(4, dtype=BF), skip_weights[layer])
        bias = jnp.tile(skip_bias[layer], 4)[None, :]
        if layer + 1 < LAYERS:
            grid, modes = call(
                inner_layer_body,
                (shaped((4, 8, 128, 256)), shaped((8, 256, 256))),
                columns, grid, t["z_back"], skip, bias, t["z_forward"],
                limit=32,
            )
        else:
            final = call(
                last_layer_body,
                shaped((128, 64, 128)),
                columns, grid, t["z_back"], skip, bias, t["eye"],
                limit=32,
            )
    reply = call(
        decode_body, shaped((DEV, 128, 128)), meta, got, final, specs=[SM, VM, VM], limit=32
    )
    returned = exchange(reply, ("px", "py"))
    return call(
        pick_body,
        shaped((DEV, 64, 128)),
        slots, returned.reshape(2 * DEV, 64, 128),
        specs=[SM, VM],
        limit=32,
    )


def solution(mesh):
    return jax.shard_map(
        per_device,
        mesh=mesh,
        in_specs=(
            P(("px", "py"), None, None),
            P(("px", "py"), None, None),
            P(("px", "py")),
            P(("px", "py"), None),
            P(None, None, "px", "py", None, None),
            P(),
            P(),
        ),
        out_specs=P(("px", "py"), None, None),
        check_vma=False,
    )
```

```python
import functools
import math

import jax
import jax.numpy as jnp
import numpy as np
from jax import lax
from jax.experimental import pallas as pl
from jax.experimental.pallas import tpu as pltpu
from jax.sharding import PartitionSpec as P

CH = 64
MODES = 32
LAYERS = 2
DEV = 128
AMPLITUDE = 0.25
SPREAD = 4.5
DECODE_SCALE = 0.1
BF = jnp.bfloat16
F32 = jnp.float32
MIB = 1024 * 1024
NT = (((1,), (1,)), ((), ()))
UNIT = math.sqrt(math.log2(math.e) / SPREAD)


def halves(table):
    high = np.asarray(table, np.float32).astype(BF)
    low = (np.asarray(table, np.float64) - high.astype(np.float64)).astype(np.float32).astype(BF)
    return high, low


def waves():
    j = np.arange(MODES)
    return np.where(j < MODES // 2, j, j - MODES)


def turn(frequency, place):
    return 2.0 * math.pi / 128 * ((frequency * place) % 128)


def forward_pair(angle):
    c, s = np.cos(angle) / math.sqrt(128), np.sin(angle) / math.sqrt(128)
    return np.array([[c, s], [-s, c]])


def backward_pair(angle):
    c, s = np.cos(angle) / math.sqrt(128), np.sin(angle) / math.sqrt(128)
    return np.array([[c, -s], [s, c]])


@functools.lru_cache(None)
def tables():
    k = np.arange(MODES)
    z = np.arange(128)
    angle = turn(k[:, None], z[None, :])
    mz = np.stack([np.cos(angle), -np.sin(angle)], 1).reshape(64, 128) / math.sqrt(128)
    mz_high, mz_low = halves(mz)
    z_forward = np.concatenate([mz_high, mz_low], 0)
    weight = np.where(k == 0, 1.0, 2.0)[:, None, None]
    inv = np.stack([np.cos(angle), -np.sin(angle)], 1) / math.sqrt(128) * weight
    inv = inv.reshape(8, 8, 128)
    zi = np.zeros((2, 128, 8, 2, 8))
    for y2 in range(2):
        zi[y2, :, :, y2, :] = inv.transpose(2, 0, 1)
    z_back = np.concatenate(halves(zi.reshape(256, 128)), 1)
    f = waves()
    y = np.arange(128)
    pair = forward_pair(turn(f[:, None], y[None, :])).reshape(2, 2, 16, 2, 32, 4)
    ty = np.zeros((4, 16, 2, 2, 32, 4, 4, 2))
    for k4 in range(4):
        ty[k4, :, :, :, :, :, k4, :] = pair.transpose(2, 3, 0, 4, 5, 1)
    y_forward = np.concatenate(halves(ty.reshape(256, 1024)), 0)
    pair = backward_pair(turn(f[:, None], y[None, :])).reshape(2, 2, 16, 2, 32, 4)
    ti = np.zeros((32, 4, 4, 2, 4, 16, 2, 2))
    for k4 in range(4):
        ti[:, :, k4, :, k4, :, :, :] = pair.transpose(4, 5, 0, 2, 3, 1)
    y_back = np.concatenate(halves(ti.reshape(1024, 256)), 1)
    x = np.arange(128)
    pair = forward_pair(turn(f[:, None], x[None, :])).reshape(2, 2, 32, 16, 4, 2)
    tx = np.zeros((32, 2, 2, 16, 2, 4, 2, 2))
    for ky in range(2):
        tx[:, ky, :, :, :, :, ky, :] = pair.transpose(2, 0, 3, 5, 4, 1)
    x_forward = np.concatenate(halves(tx.reshape(128, 512)), 0)
    pair = backward_pair(turn(f[:, None], x[None, :])).reshape(2, 2, 32, 16, 4, 2)
    txi = np.zeros((16, 2, 4, 2, 2, 2, 32, 2))
    for ky in range(2):
        txi[:, :, :, ky, :, :, :, ky] = pair.transpose(3, 5, 4, 0, 1, 2)
    high, low = halves(txi.reshape(512, 128))
    x_back = np.concatenate([high, low, high], 1)
    order = np.arange(512).reshape(8, 16, 4).transpose(1, 0, 2).reshape(-1)
    to_send = np.eye(512)[order].astype(BF)
    from_send = np.ascontiguousarray(np.eye(512)[order].T).astype(BF)
    row = np.arange(512)
    repeat = np.eye(128)[(row // 8) * 2 + row % 2].astype(BF)
    return dict(
        z_forward=z_forward, z_back=z_back, y_forward=y_forward, y_back=y_back,
        x_forward=x_forward, x_back=x_back, to_send=to_send, from_send=from_send,
        repeat=repeat, eye=np.eye(256).astype(BF),
    )


def dot(a, b):
    return jnp.dot(a, b, preferred_element_type=F32)


def dot_nt(a, b):
    return lax.dot_general(a, b, NT, preferred_element_type=F32)


def call(body, out_shape, *args, scratch=(), specs=None, out_specs=None, limit=40):
    vm = pl.BlockSpec(memory_space=pltpu.VMEM)
    single = not isinstance(out_shape, (tuple, list))
    if specs is None:
        specs = [vm] * len(args)
    if out_specs is None:
        out_specs = vm if single else [vm] * len(out_shape)
    return pl.pallas_call(
        body,
        out_shape=out_shape,
        in_specs=specs,
        out_specs=out_specs,
        scratch_shapes=list(scratch),
        compiler_params=pltpu.CompilerParams(vmem_limit_bytes=limit * MIB),
    )(*args)


VM = pl.BlockSpec(memory_space=pltpu.VMEM)
SM = pl.BlockSpec(memory_space=pltpu.SMEM)
HB = pl.BlockSpec(memory_space=pltpu.HBM)


def in_hbm(x):
    return pltpu.with_memory_space_constraint(x, pltpu.HBM)


def shaped(shape, dtype=BF):
    return jax.ShapeDtypeStruct(shape, dtype)


def pack_body(bricks, counts, values, offsets, send, slots, seen, aux):
    def clear(d, _):
        send[d] = jnp.zeros((136, 128), BF)
        aux[d] = jnp.zeros((8, 128), F32)
        seen[d] = 0
        return 0

    lax.fori_loop(0, DEV, clear, 0, unroll=4)
    lane = lax.broadcasted_iota(jnp.int32, (1, 128), 1)
    half = lax.broadcasted_iota(jnp.int32, (8, 128), 0) // 4

    def one(b, _):
        first = bricks[4 * b]
        owner = first // 128
        rank = seen[owner]
        seen[owner] = rank + 1
        slots[b] = owner * 2 + rank
        base = owner * 128
        send[owner, pl.ds(pl.multiple_of(rank * 64, 64), 64), :] = values[b]
        meta = jnp.where(lane == 0, counts[b], 0)
        for h in range(4):
            meta = jnp.where(lane == 1 + h, bricks[4 * b + h] - base, meta)
        rows = jnp.concatenate([offsets[b].astype(F32), meta.astype(F32)], 0)
        both = jnp.concatenate([rows, rows], 0)
        aux[owner] = aux[owner] + jnp.where(half == rank, both, 0.0)
        return 0

    lax.fori_loop(0, DEV, one, 0, unroll=2)

    def finish(d, _):
        send[d, 128:136, :] = aux[d].astype(BF)
        return 0

    lax.fori_loop(0, DEV, finish, 0, unroll=4)


def pack(values, offsets, counts, bricks):
    return call(
        pack_body,
        (shaped((DEV, 136, 128)), shaped((DEV,), jnp.int32)),
        bricks.reshape(-1), counts, values, offsets,
        scratch=(pltpu.SMEM((DEV,), jnp.int32), pltpu.VMEM((DEV, 8, 128), F32)),
        specs=[SM, SM, VM, VM],
        out_specs=[VM, SM],
        limit=32,
    )


def spread_weights(place, count, ids):
    lane = lax.broadcasted_iota(jnp.int32, (1, 128), 1)
    sub = lax.broadcasted_iota(jnp.int32, (8, 128), 0)
    xs = ((sub // 4).astype(F32) + 0.5) * UNIT
    ys = ((sub % 4).astype(F32) + 0.5) * UNIT
    zs = (lax.broadcasted_iota(jnp.int32, (16, 128), 0).astype(F32) + 0.5) * UNIT
    place = place * UNIT
    px = jnp.where(lane < count, place[0:1], 1.0e4) - xs
    py = place[1:2] - ys
    pz = place[2:3] - zs
    grid_at = [(i >> 5, (i >> 3) & 3, i & 7) for i in ids]
    parts = []
    for h in range(4):
        shift = [(a - b).astype(F32) for a, b in zip(grid_at[h], grid_at[0])]
        dx = px - shift[0] * (2 * UNIT)
        dy = py - shift[1] * (4 * UNIT)
        dz = pz - shift[2] * (16 * UNIT)
        xy = jnp.exp2(math.log2(AMPLITUDE) - dx * dx - dy * dy)
        zz = jnp.exp2(-(dz * dz))
        for i in range(8):
            parts.append((xy[i : i + 1] * zz).astype(BF))
    return jnp.concatenate(parts, 0)


def to_relative(me, chunks, sends):
    for j in range(8):
        sends[j][...] = chunks[(me[0] + j) & 7]


def from_relative(me, gots, chunks):
    for j in range(8):
        chunks[(me[0] - j) & 7] = gots[j][...]


def third_forward(grid_at, table, out):
    for by in range(4):
        for j in range(4):
            modes = []
            for half in range(2):
                both = dot(table, grid_at(by, 2 * j + half))
                modes.append(both[:64] + both[64:])
            for kg in range(8):
                piece = jnp.concatenate([m[8 * kg : 8 * kg + 8] for m in modes], 0)
                at = by * 64 + j * 16
                out[kg, at : at + 16, :] = piece.astype(BF)


def encode_body(meta, me, got, eye, z_table, grid, aux, *rest):
    *sends, modes, acc = rest
    def clear(b, _):
        acc[b] = jnp.zeros((64, 128), F32)
        return 0

    lax.fori_loop(0, 128, clear, 0, unroll=4)

    def one(d, _):
        aux[d] = got[d, 128:136, :]
        rows = got[d, 128:136, :].astype(F32)
        for r in range(2):
            at = d * 10 + r * 5
            ids = [meta[at + 1 + h] for h in range(4)]
            weights = spread_weights(rows[4 * r : 4 * r + 3], meta[at], ids)
            tile = dot_nt(got[d, 64 * r : 64 * r + 64, :], weights)
            for h in range(4):
                acc[ids[h]] = acc[ids[h]] + tile[:, 128 * h : 128 * h + 128]
        return 0

    lax.fori_loop(0, DEV, one, 0, unroll=4)
    eye128 = eye[0:128, 0:128]
    for by in range(4):
        for bz in range(8):
            bricks = jnp.concatenate([acc[(bx * 4 + by) * 8 + bz] for bx in range(4)], 0)
            cells = dot_nt(eye128, bricks.astype(BF)).astype(BF)
            for xy in range(8):
                grid[by, xy, 16 * bz : 16 * bz + 16, :] = cells[16 * xy : 16 * xy + 16]
    third_forward(lambda by, xy: grid[by, xy], z_table[...], modes)
    to_relative(me, modes, sends)


def encode(meta, me, got, t):
    out = call(
        encode_body,
        [shaped((4, 8, 128, 256)), shaped((DEV, 8, 128))] + [shaped((256, 256))] * 8,
        meta, me, got, t["eye"], t["z_forward"],
        scratch=(pltpu.VMEM((8, 256, 256), BF), pltpu.VMEM((128, 64, 128), F32)),
        specs=[SM, SM, VM, VM, VM],
        limit=40,
    )
    return out[0], out[1], out[2:]


def second_body(me, *refs):
    *gots, table, order, send, got = refs
    from_relative(me, gots, got)
    rows = []
    for x2 in range(2):
        data = jnp.concatenate(
            [
                got[py, by * 64 + x2 * 32 : by * 64 + x2 * 32 + 32, :]
                for py in range(8)
                for by in range(4)
            ],
            0,
        )
        both = dot(table[...], data)
        out = both[:256] + both[256:]
        for bx in range(4):
            rows.append(
                jnp.concatenate(
                    [out[64 * k : 64 * k + 64, 64 * bx : 64 * bx + 64] for k in range(4)], 1
                ).astype(BF)
            )
    send[...] = dot(order[...], jnp.concatenate(rows, 0)).astype(BF)


def mix_body(layer, got, weights_at, forward, back, repeat, send, product, weights, sems):
    copies = [
        pltpu.make_async_copy(
            weights_at.at[pl.ds(layer * 64 + 8 * i, 8)], weights.at[pl.ds(8 * i, 8)], sems.at[i]
        )
        for i in range(8)
    ]
    for copy in copies:
        copy.start()
    both = dot(forward[...], got[...])
    modes = (both[:128] + both[128:]).astype(BF)
    spread = dot(repeat[...], modes)
    row = lax.broadcasted_iota(jnp.int32, (512, 256), 0)
    col = lax.broadcasted_iota(jnp.int32, (512, 256), 1)
    spread = jnp.where(col // 64 == (row % 8) // 2, spread, 0.0)
    for m in range(64):
        if m % 8 == 0:
            copies[m // 8].wait()
        product[8 * m : 8 * m + 8, :] = dot(spread[8 * m : 8 * m + 8].astype(BF), weights[m])
    real, imag = [], []
    for kz in range(4):
        from_real = product[pl.ds(2 * kz, 64, stride=8), :]
        from_imag = product[pl.ds(2 * kz + 1, 64, stride=8), :]
        real.append(from_real[:, :64] - from_imag[:, 64:])
        imag.append(from_real[:, 64:] + from_imag[:, :64])
    mixed = jnp.concatenate([jnp.concatenate(real, 1), jnp.concatenate(imag, 1)], 0)
    high = mixed.astype(BF)
    low = (mixed - high.astype(F32)).astype(BF)
    send[...] = dot(back[...], jnp.concatenate([high, high, low], 0)).astype(BF)


def second_back_body(me, got, table, order, *rest):
    *sends, send = rest
    ordered = dot(order[...], got[...])
    for x2 in range(2):
        parts = []
        for k in range(4):
            parts.append(
                jnp.concatenate(
                    [
                        ordered[
                            (x2 * 4 + bx) * 64 : (x2 * 4 + bx) * 64 + 64, 64 * k : 64 * k + 64
                        ]
                        for bx in range(4)
                    ],
                    1,
                ).astype(BF)
            )
        data = jnp.concatenate(parts, 0)
        out = dot(table[...], jnp.concatenate([data, data], 0)).astype(BF)
        for py in range(8):
            for by in range(4):
                at = py * 128 + by * 32
                send[py, by * 64 + x2 * 32 : by * 64 + x2 * 32 + 32, :] = out[at : at + 32]
    to_relative(me, send, sends)


def layer_values(by, j, got, grid, z_back, skip, bias):
    at = by * 64 + j * 16
    data = jnp.concatenate([got[kg, at : at + 16, :] for kg in range(8)], 0)
    total = dot(z_back, jnp.concatenate([data, data], 0))
    total = total + dot(grid[by, 2 * j : 2 * j + 2].reshape(256, 256), skip)
    total = total + bias
    result = 0.5 * total * (1.0 + lax.erf(total * math.sqrt(0.5)))
    return result.astype(BF)


def load_grid(grid_at, grid, sems):
    copies = [
        pltpu.make_async_copy(grid_at.at[by], grid.at[by], sems.at[by]) for by in range(4)
    ]
    for copy in copies:
        copy.start()
    return copies


def inner_layer_body(me, *refs):
    *gots, grid_at, z_back, skip, bias, z_table, new_grid = refs[:14]
    *sends, got, grid, modes, sems = refs[14:]
    copies = load_grid(grid_at, grid, sems)
    from_relative(me, gots, got)
    for by in range(4):
        copies[by].wait()
        for j in range(4):
            values = layer_values(by, j, got, grid, z_back[...], skip[...], bias[...])
            new_grid[by, 2 * j] = values[:128]
            new_grid[by, 2 * j + 1] = values[128:]
    third_forward(lambda by, xy: new_grid[by, xy], z_table[...], modes)
    to_relative(me, modes, sends)


def last_layer_body(me, *refs):
    *gots, grid_at, z_back, skip, bias, eye, bricks, got, grid, sems = refs
    copies = load_grid(grid_at, grid, sems)
    from_relative(me, gots, got)
    for by in range(4):
        copies[by].wait()
        values = [
            layer_values(by, j, got, grid, z_back[...], skip[...], bias[...]) for j in range(4)
        ]
        for bz in range(8):
            cells = jnp.concatenate(
                [
                    values[xy // 2][(xy % 2) * 128 + 16 * bz : (xy % 2) * 128 + 16 * bz + 16]
                    for xy in range(8)
                ],
                0,
            )
            turned = dot_nt(eye[...], cells).astype(BF)
            for bx in range(4):
                bricks[(bx * 4 + by) * 8 + bz] = turned[64 * bx : 64 * bx + 64]


def decode_body(meta, aux, bricks, reply):
    def one(d, _):
        rows = aux[d].astype(F32)
        for r in range(2):
            at = d * 10 + r * 5
            ids = [meta[at + 1 + h] for h in range(4)]
            weights = spread_weights(rows[4 * r : 4 * r + 3], meta[at], ids)
            near = jnp.concatenate([bricks[ids[h]] for h in range(4)], 1)
            reply[d, 64 * r : 64 * r + 64, :] = (DECODE_SCALE * dot(near, weights)).astype(BF)
        return 0

    lax.fori_loop(0, DEV, one, 0, unroll=4)


def pick_body(slots, got, out):
    def one(b, _):
        out[b] = got[slots[b]]
        return 0

    lax.fori_loop(0, DEV, one, 0, unroll=4)


def exchange(x, axis):
    return lax.all_to_all(x, axis, split_axis=0, concat_axis=0, tiled=True)


def exchange_lines(chunks):
    got = [chunks[0]]
    for j in range(1, 8):
        got.append(lax.ppermute(chunks[j], "py", [(i, (i + j) % 8) for i in range(8)]))
    return got


def per_device(values, offsets, counts, bricks, spectral_weights, skip_weights, skip_bias):
    t = {name: jnp.asarray(table) for name, table in tables().items()}
    me = lax.axis_index("py").astype(jnp.int32).reshape(1)
    weights = in_hbm(spectral_weights.reshape(LAYERS * 64, 256, 128))
    send, slots = pack(values, offsets, counts, bricks)
    got = exchange(send, ("px", "py"))
    meta = got[:, 128:, :5].reshape(DEV, 2, 4, 5)[:, :, 3].astype(jnp.int32).reshape(-1)
    grid, aux, modes = encode(meta, me, got, t)
    grid = in_hbm(grid)
    chunks = pltpu.VMEM((8, 256, 256), BF)
    grid_scratch = pltpu.VMEM((4, 8, 128, 256), BF)
    four = pltpu.SemaphoreType.DMA((4,))
    piece = shaped((256, 256))
    for layer in range(LAYERS):
        columns = exchange_lines(modes)
        second = call(
            second_body,
            shaped((512, 256)),
            me, *columns, t["y_forward"], t["to_send"],
            scratch=(chunks,),
            specs=[SM] + [VM] * 10,
            limit=24,
        )
        lines = exchange(second.reshape(16, 32, 256), "px").reshape(512, 256)
        back = call(
            functools.partial(mix_body, layer),
            shaped((512, 256)),
            lines, weights, t["x_forward"], t["x_back"], t["repeat"],
            scratch=(
                pltpu.VMEM((512, 128), F32),
                pltpu.VMEM((64, 256, 128), BF),
                pltpu.SemaphoreType.DMA((8,)),
            ),
            specs=[VM, HB, VM, VM, VM],
            limit=24,
        )
        lines = exchange(back.reshape(16, 32, 256), "px").reshape(512, 256)
        columns = call(
            second_back_body,
            [piece] * 8,
            me, lines, t["y_back"], t["from_send"],
            scratch=(chunks,),
            specs=[SM, VM, VM, VM],
            limit=24,
        )
        columns = exchange_lines(columns)
        skip = jnp.kron(jnp.eye(4, dtype=BF), skip_weights[layer])
        bias = jnp.tile(skip_bias[layer], 4)[None, :]
        if layer + 1 < LAYERS:
            grid, *modes = call(
                inner_layer_body,
                [shaped((4, 8, 128, 256))] + [piece] * 8,
                me, *columns, grid, t["z_back"], skip, bias, t["z_forward"],
                scratch=(chunks, grid_scratch, chunks, four),
                specs=[SM] + [VM] * 8 + [HB] + [VM] * 4,
                limit=32,
            )
            grid = in_hbm(grid)
        else:
            final = call(
                last_layer_body,
                shaped((128, 64, 128)),
                me, *columns, grid, t["z_back"], skip, bias, t["eye"],
                scratch=(chunks, grid_scratch, four),
                specs=[SM] + [VM] * 8 + [HB] + [VM] * 4,
                limit=32,
            )
    reply = call(
        decode_body, shaped((DEV, 128, 128)), meta, aux, final, specs=[SM, VM, VM], limit=32
    )
    returned = exchange(reply, ("px", "py"))
    return call(
        pick_body,
        shaped((DEV, 64, 128)),
        slots, returned.reshape(2 * DEV, 64, 128),
        specs=[SM, VM],
        limit=32,
    )


def solution(mesh):
    return jax.shard_map(
        per_device,
        mesh=mesh,
        in_specs=(
            P(("px", "py"), None, None),
            P(("px", "py"), None, None),
            P(("px", "py")),
            P(("px", "py"), None),
            P(None, None, "px", "py", None, None),
            P(),
            P(),
        ),
        out_specs=P(("px", "py"), None, None),
        check_vma=False,
    )
```

```python
import functools
import math

import jax
import jax.numpy as jnp
import numpy as np
from jax import lax
from jax.experimental import pallas as pl
from jax.experimental.pallas import tpu as pltpu
from jax.sharding import PartitionSpec as P

CH = 64
MODES = 32
LAYERS = 2
DEV = 128
AMPLITUDE = 0.25
SPREAD = 4.5
DECODE_SCALE = 0.1
BF = jnp.bfloat16
F32 = jnp.float32
MIB = 1024 * 1024
NT = (((1,), (1,)), ((), ()))
UNIT = math.sqrt(math.log2(math.e) / SPREAD)


def halves(table):
    high = np.asarray(table, np.float32).astype(BF)
    low = (np.asarray(table, np.float64) - high.astype(np.float64)).astype(np.float32).astype(BF)
    return high, low


def waves():
    j = np.arange(MODES)
    return np.where(j < MODES // 2, j, j - MODES)


def turn(frequency, place):
    return 2.0 * math.pi / 128 * ((frequency * place) % 128)


def forward_pair(angle):
    c, s = np.cos(angle) / math.sqrt(128), np.sin(angle) / math.sqrt(128)
    return np.array([[c, s], [-s, c]])


def backward_pair(angle):
    c, s = np.cos(angle) / math.sqrt(128), np.sin(angle) / math.sqrt(128)
    return np.array([[c, -s], [s, c]])


@functools.lru_cache(None)
def tables():
    k = np.arange(MODES)
    z = np.arange(128)
    angle = turn(k[:, None], z[None, :])
    mz = np.stack([np.cos(angle), -np.sin(angle)], 1).reshape(64, 128) / math.sqrt(128)
    mz_high, mz_low = halves(mz)
    z_forward = np.concatenate([mz_high, mz_low], 0)
    weight = np.where(k == 0, 1.0, 2.0)[:, None, None]
    inv = np.stack([np.cos(angle), -np.sin(angle)], 1) / math.sqrt(128) * weight
    inv = inv.reshape(8, 8, 128)
    zi = np.zeros((2, 128, 8, 2, 8))
    for y2 in range(2):
        zi[y2, :, :, y2, :] = inv.transpose(2, 0, 1)
    z_back = np.concatenate(halves(zi.reshape(256, 128)), 1)
    f = waves()
    y = np.arange(128)
    pair = forward_pair(turn(f[:, None], y[None, :])).reshape(2, 2, 16, 2, 32, 4)
    ty = np.zeros((4, 16, 2, 2, 32, 4, 4, 2))
    for k4 in range(4):
        ty[k4, :, :, :, :, :, k4, :] = pair.transpose(2, 3, 0, 4, 5, 1)
    y_forward = np.concatenate(halves(ty.reshape(256, 1024)), 0)
    pair = backward_pair(turn(f[:, None], y[None, :])).reshape(2, 2, 16, 2, 32, 4)
    ti = np.zeros((32, 4, 4, 2, 4, 16, 2, 2))
    for k4 in range(4):
        ti[:, :, k4, :, k4, :, :, :] = pair.transpose(4, 5, 0, 2, 3, 1)
    y_back = np.concatenate(halves(ti.reshape(1024, 256)), 1)
    x = np.arange(128)
    pair = forward_pair(turn(f[:, None], x[None, :])).reshape(2, 2, 32, 16, 4, 2)
    tx = np.zeros((32, 2, 2, 16, 2, 4, 2, 2))
    for ky in range(2):
        tx[:, ky, :, :, :, :, ky, :] = pair.transpose(2, 0, 3, 5, 4, 1)
    x_forward = np.concatenate(halves(tx.reshape(128, 512)), 0)
    pair = backward_pair(turn(f[:, None], x[None, :])).reshape(2, 2, 32, 16, 4, 2)
    txi = np.zeros((16, 2, 4, 2, 2, 2, 32, 2))
    for ky in range(2):
        txi[:, :, :, ky, :, :, :, ky] = pair.transpose(3, 5, 4, 0, 1, 2)
    high, low = halves(txi.reshape(512, 128))
    x_back = np.concatenate([high, low, high], 1)
    order = np.arange(512).reshape(8, 16, 4).transpose(1, 0, 2).reshape(-1)
    to_send = np.eye(512)[order].astype(BF)
    from_send = np.ascontiguousarray(np.eye(512)[order].T).astype(BF)
    row = np.arange(512)
    repeat = np.eye(128)[(row // 8) * 2 + row % 2].astype(BF)
    return dict(
        z_forward=z_forward, z_back=z_back, y_forward=y_forward, y_back=y_back,
        x_forward=x_forward, x_back=x_back, to_send=to_send, from_send=from_send,
        repeat=repeat, eye=np.eye(256).astype(BF),
    )


def dot(a, b):
    return jnp.dot(a, b, preferred_element_type=F32)


def dot_nt(a, b):
    return lax.dot_general(a, b, NT, preferred_element_type=F32)


def call(
    body, out_shape, *args, scratch=(), specs=None, out_specs=None, limit=40, aliases=None
):
    vm = pl.BlockSpec(memory_space=pltpu.VMEM)
    single = not isinstance(out_shape, (tuple, list))
    if specs is None:
        specs = [vm] * len(args)
    if out_specs is None:
        out_specs = vm if single else [vm] * len(out_shape)
    return pl.pallas_call(
        body,
        out_shape=out_shape,
        in_specs=specs,
        out_specs=out_specs,
        scratch_shapes=list(scratch),
        input_output_aliases=aliases or {},
        compiler_params=pltpu.CompilerParams(vmem_limit_bytes=limit * MIB),
    )(*args)


VM = pl.BlockSpec(memory_space=pltpu.VMEM)
SM = pl.BlockSpec(memory_space=pltpu.SMEM)
HB = pl.BlockSpec(memory_space=pltpu.HBM)


def in_hbm(x):
    return pltpu.with_memory_space_constraint(x, pltpu.HBM)


def shaped(shape, dtype=BF):
    return jax.ShapeDtypeStruct(shape, dtype)


def pack_body(
    me, bricks, counts, values_at, offsets_at, send, slots, seen, aux, offsets, values, sems
):
    loads = [
        pltpu.make_async_copy(
            values_at.at[pl.ds(32 * i, 32)], values.at[pl.ds(32 * i, 32)], sems.at[i]
        )
        for i in range(4)
    ]
    for load in loads:
        load.start()
    offsets[...] = offsets_at[...].astype(F32)
    slots[DEV] = me[0]

    def clear(d, _):
        send[d] = jnp.zeros((136, 128), BF)
        aux[d] = jnp.zeros((8, 128), F32)
        seen[d] = 0
        return 0

    lax.fori_loop(0, DEV, clear, 0, unroll=4)
    lane = lax.broadcasted_iota(jnp.int32, (1, 128), 1)
    half = lax.broadcasted_iota(jnp.int32, (8, 128), 0) // 4
    for load in loads:
        load.wait()

    def one(b, _):
        head = bricks[0, b]
        owner = head >> 7
        rank = seen[owner]
        seen[owner] = rank + 1
        slots[b] = owner * 2 + rank

        send[owner, pl.ds(pl.multiple_of(rank * 64, 64), 64), :] = values[b]
        meta = jnp.where(lane == 0, counts[b], 0)
        for h in range(4):
            meta = jnp.where(lane == 1 + h, bricks[h, b] & 127, meta)
        rows = [offsets[k, pl.ds(b, 1), :] for k in range(3)] + [meta.astype(F32)]
        both = jnp.concatenate(rows + rows, 0)
        aux[owner] = aux[owner] + jnp.where(half == rank, both, 0.0)
        return 0

    lax.fori_loop(0, DEV, one, 0, unroll=2)

    def finish(d, _):
        send[d, 128:136, :] = aux[d].astype(BF)
        return 0

    lax.fori_loop(0, DEV, finish, 0, unroll=4)


def pack(me, values, offsets, counts, bricks):
    return call(
        pack_body,
        (shaped((DEV, 136, 128)), shaped((DEV + 8,), jnp.int32)),
        me, bricks.T, counts, in_hbm(values), offsets.transpose(1, 0, 2),
        scratch=(
            pltpu.SMEM((DEV,), jnp.int32),
            pltpu.VMEM((DEV, 8, 128), F32),
            pltpu.VMEM((3, 128, 128), F32),
            pltpu.VMEM((DEV, 64, 128), BF),
            pltpu.SemaphoreType.DMA((4,)),
        ),
        specs=[SM, SM, SM, HB, VM],
        out_specs=[VM, SM],
        limit=24,
    )


def spread_weights(place, count, ids):
    lane = lax.broadcasted_iota(jnp.int32, (1, 128), 1)
    sub = lax.broadcasted_iota(jnp.int32, (8, 128), 0)
    xs = ((sub // 4).astype(F32) + 0.5) * UNIT
    ys = ((sub % 4).astype(F32) + 0.5) * UNIT
    zs = (lax.broadcasted_iota(jnp.int32, (16, 128), 0).astype(F32) + 0.5) * UNIT
    place = place * UNIT
    px = jnp.where(lane < count, place[0:1], 1.0e4) - xs
    py = place[1:2] - ys
    pz = place[2:3] - zs
    grid_at = [(i >> 5, (i >> 3) & 3, i & 7) for i in ids]
    parts = []
    for h in range(4):
        shift = [(a - b).astype(F32) for a, b in zip(grid_at[h], grid_at[0])]
        dx = px - shift[0] * (2 * UNIT)
        dy = py - shift[1] * (4 * UNIT)
        dz = pz - shift[2] * (16 * UNIT)
        xy = jnp.exp2(math.log2(AMPLITUDE) - dx * dx - dy * dy)
        zz = jnp.exp2(-(dz * dz))
        for i in range(8):
            parts.append((xy[i : i + 1] * zz).astype(BF))
    return jnp.concatenate(parts, 0)


def to_relative(slots, chunks, sends):
    for j in range(8):
        sends[j][...] = chunks[(slots[DEV] + j) & 7]


def from_relative(slots, gots, chunks):
    for j in range(8):
        chunks[(slots[DEV] - j) & 7] = gots[j][...]


def third_forward(by, grid_at, table, out):
    for j in range(4):
        modes = []
        for half in range(2):
            both = dot(table, grid_at(2 * j + half))
            modes.append(both[:64] + both[64:])
        for kg in range(8):
            piece = jnp.concatenate([m[8 * kg : 8 * kg + 8] for m in modes], 0)
            at = by * 64 + j * 16
            out[kg, at : at + 16, :] = piece.astype(BF)


def spread_one(rank, d, meta, rows, block, acc):
    at = d * 10 + rank * 5
    ids = [meta[at + 1 + h] for h in range(4)]
    weights = spread_weights(rows[4 * rank : 4 * rank + 3], meta[at], ids)
    tile = dot_nt(block, weights)
    for h in range(4):
        acc[ids[h]] = acc[ids[h]] + tile[:, 128 * h : 128 * h + 128]


def quarter(source, target, sems, i):
    return pltpu.make_async_copy(
        source.at[pl.ds(32 * i, 32)], target.at[pl.ds(32 * i, 32)], sems.at[i]
    )


def encode_body(meta, me, got_at, eye, z_table, grid_at, *rest):
    *sends, modes, grid, acc, got, got_sems, grid_sems = rest
    for i in range(4):
        quarter(got_at, got, got_sems, i).start()

    def clear(b, _):
        acc[b] = jnp.zeros((64, 128), F32)
        return 0

    lax.fori_loop(0, 128, clear, 0, unroll=4)

    def part(i, _):
        quarter(got_at, got, got_sems, i).wait()

        def one(k, _):
            d = 32 * i + k
            rows = got[d, 128:136, :].astype(F32)
            for rank in range(2):
                spread_one(rank, d, meta, rows, got[d, 64 * rank : 64 * rank + 64, :], acc)
            return 0

        return lax.fori_loop(0, 32, one, 0, unroll=4)

    lax.fori_loop(0, 4, part, 0)
    eye128 = eye[0:128, 0:128]
    stores = []
    for by in range(4):
        for bz in range(8):
            bricks = jnp.concatenate([acc[(bx * 4 + by) * 8 + bz] for bx in range(4)], 0)
            cells = dot_nt(eye128, bricks.astype(BF)).astype(BF)
            for xy in range(8):
                grid[by, xy, 16 * bz : 16 * bz + 16, :] = cells[16 * xy : 16 * xy + 16]
        stores.append(pltpu.make_async_copy(grid.at[by], grid_at.at[by], grid_sems.at[by]))
        stores[-1].start()
        third_forward(by, lambda xy: grid[by, xy], z_table[...], modes)
    to_relative(me, modes, sends)
    for store in stores:
        store.wait()


def encode(meta, me, got, t):
    out = call(
        encode_body,
        [pltpu.HBM((4, 8, 128, 256), BF)] + [shaped((256, 256))] * 8,
        meta, me, in_hbm(got), t["eye"], t["z_forward"],
        scratch=(
            pltpu.VMEM((8, 256, 256), BF),
            pltpu.VMEM((4, 8, 128, 256), BF),
            pltpu.VMEM((128, 64, 128), F32),
            pltpu.VMEM((DEV, 136, 128), BF),
            pltpu.SemaphoreType.DMA((4,)),
            pltpu.SemaphoreType.DMA((4,)),
        ),
        specs=[SM, SM, HB, VM, VM],
        out_specs=[HB] + [VM] * 8,
        limit=24,
    )
    return in_hbm(out[0]), out[1:]


def second_body(layer, me, *refs):
    *gots, table, order, weights_at, send, weights, got, sem = refs
    load = pltpu.make_async_copy(weights_at.at[pl.ds(layer * 64, 64)], weights, sem)
    load.start()
    from_relative(me, gots, got)
    rows = []
    for x2 in range(2):
        data = jnp.concatenate(
            [
                got[py, by * 64 + x2 * 32 : by * 64 + x2 * 32 + 32, :]
                for py in range(8)
                for by in range(4)
            ],
            0,
        )
        both = dot(table[...], data)
        out = both[:256] + both[256:]
        for bx in range(4):
            rows.append(
                jnp.concatenate(
                    [out[64 * k : 64 * k + 64, 64 * bx : 64 * bx + 64] for k in range(4)], 1
                ).astype(BF)
            )
    send[...] = dot(order[...], jnp.concatenate(rows, 0)).astype(BF)
    load.wait()


def mix_body(got, weights, forward, back, repeat, send, product):
    both = dot(forward[...], got[...])
    modes = (both[:128] + both[128:]).astype(BF)
    spread = dot(repeat[...], modes)
    row = lax.broadcasted_iota(jnp.int32, (512, 256), 0)
    col = lax.broadcasted_iota(jnp.int32, (512, 256), 1)
    spread = jnp.where(col // 64 == (row % 8) // 2, spread, 0.0)
    for m in range(64):
        product[8 * m : 8 * m + 8, :] = dot(spread[8 * m : 8 * m + 8].astype(BF), weights[m])
    real, imag = [], []
    for kz in range(4):
        from_real = product[pl.ds(2 * kz, 64, stride=8), :]
        from_imag = product[pl.ds(2 * kz + 1, 64, stride=8), :]
        real.append(from_real[:, :64] - from_imag[:, 64:])
        imag.append(from_real[:, 64:] + from_imag[:, :64])
    mixed = jnp.concatenate([jnp.concatenate(real, 1), jnp.concatenate(imag, 1)], 0)
    high = mixed.astype(BF)
    low = (mixed - high.astype(F32)).astype(BF)
    send[...] = dot(back[...], jnp.concatenate([high, high, low], 0)).astype(BF)


def second_back_body(me, got, table, order, *rest):
    *sends, send = rest
    ordered = dot(order[...], got[...])
    for x2 in range(2):
        parts = []
        for k in range(4):
            parts.append(
                jnp.concatenate(
                    [
                        ordered[
                            (x2 * 4 + bx) * 64 : (x2 * 4 + bx) * 64 + 64, 64 * k : 64 * k + 64
                        ]
                        for bx in range(4)
                    ],
                    1,
                ).astype(BF)
            )
        data = jnp.concatenate(parts, 0)
        out = dot(table[...], jnp.concatenate([data, data], 0)).astype(BF)
        for py in range(8):
            for by in range(4):
                at = py * 128 + by * 32
                send[py, by * 64 + x2 * 32 : by * 64 + x2 * 32 + 32, :] = out[at : at + 32]
    to_relative(me, send, sends)


def layer_values(by, j, got, grid, z_back, skip, bias):
    at = by * 64 + j * 16
    data = jnp.concatenate([got[kg, at : at + 16, :] for kg in range(8)], 0)
    total = dot(z_back, jnp.concatenate([data, data], 0))
    total = total + dot(grid[by, 2 * j : 2 * j + 2].reshape(256, 256), skip)
    total = total + bias
    result = 0.5 * total * (1.0 + lax.erf(total * math.sqrt(0.5)))
    return result.astype(BF)


def load_grid(grid_at, grid, sems):
    copies = [
        pltpu.make_async_copy(grid_at.at[by], grid.at[by], sems.at[by]) for by in range(4)
    ]
    for copy in copies:
        copy.start()
    return copies


def four_fold(layer, skip, bias):
    wide = jnp.concatenate([skip[layer].astype(F32)] * 4, 1)
    tall = jnp.concatenate([wide] * 4, 0)
    row = lax.broadcasted_iota(jnp.int32, (256, 256), 0)
    col = lax.broadcasted_iota(jnp.int32, (256, 256), 1)
    matrix = jnp.where(row // 64 == col // 64, tall, 0.0).astype(BF)
    return matrix, jnp.concatenate([bias[layer : layer + 1, :]] * 4, 1)


def inner_layer_body(layer, me, *refs):
    *gots, grid_at, z_back, skip, bias, z_table, new_grid = refs[:14]
    *sends, got, grid, modes, sems = refs[14:]
    copies = load_grid(grid_at, grid, sems)
    from_relative(me, gots, got)
    skip, bias = four_fold(layer, skip, bias)
    for by in range(4):
        copies[by].wait()
        for j in range(4):
            values = layer_values(by, j, got, grid, z_back[...], skip, bias)
            new_grid[by, 2 * j] = values[:128]
            new_grid[by, 2 * j + 1] = values[128:]
        third_forward(by, lambda xy: new_grid[by, xy], z_table[...], modes)
    to_relative(me, modes, sends)


def last_layer_body(layer, me, *refs):
    *gots, grid_at, z_back, skip, bias, eye, bricks, got, grid, sems = refs
    copies = load_grid(grid_at, grid, sems)
    from_relative(me, gots, got)
    skip, bias = four_fold(layer, skip, bias)
    for by in range(4):
        copies[by].wait()
        values = [
            layer_values(by, j, got, grid, z_back[...], skip, bias) for j in range(4)
        ]
        for bz in range(8):
            cells = jnp.concatenate(
                [
                    values[xy // 2][(xy % 2) * 128 + 16 * bz : (xy % 2) * 128 + 16 * bz + 16]
                    for xy in range(8)
                ],
                0,
            )
            turned = dot_nt(eye[...], cells).astype(BF)
            for bx in range(4):
                bricks[(bx * 4 + by) * 8 + bz] = turned[64 * bx : 64 * bx + 64]


def decode_body(meta, aux, bricks, reply):
    def one(d, _):
        rows = aux[d].astype(F32)
        for rank in range(2):
            at = d * 10 + rank * 5
            ids = [meta[at + 1 + h] for h in range(4)]
            weights = spread_weights(rows[4 * rank : 4 * rank + 3], meta[at], ids)
            near = jnp.concatenate([bricks[ids[h]] for h in range(4)], 1)
            reply[d, 64 * rank : 64 * rank + 64, :] = (DECODE_SCALE * dot(near, weights)).astype(BF)
        return 0

    lax.fori_loop(0, DEV, one, 0, unroll=4)


def pick_body(slots, got, out):
    def one(b, _):
        out[b] = got[slots[b]]
        return 0

    lax.fori_loop(0, DEV, one, 0, unroll=4)


def exchange(x, axis):
    return lax.all_to_all(x, axis, split_axis=0, concat_axis=0, tiled=True)


def exchange_lines(chunks):
    got = [chunks[0]]
    for j in range(1, 8):
        got.append(lax.ppermute(chunks[j], "py", [(i, (i + j) % 8) for i in range(8)]))
    return got


def per_device(values, offsets, counts, bricks, spectral_weights, skip_weights, skip_bias):
    t = {name: jnp.asarray(table) for name, table in tables().items()}
    me = lax.axis_index("py").astype(jnp.int32).reshape(1)
    weights = in_hbm(spectral_weights.reshape(LAYERS * 64, 256, 128))
    send, slots = pack(me, values, offsets, counts, bricks)
    got = exchange(send, ("px", "py"))
    aux = lax.optimization_barrier(got[:, 128:, :])
    meta = aux[:, :, :5].reshape(DEV, 2, 4, 5)[:, :, 3].astype(jnp.int32).reshape(-1)
    grid, modes = encode(meta, slots, got, t)
    chunks = pltpu.VMEM((8, 256, 256), BF)
    grid_scratch = pltpu.VMEM((4, 8, 128, 256), BF)
    four = pltpu.SemaphoreType.DMA((4,))
    piece = shaped((256, 256))
    for layer in range(LAYERS):
        columns = exchange_lines(modes)
        second, kept = call(
            functools.partial(second_body, layer),
            [shaped((512, 256)), shaped((64, 256, 128))],
            slots, *columns, t["y_forward"], t["to_send"], weights,
            scratch=(chunks, pltpu.SemaphoreType.DMA),
            specs=[SM] + [VM] * 10 + [HB],
            limit=24,
        )
        lines = exchange(second.reshape(16, 32, 256), "px").reshape(512, 256)
        back = call(
            mix_body,
            shaped((512, 256)),
            lines, kept, t["x_forward"], t["x_back"], t["repeat"],
            scratch=(pltpu.VMEM((512, 128), F32),),
            limit=24,
        )
        lines = exchange(back.reshape(16, 32, 256), "px").reshape(512, 256)
        columns = call(
            second_back_body,
            [piece] * 8,
            slots, lines, t["y_back"], t["from_send"],
            scratch=(chunks,),
            specs=[SM, VM, VM, VM],
            limit=24,
        )
        columns = exchange_lines(columns)
        if layer + 1 < LAYERS:
            grid, *modes = call(
                functools.partial(inner_layer_body, layer),
                [shaped((4, 8, 128, 256))] + [piece] * 8,
                slots, *columns, grid, t["z_back"], skip_weights, skip_bias, t["z_forward"],
                scratch=(chunks, grid_scratch, chunks, four),
                specs=[SM] + [VM] * 8 + [HB] + [VM] * 4,
                limit=32,
            )
            grid = in_hbm(grid)
        else:
            final = call(
                functools.partial(last_layer_body, layer),
                shaped((128, 64, 128)),
                slots, *columns, grid, t["z_back"], skip_weights, skip_bias, t["eye"],
                scratch=(chunks, grid_scratch, four),
                specs=[SM] + [VM] * 8 + [HB] + [VM] * 4,
                limit=32,
            )
    reply = call(
        decode_body, shaped((DEV, 128, 128)), meta, aux, final, specs=[SM, VM, VM], limit=24
    )
    returned = exchange(reply, ("px", "py"))
    return call(
        pick_body,
        shaped((DEV, 64, 128)),
        slots, returned.reshape(2 * DEV, 64, 128),
        specs=[SM, VM],
        limit=24,
    )


def solution(mesh):
    return jax.shard_map(
        per_device,
        mesh=mesh,
        in_specs=(
            P(("px", "py"), None, None),
            P(("px", "py"), None, None),
            P(("px", "py")),
            P(("px", "py"), None),
            P(None, None, "px", "py", None, None),
            P(),
            P(),
        ),
        out_specs=P(("px", "py"), None, None),
        check_vma=False,
    )
```

```python
import functools
import math

import jax
import jax.numpy as jnp
import numpy as np
from jax import lax
from jax.experimental import pallas as pl
from jax.experimental.pallas import tpu as pltpu
from jax.sharding import PartitionSpec as P

CH = 64
MODES = 32
LAYERS = 2
DEV = 128
AMPLITUDE = 0.25
SPREAD = 4.5
DECODE_SCALE = 0.1
BF = jnp.bfloat16
F32 = jnp.float32
MIB = 1024 * 1024
NT = (((1,), (1,)), ((), ()))
UNIT = math.sqrt(math.log2(math.e) / SPREAD)


def halves(table):
    high = np.asarray(table, np.float32).astype(BF)
    low = (np.asarray(table, np.float64) - high.astype(np.float64)).astype(np.float32).astype(BF)
    return high, low


def waves():
    j = np.arange(MODES)
    return np.where(j < MODES // 2, j, j - MODES)


def turn(frequency, place):
    return 2.0 * math.pi / 128 * ((frequency * place) % 128)


def forward_pair(angle):
    c, s = np.cos(angle) / math.sqrt(128), np.sin(angle) / math.sqrt(128)
    return np.array([[c, s], [-s, c]])


def backward_pair(angle):
    c, s = np.cos(angle) / math.sqrt(128), np.sin(angle) / math.sqrt(128)
    return np.array([[c, -s], [s, c]])


@functools.lru_cache(None)
def tables():
    k = np.arange(MODES)
    z = np.arange(128)
    angle = turn(k[:, None], z[None, :])
    mz = np.stack([np.cos(angle), -np.sin(angle)], 1).reshape(64, 128) / math.sqrt(128)
    mz_high, mz_low = halves(mz)
    z_forward = np.concatenate([mz_high, mz_low], 0)
    weight = np.where(k == 0, 1.0, 2.0)[:, None, None]
    inv = np.stack([np.cos(angle), -np.sin(angle)], 1) / math.sqrt(128) * weight
    inv = inv.reshape(8, 8, 128)
    zi = np.zeros((2, 128, 8, 2, 8))
    for y2 in range(2):
        zi[y2, :, :, y2, :] = inv.transpose(2, 0, 1)
    z_back = np.concatenate(halves(zi.reshape(256, 128)), 1)
    f = waves()
    y = np.arange(128)
    pair = forward_pair(turn(f[:, None], y[None, :])).reshape(2, 2, 16, 2, 32, 4)
    ty = np.zeros((4, 16, 2, 2, 32, 4, 4, 2))
    for k4 in range(4):
        ty[k4, :, :, :, :, :, k4, :] = pair.transpose(2, 3, 0, 4, 5, 1)
    y_forward = np.concatenate(halves(ty.reshape(256, 1024)), 0)
    pair = backward_pair(turn(f[:, None], y[None, :])).reshape(2, 2, 16, 2, 32, 4)
    ti = np.zeros((32, 4, 4, 2, 4, 16, 2, 2))
    for k4 in range(4):
        ti[:, :, k4, :, k4, :, :, :] = pair.transpose(4, 5, 0, 2, 3, 1)
    y_back = np.concatenate(halves(ti.reshape(1024, 256)), 1)
    x = np.arange(128)
    pair = forward_pair(turn(f[:, None], x[None, :])).reshape(2, 2, 32, 16, 4, 2)
    tx = np.zeros((32, 2, 2, 16, 2, 4, 2, 2))
    for ky in range(2):
        tx[:, ky, :, :, :, :, ky, :] = pair.transpose(2, 0, 3, 5, 4, 1)
    x_forward = np.concatenate(halves(tx.reshape(128, 512)), 0)
    pair = backward_pair(turn(f[:, None], x[None, :])).reshape(2, 2, 32, 16, 4, 2)
    txi = np.zeros((16, 2, 4, 2, 2, 2, 32, 2))
    for ky in range(2):
        txi[:, :, :, ky, :, :, :, ky] = pair.transpose(3, 5, 4, 0, 1, 2)
    high, low = halves(txi.reshape(512, 128))
    x_back = np.concatenate([high, low, high], 1)
    order = np.arange(512).reshape(8, 16, 4).transpose(1, 0, 2).reshape(-1)
    to_send = np.eye(512)[order].astype(BF)
    from_send = np.ascontiguousarray(np.eye(512)[order].T).astype(BF)
    row = np.arange(512)
    repeat = np.eye(128)[(row // 8) * 2 + row % 2].astype(BF)
    return dict(
        z_forward=z_forward, z_back=z_back, y_forward=y_forward, y_back=y_back,
        x_forward=x_forward, x_back=x_back, to_send=to_send, from_send=from_send,
        repeat=repeat, eye=np.eye(256).astype(BF),
    )


def dot(a, b):
    return jnp.dot(a, b, preferred_element_type=F32)


def dot_nt(a, b):
    return lax.dot_general(a, b, NT, preferred_element_type=F32)


def call(
    body, out_shape, *args, scratch=(), specs=None, out_specs=None, limit=40, aliases=None
):
    vm = pl.BlockSpec(memory_space=pltpu.VMEM)
    single = not isinstance(out_shape, (tuple, list))
    if specs is None:
        specs = [vm] * len(args)
    if out_specs is None:
        out_specs = vm if single else [vm] * len(out_shape)
    return pl.pallas_call(
        body,
        out_shape=out_shape,
        in_specs=specs,
        out_specs=out_specs,
        scratch_shapes=list(scratch),
        input_output_aliases=aliases or {},
        compiler_params=pltpu.CompilerParams(vmem_limit_bytes=limit * MIB),
    )(*args)


VM = pl.BlockSpec(memory_space=pltpu.VMEM)
SM = pl.BlockSpec(memory_space=pltpu.SMEM)
HB = pl.BlockSpec(memory_space=pltpu.HBM)


def in_hbm(x):
    return pltpu.with_memory_space_constraint(x, pltpu.HBM)


def shaped(shape, dtype=BF):
    return jax.ShapeDtypeStruct(shape, dtype)


def pack_body(
    me, bricks_at, counts_at, values_at, offsets_at, send, slots,
    seen, aux, bricks, counts, offsets_in, offsets, values, sems,
):
    loads = [
        pltpu.make_async_copy(
            values_at.at[pl.ds(32 * i, 32)], values.at[pl.ds(32 * i, 32)], sems.at[i]
        )
        for i in range(4)
    ]
    for load in loads:
        load.start()
    small = [
        pltpu.make_async_copy(source, target, sems.at[4 + i])
        for i, (source, target) in enumerate(
            [(bricks_at, bricks), (counts_at, counts), (offsets_at, offsets_in)]
        )
    ]
    for load in small:
        load.start()
    slots[DEV] = me[0]

    def clear(d, _):
        send[d] = jnp.zeros((136, 128), BF)
        aux[d] = jnp.zeros((8, 128), F32)
        seen[d] = 0
        return 0

    lax.fori_loop(0, DEV, clear, 0, unroll=4)
    lane = lax.broadcasted_iota(jnp.int32, (1, 128), 1)
    half = lax.broadcasted_iota(jnp.int32, (8, 128), 0) // 4
    for load in small:
        load.wait()
    offsets[...] = offsets_in[...].astype(F32)
    for load in loads:
        load.wait()

    def one(b, _):
        head = bricks[0, b]
        owner = head >> 7
        rank = seen[owner]
        seen[owner] = rank + 1
        slots[b] = owner * 2 + rank

        send[owner, pl.ds(pl.multiple_of(rank * 64, 64), 64), :] = values[b]
        meta = jnp.where(lane == 0, counts[b], 0)
        for h in range(4):
            meta = jnp.where(lane == 1 + h, bricks[h, b] & 127, meta)
        rows = [offsets[k, pl.ds(b, 1), :] for k in range(3)] + [meta.astype(F32)]
        both = jnp.concatenate(rows + rows, 0)
        aux[owner] = aux[owner] + jnp.where(half == rank, both, 0.0)
        return 0

    lax.fori_loop(0, DEV, one, 0, unroll=2)

    def finish(d, _):
        send[d, 128:136, :] = aux[d].astype(BF)
        return 0

    lax.fori_loop(0, DEV, finish, 0, unroll=4)


def pack(me, values, offsets, counts, bricks):
    return call(
        pack_body,
        (shaped((DEV, 136, 128)), shaped((DEV + 8,), jnp.int32)),
        me, in_hbm(bricks.T), in_hbm(counts), in_hbm(values), in_hbm(offsets.transpose(1, 0, 2)),
        scratch=(
            pltpu.SMEM((DEV,), jnp.int32),
            pltpu.VMEM((DEV, 8, 128), F32),
            pltpu.SMEM((4, DEV), jnp.int32),
            pltpu.SMEM((DEV,), jnp.int32),
            pltpu.VMEM((3, 128, 128), BF),
            pltpu.VMEM((3, 128, 128), F32),
            pltpu.VMEM((DEV, 64, 128), BF),
            pltpu.SemaphoreType.DMA((7,)),
        ),
        specs=[SM, HB, HB, HB, HB],
        out_specs=[VM, SM],
        limit=24,
    )


def spread_weights(place, count, ids):
    lane = lax.broadcasted_iota(jnp.int32, (1, 128), 1)
    sub = lax.broadcasted_iota(jnp.int32, (8, 128), 0)
    xs = ((sub // 4).astype(F32) + 0.5) * UNIT
    ys = ((sub % 4).astype(F32) + 0.5) * UNIT
    zs = (lax.broadcasted_iota(jnp.int32, (16, 128), 0).astype(F32) + 0.5) * UNIT
    place = place * UNIT
    px = jnp.where(lane < count, place[0:1], 1.0e4) - xs
    py = place[1:2] - ys
    pz = place[2:3] - zs
    grid_at = [(i >> 5, (i >> 3) & 3, i & 7) for i in ids]
    parts = []
    for h in range(4):
        shift = [(a - b).astype(F32) for a, b in zip(grid_at[h], grid_at[0])]
        dx = px - shift[0] * (2 * UNIT)
        dy = py - shift[1] * (4 * UNIT)
        dz = pz - shift[2] * (16 * UNIT)
        xy = jnp.exp2(math.log2(AMPLITUDE) - dx * dx - dy * dy)
        zz = jnp.exp2(-(dz * dz))
        for i in range(8):
            parts.append((xy[i : i + 1] * zz).astype(BF))
    return jnp.concatenate(parts, 0)


def to_relative(slots, chunks, sends):
    for j in range(8):
        sends[j][...] = chunks[(slots[DEV] + j) & 7]


def from_relative(slots, gots, chunks):
    for j in range(8):
        chunks[(slots[DEV] - j) & 7] = gots[j][...]


def third_forward(by, grid_at, table, out):
    for j in range(4):
        modes = []
        for half in range(2):
            both = dot(table, grid_at(2 * j + half))
            modes.append(both[:64] + both[64:])
        for kg in range(8):
            piece = jnp.concatenate([m[8 * kg : 8 * kg + 8] for m in modes], 0)
            at = by * 64 + j * 16
            out[kg, at : at + 16, :] = piece.astype(BF)


def block_weights(rank, d, meta, rows):
    ids = [meta[8 * rank + 1 + h, d] for h in range(4)]
    return ids, spread_weights(rows[4 * rank : 4 * rank + 3], meta[8 * rank, d], ids)


def spread_one(rank, d, meta, rows, block, acc):
    ids, weights = block_weights(rank, d, meta, rows)
    tile = dot_nt(block, weights)
    for h in range(4):
        acc[ids[h]] = acc[ids[h]] + tile[:, 128 * h : 128 * h + 128]


def quarter(source, target, sems, i):
    return pltpu.make_async_copy(
        source.at[pl.ds(32 * i, 32)], target.at[pl.ds(32 * i, 32)], sems.at[i]
    )


def encode_body(slots, got_at, eye, z_table, weights_at, grid_at, aux, meta_out, weights, *rest):
    *sends, modes, grid, acc, got, wide, meta, got_sems, grid_sems, sems = rest
    first = pltpu.make_async_copy(got_at.at[:, pl.ds(128, 8), :], aux, sems.at[0])
    first.start()
    for i in range(4):
        quarter(got_at, got, got_sems, i).start()
    fetch = pltpu.make_async_copy(weights_at.at[pl.ds(0, 64)], weights, sems.at[1])
    fetch.start()
    first.wait()
    wide[...] = aux[...].astype(F32).reshape(8 * DEV, 128)
    for rank in range(2):
        numbers = wide[pl.ds(4 * rank + 3, DEV, stride=8), :].T
        meta_out[8 * rank : 8 * rank + 8, :] = numbers[0:8].astype(jnp.int32)
    to_scalar = pltpu.make_async_copy(meta_out, meta, sems.at[2])
    to_scalar.start()

    def clear(b, _):
        acc[b] = jnp.zeros((64, 128), F32)
        return 0

    lax.fori_loop(0, 128, clear, 0, unroll=4)

    to_scalar.wait()

    def part(i, _):
        quarter(got_at, got, got_sems, i).wait()

        def one(k, _):
            d = 32 * i + k
            rows = aux[d].astype(F32)
            for rank in range(2):
                spread_one(rank, d, meta, rows, got[d, 64 * rank : 64 * rank + 64, :], acc)
            return 0

        return lax.fori_loop(0, 32, one, 0, unroll=8)

    lax.fori_loop(0, 4, part, 0)
    eye128 = eye[0:128, 0:128]
    stores = []
    for by in range(4):
        for bz in range(8):
            bricks = jnp.concatenate([acc[(bx * 4 + by) * 8 + bz] for bx in range(4)], 0)
            cells = dot_nt(eye128, bricks.astype(BF)).astype(BF)
            for xy in range(8):
                grid[by, xy, 16 * bz : 16 * bz + 16, :] = cells[16 * xy : 16 * xy + 16]
        stores.append(pltpu.make_async_copy(grid.at[by], grid_at.at[by], grid_sems.at[by]))
        stores[-1].start()
        third_forward(by, lambda xy: grid[by, xy], z_table[...], modes)
    to_relative(slots, modes, sends)
    for store in stores:
        store.wait()
    fetch.wait()


def encode(slots, got, weights, t):
    out = call(
        encode_body,
        [
            pltpu.HBM((4, 8, 128, 256), BF),
            shaped((DEV, 8, 128)),
            shaped((16, DEV), jnp.int32),
            shaped((64, 256, 128)),
        ]
        + [shaped((256, 256))] * 8,
        slots, in_hbm(got), t["eye"], t["z_forward"], weights,
        scratch=(
            pltpu.VMEM((8, 256, 256), BF),
            pltpu.VMEM((4, 8, 128, 256), BF),
            pltpu.VMEM((128, 64, 128), F32),
            pltpu.VMEM((DEV, 136, 128), BF),
            pltpu.VMEM((8 * DEV, 128), F32),
            pltpu.SMEM((16, DEV), jnp.int32),
            pltpu.SemaphoreType.DMA((4,)),
            pltpu.SemaphoreType.DMA((4,)),
            pltpu.SemaphoreType.DMA((3,)),
        ),
        specs=[SM, HB, VM, VM, HB],
        out_specs=[HB] + [VM] * 11,
        limit=24,
    )
    return in_hbm(out[0]), out[1], out[2], out[3], out[4:]


def second_body(me, *refs):
    *gots, table, order, send, got = refs
    from_relative(me, gots, got)
    rows = []
    for x2 in range(2):
        data = jnp.concatenate(
            [
                got[py, by * 64 + x2 * 32 : by * 64 + x2 * 32 + 32, :]
                for py in range(8)
                for by in range(4)
            ],
            0,
        )
        both = dot(table[...], data)
        out = both[:256] + both[256:]
        for bx in range(4):
            rows.append(
                jnp.concatenate(
                    [out[64 * k : 64 * k + 64, 64 * bx : 64 * bx + 64] for k in range(4)], 1
                ).astype(BF)
            )
    send[...] = dot(order[...], jnp.concatenate(rows, 0)).astype(BF)


def mix_body(got, weights, forward, back, repeat, send, product):
    both = dot(forward[...], got[...])
    modes = (both[:128] + both[128:]).astype(BF)
    spread = dot(repeat[...], modes)
    row = lax.broadcasted_iota(jnp.int32, (512, 256), 0)
    col = lax.broadcasted_iota(jnp.int32, (512, 256), 1)
    spread = jnp.where(col // 64 == (row % 8) // 2, spread, 0.0)
    for m in range(64):
        product[8 * m : 8 * m + 8, :] = dot(spread[8 * m : 8 * m + 8].astype(BF), weights[m])
    real, imag = [], []
    for kz in range(4):
        from_real = product[pl.ds(2 * kz, 64, stride=8), :]
        from_imag = product[pl.ds(2 * kz + 1, 64, stride=8), :]
        real.append(from_real[:, :64] - from_imag[:, 64:])
        imag.append(from_real[:, 64:] + from_imag[:, :64])
    mixed = jnp.concatenate([jnp.concatenate(real, 1), jnp.concatenate(imag, 1)], 0)
    high = mixed.astype(BF)
    low = (mixed - high.astype(F32)).astype(BF)
    send[...] = dot(back[...], jnp.concatenate([high, high, low], 0)).astype(BF)


def second_back_body(me, got, table, order, *rest):
    *sends, send = rest
    ordered = dot(order[...], got[...])
    for x2 in range(2):
        parts = []
        for k in range(4):
            parts.append(
                jnp.concatenate(
                    [
                        ordered[
                            (x2 * 4 + bx) * 64 : (x2 * 4 + bx) * 64 + 64, 64 * k : 64 * k + 64
                        ]
                        for bx in range(4)
                    ],
                    1,
                ).astype(BF)
            )
        data = jnp.concatenate(parts, 0)
        out = dot(table[...], jnp.concatenate([data, data], 0)).astype(BF)
        for py in range(8):
            for by in range(4):
                at = py * 128 + by * 32
                send[py, by * 64 + x2 * 32 : by * 64 + x2 * 32 + 32, :] = out[at : at + 32]
    to_relative(me, send, sends)


def layer_values(by, j, got, grid, z_back, skip, bias):
    at = by * 64 + j * 16
    data = jnp.concatenate([got[kg, at : at + 16, :] for kg in range(8)], 0)
    total = dot(z_back, jnp.concatenate([data, data], 0))
    total = total + dot(grid[by, 2 * j : 2 * j + 2].reshape(256, 256), skip)
    total = total + bias
    result = 0.5 * total * (1.0 + lax.erf(total * math.sqrt(0.5)))
    return result.astype(BF)


def load_grid(grid_at, grid, sems):
    copies = [
        pltpu.make_async_copy(grid_at.at[by], grid.at[by], sems.at[by]) for by in range(4)
    ]
    for copy in copies:
        copy.start()
    return copies


def four_fold(layer, skip, bias):
    wide = jnp.concatenate([skip[layer].astype(F32)] * 4, 1)
    tall = jnp.concatenate([wide] * 4, 0)
    row = lax.broadcasted_iota(jnp.int32, (256, 256), 0)
    col = lax.broadcasted_iota(jnp.int32, (256, 256), 1)
    matrix = jnp.where(row // 64 == col // 64, tall, 0.0).astype(BF)
    return matrix, jnp.concatenate([bias[layer : layer + 1, :]] * 4, 1)


def inner_layer_body(layer, me, *refs):
    *gots, grid_at, z_back, skip, bias, z_table, weights_at, new_grid_at, weights = refs[:16]
    *sends, got, grid, new_grid, modes, sems, out_sems, sem = refs[16:]
    copies = load_grid(grid_at, grid, sems)
    fetch = pltpu.make_async_copy(weights_at.at[pl.ds(layer * 64 + 64, 64)], weights, sem)
    fetch.start()
    from_relative(me, gots, got)
    skip, bias = four_fold(layer, skip, bias)
    stores = []
    for by in range(4):
        copies[by].wait()
        for j in range(4):
            values = layer_values(by, j, got, grid, z_back[...], skip, bias)
            new_grid[by, 2 * j] = values[:128]
            new_grid[by, 2 * j + 1] = values[128:]
        stores.append(
            pltpu.make_async_copy(new_grid.at[by], new_grid_at.at[by], out_sems.at[by])
        )
        stores[-1].start()
        third_forward(by, lambda xy: new_grid[by, xy], z_table[...], modes)
    to_relative(me, modes, sends)
    for store in stores:
        store.wait()
    fetch.wait()


def last_layer_body(layer, me, *refs):
    *gots, grid_at, z_back, skip, bias, eye, bricks, got, grid, sems = refs
    copies = load_grid(grid_at, grid, sems)
    from_relative(me, gots, got)
    skip, bias = four_fold(layer, skip, bias)
    for by in range(4):
        copies[by].wait()
        values = [
            layer_values(by, j, got, grid, z_back[...], skip, bias) for j in range(4)
        ]
        for bz in range(8):
            cells = jnp.concatenate(
                [
                    values[xy // 2][(xy % 2) * 128 + 16 * bz : (xy % 2) * 128 + 16 * bz + 16]
                    for xy in range(8)
                ],
                0,
            )
            turned = dot_nt(eye[...], cells).astype(BF)
            for bx in range(4):
                bricks[(bx * 4 + by) * 8 + bz] = turned[64 * bx : 64 * bx + 64]


def decode_body(meta, aux, bricks, reply):
    def one(d, _):
        rows = aux[d].astype(F32)
        near, weights = [], []
        for rank in range(2):
            ids, kernel = block_weights(rank, d, meta, rows)
            weights.append(kernel)
            near.append(jnp.concatenate([bricks[i] for i in ids], 1))
        both = DECODE_SCALE * dot(jnp.concatenate(near, 0), jnp.concatenate(weights, 1))
        reply[d, 0:64, :] = both[:64, :128].astype(BF)
        reply[d, 64:128, :] = both[64:, 128:].astype(BF)
        return 0

    lax.fori_loop(0, DEV, one, 0, unroll=8)


def pick_body(slots, got, out_at, out, sems):
    def part(i, _):
        def one(k, _):
            b = 32 * i + k
            out[b] = got[slots[b]]
            return 0

        lax.fori_loop(0, 32, one, 0, unroll=8)
        quarter(out, out_at, sems, i).start()
        return 0

    lax.fori_loop(0, 4, part, 0)
    for i in range(4):
        quarter(out, out_at, sems, i).wait()


def exchange(x, axis):
    return lax.all_to_all(x, axis, split_axis=0, concat_axis=0, tiled=True)


def exchange_lines(chunks):
    got = [chunks[0]]
    for j in range(1, 8):
        got.append(lax.ppermute(chunks[j], "py", [(i, (i + j) % 8) for i in range(8)]))
    return got


def per_device(values, offsets, counts, bricks, spectral_weights, skip_weights, skip_bias):
    t = {name: jnp.asarray(table) for name, table in tables().items()}
    me = lax.axis_index("py").astype(jnp.int32).reshape(1)
    weights = in_hbm(spectral_weights.reshape(LAYERS * 64, 256, 128))
    send, slots = pack(me, values, offsets, counts, bricks)
    got = exchange(send, ("px", "py"))
    grid, aux, meta, kept, modes = encode(slots, got, weights, t)
    chunks = pltpu.VMEM((8, 256, 256), BF)
    grid_scratch = pltpu.VMEM((4, 8, 128, 256), BF)
    four = pltpu.SemaphoreType.DMA((4,))
    piece = shaped((256, 256))
    for layer in range(LAYERS):
        columns = exchange_lines(modes)
        second = call(
            second_body,
            shaped((512, 256)),
            slots, *columns, t["y_forward"], t["to_send"],
            scratch=(chunks,),
            specs=[SM] + [VM] * 10,
            limit=24,
        )
        lines = exchange(second.reshape(16, 32, 256), "px").reshape(512, 256)
        back = call(
            mix_body,
            shaped((512, 256)),
            lines, kept, t["x_forward"], t["x_back"], t["repeat"],
            scratch=(pltpu.VMEM((512, 128), F32),),
            limit=24,
        )
        lines = exchange(back.reshape(16, 32, 256), "px").reshape(512, 256)
        columns = call(
            second_back_body,
            [piece] * 8,
            slots, lines, t["y_back"], t["from_send"],
            scratch=(chunks,),
            specs=[SM, VM, VM, VM],
            limit=24,
        )
        columns = exchange_lines(columns)
        if layer + 1 < LAYERS:
            grid, kept, *modes = call(
                functools.partial(inner_layer_body, layer),
                [pltpu.HBM((4, 8, 128, 256), BF), shaped((64, 256, 128))] + [piece] * 8,
                slots, *columns, grid, t["z_back"], skip_weights, skip_bias, t["z_forward"],
                weights,
                scratch=(
                    chunks, grid_scratch, grid_scratch, chunks, four, four,
                    pltpu.SemaphoreType.DMA,
                ),
                specs=[SM] + [VM] * 8 + [HB] + [VM] * 4 + [HB],
                out_specs=[HB] + [VM] * 9,
                limit=32,
            )
            grid = in_hbm(grid)
        else:
            final = call(
                functools.partial(last_layer_body, layer),
                shaped((128, 64, 128)),
                slots, *columns, grid, t["z_back"], skip_weights, skip_bias, t["eye"],
                scratch=(chunks, grid_scratch, four),
                specs=[SM] + [VM] * 8 + [HB] + [VM] * 4,
                limit=32,
            )
    reply = call(
        decode_body, shaped((DEV, 128, 128)), meta, aux, final, specs=[SM, VM, VM], limit=24
    )
    returned = exchange(reply, ("px", "py"))
    return call(
        pick_body,
        shaped((DEV, 64, 128)),
        slots, returned.reshape(2 * DEV, 64, 128),
        scratch=(pltpu.VMEM((DEV, 64, 128), BF), pltpu.SemaphoreType.DMA((4,))),
        specs=[SM, VM],
        out_specs=HB,
        limit=24,
    )


def solution(mesh):
    return jax.shard_map(
        per_device,
        mesh=mesh,
        in_specs=(
            P(("px", "py"), None, None),
            P(("px", "py"), None, None),
            P(("px", "py")),
            P(("px", "py"), None),
            P(None, None, "px", "py", None, None),
            P(),
            P(),
        ),
        out_specs=P(("px", "py"), None, None),
        check_vma=False,
    )
```

```python
import functools
import math

import jax
import jax.numpy as jnp
import numpy as np
from jax import lax
from jax.experimental import pallas as pl
from jax.experimental.pallas import tpu as pltpu
from jax.sharding import PartitionSpec as P

CH = 64
MODES = 32
LAYERS = 2
DEV = 128
AMPLITUDE = 0.25
SPREAD = 4.5
DECODE_SCALE = 0.1
BF = jnp.bfloat16
F32 = jnp.float32
MIB = 1024 * 1024
NT = (((1,), (1,)), ((), ()))
UNIT = math.sqrt(math.log2(math.e) / SPREAD)


def halves(table):
    high = np.asarray(table, np.float32).astype(BF)
    low = (np.asarray(table, np.float64) - high.astype(np.float64)).astype(np.float32).astype(BF)
    return high, low


def waves():
    j = np.arange(MODES)
    return np.where(j < MODES // 2, j, j - MODES)


def turn(frequency, place):
    return 2.0 * math.pi / 128 * ((frequency * place) % 128)


def forward_pair(angle):
    c, s = np.cos(angle) / math.sqrt(128), np.sin(angle) / math.sqrt(128)
    return np.array([[c, s], [-s, c]])


def backward_pair(angle):
    c, s = np.cos(angle) / math.sqrt(128), np.sin(angle) / math.sqrt(128)
    return np.array([[c, -s], [s, c]])


@functools.lru_cache(None)
def tables():
    k = np.arange(MODES)
    z = np.arange(128)
    angle = turn(k[:, None], z[None, :])
    mz = np.stack([np.cos(angle), -np.sin(angle)], 1).reshape(64, 128) / math.sqrt(128)
    mz_high, mz_low = halves(mz)
    z_forward = np.concatenate([mz_high, mz_low], 0)
    weight = np.where(k == 0, 1.0, 2.0)[:, None, None]
    inv = np.stack([np.cos(angle), -np.sin(angle)], 1) / math.sqrt(128) * weight
    inv = inv.reshape(8, 8, 128)
    zi = np.zeros((2, 128, 8, 2, 8))
    for y2 in range(2):
        zi[y2, :, :, y2, :] = inv.transpose(2, 0, 1)
    z_back = np.concatenate(halves(zi.reshape(256, 128)), 1)
    f = waves()
    y = np.arange(128)
    pair = forward_pair(turn(f[:, None], y[None, :])).reshape(2, 2, 16, 2, 32, 4)
    ty = np.zeros((4, 16, 2, 2, 32, 4, 4, 2))
    for k4 in range(4):
        ty[k4, :, :, :, :, :, k4, :] = pair.transpose(2, 3, 0, 4, 5, 1)
    y_forward = np.concatenate(halves(ty.reshape(256, 1024)), 0)
    pair = backward_pair(turn(f[:, None], y[None, :])).reshape(2, 2, 16, 2, 32, 4)
    ti = np.zeros((32, 4, 4, 2, 4, 16, 2, 2))
    for k4 in range(4):
        ti[:, :, k4, :, k4, :, :, :] = pair.transpose(4, 5, 0, 2, 3, 1)
    y_back = np.concatenate(halves(ti.reshape(1024, 256)), 1)
    x = np.arange(128)
    pair = forward_pair(turn(f[:, None], x[None, :])).reshape(2, 2, 32, 16, 4, 2)
    tx = np.zeros((32, 2, 2, 16, 2, 4, 2, 2))
    for ky in range(2):
        tx[:, ky, :, :, :, :, ky, :] = pair.transpose(2, 0, 3, 5, 4, 1)
    x_forward = np.concatenate(halves(tx.reshape(128, 512)), 0)
    pair = backward_pair(turn(f[:, None], x[None, :])).reshape(2, 2, 32, 16, 4, 2)
    txi = np.zeros((16, 2, 4, 2, 2, 2, 32, 2))
    for ky in range(2):
        txi[:, :, :, ky, :, :, :, ky] = pair.transpose(3, 5, 4, 0, 1, 2)
    high, low = halves(txi.reshape(512, 128))
    x_back = np.concatenate([high, low, high], 1)
    order = np.arange(512).reshape(8, 16, 4).transpose(1, 0, 2).reshape(-1)
    to_send = np.eye(512)[order].astype(BF)
    from_send = np.ascontiguousarray(np.eye(512)[order].T).astype(BF)
    row = np.arange(512)
    repeat = np.eye(128)[(row // 8) * 2 + row % 2].astype(BF)
    return dict(
        z_forward=z_forward, z_back=z_back, y_forward=y_forward, y_back=y_back,
        x_forward=x_forward, x_back=x_back, to_send=to_send, from_send=from_send,
        repeat=repeat, eye=np.eye(256).astype(BF),
    )


def dot(a, b):
    return jnp.dot(a, b, preferred_element_type=F32)


def dot_nt(a, b):
    return lax.dot_general(a, b, NT, preferred_element_type=F32)


def call(
    body, out_shape, *args, scratch=(), specs=None, out_specs=None, limit=40, flops=None
):
    vm = pl.BlockSpec(memory_space=pltpu.VMEM)
    single = not isinstance(out_shape, (tuple, list))
    if specs is None:
        specs = [vm] * len(args)
    if out_specs is None:
        out_specs = vm if single else [vm] * len(out_shape)
    return pl.pallas_call(
        body,
        out_shape=out_shape,
        in_specs=specs,
        out_specs=out_specs,
        scratch_shapes=list(scratch),
        cost_estimate=flops and pl.CostEstimate(
            flops=flops, bytes_accessed=flops // 100, transcendentals=0
        ),
        compiler_params=pltpu.CompilerParams(vmem_limit_bytes=limit * MIB),
    )(*args)


VM = pl.BlockSpec(memory_space=pltpu.VMEM)
SM = pl.BlockSpec(memory_space=pltpu.SMEM)
HB = pl.BlockSpec(memory_space=pltpu.HBM)


def in_hbm(x):
    return pltpu.with_memory_space_constraint(x, pltpu.HBM)


def shaped(shape, dtype=BF):
    return jax.ShapeDtypeStruct(shape, dtype)


def pack_body(
    me, bricks_at, counts_at, values_at, offsets_at, send, slots,
    seen, aux, bricks, counts, offsets_in, offsets, values, sems,
):
    loads = [
        pltpu.make_async_copy(
            values_at.at[pl.ds(32 * i, 32)], values.at[pl.ds(32 * i, 32)], sems.at[i]
        )
        for i in range(4)
    ]
    for load in loads:
        load.start()
    small = [
        pltpu.make_async_copy(source, target, sems.at[4 + i])
        for i, (source, target) in enumerate(
            [(bricks_at, bricks), (counts_at, counts), (offsets_at, offsets_in)]
        )
    ]
    for load in small:
        load.start()
    slots[DEV] = me[0]

    def clear(d, _):
        send[d] = jnp.zeros((136, 128), BF)
        aux[d] = jnp.zeros((8, 128), F32)
        seen[d] = 0
        return 0

    lax.fori_loop(0, DEV, clear, 0, unroll=4)
    lane = lax.broadcasted_iota(jnp.int32, (1, 128), 1)
    for load in small:
        load.wait()
    offsets[...] = offsets_in[...].astype(F32)
    for load in loads:
        load.wait()

    def one(b, _):
        head = bricks[0, b]
        owner = head >> 7
        rank = seen[owner]
        seen[owner] = rank + 1
        slots[b] = owner * 2 + rank

        send[owner, pl.ds(pl.multiple_of(rank * 64, 64), 64), :] = values[b]
        meta = jnp.where(lane == 0, counts[b], 0)
        for h in range(4):
            meta = jnp.where(lane == 1 + h, bricks[h, b] & 127, meta)
        rows = [offsets[k, pl.ds(b, 1), :] for k in range(3)] + [meta.astype(F32)]
        aux[owner, pl.ds(pl.multiple_of(4 * rank, 4), 4), :] = jnp.concatenate(rows, 0)
        return 0

    lax.fori_loop(0, DEV, one, 0, unroll=8)

    def finish(d, _):
        send[d, 128:136, :] = aux[d].astype(BF)
        return 0

    lax.fori_loop(0, DEV, finish, 0, unroll=4)


def pack(me, values, offsets, counts, bricks):
    return call(
        pack_body,
        (shaped((DEV, 136, 128)), shaped((DEV + 8,), jnp.int32)),
        me, in_hbm(bricks.T), in_hbm(counts), in_hbm(values), in_hbm(offsets.transpose(1, 0, 2)),
        scratch=(
            pltpu.SMEM((DEV,), jnp.int32),
            pltpu.VMEM((DEV, 8, 128), F32),
            pltpu.SMEM((4, DEV), jnp.int32),
            pltpu.SMEM((DEV,), jnp.int32),
            pltpu.VMEM((3, 128, 128), BF),
            pltpu.VMEM((3, 128, 128), F32),
            pltpu.VMEM((DEV, 64, 128), BF),
            pltpu.SemaphoreType.DMA((7,)),
        ),
        specs=[SM, HB, HB, HB, HB],
        out_specs=[VM, SM],
        limit=24,
    )


def spread_weights(place, count, ids):
    lane = lax.broadcasted_iota(jnp.int32, (1, 128), 1)
    sub = lax.broadcasted_iota(jnp.int32, (8, 128), 0)
    xs = ((sub // 4).astype(F32) + 0.5) * UNIT
    ys = ((sub % 4).astype(F32) + 0.5) * UNIT
    zs = (lax.broadcasted_iota(jnp.int32, (16, 128), 0).astype(F32) + 0.5) * UNIT
    place = place * UNIT
    px = jnp.where(lane < count, place[0:1], 1.0e4) - xs
    py = place[1:2] - ys
    pz = place[2:3] - zs
    grid_at = [(i >> 5, (i >> 3) & 3, i & 7) for i in ids]
    parts = []
    for h in range(4):
        shift = [(a - b).astype(F32) for a, b in zip(grid_at[h], grid_at[0])]
        dx = px - shift[0] * (2 * UNIT)
        dy = py - shift[1] * (4 * UNIT)
        dz = pz - shift[2] * (16 * UNIT)
        xy = jnp.exp2(math.log2(AMPLITUDE) - dx * dx - dy * dy)
        zz = jnp.exp2(-(dz * dz))
        for i in range(8):
            parts.append((xy[i : i + 1] * zz).astype(BF))
    return jnp.concatenate(parts, 0)


def to_relative(slots, chunks, sends):
    for j in range(8):
        sends[j][...] = chunks[(slots[DEV] + j) & 7]


def from_relative(slots, gots, chunks):
    for j in range(8):
        chunks[(slots[DEV] - j) & 7] = gots[j][...]


def third_forward(by, grid_at, table, out):
    for j in range(4):
        modes = []
        for half in range(2):
            both = dot(table, grid_at(2 * j + half))
            modes.append(both[:64] + both[64:])
        for kg in range(8):
            piece = jnp.concatenate([m[8 * kg : 8 * kg + 8] for m in modes], 0)
            at = by * 64 + j * 16
            out[kg, at : at + 16, :] = piece.astype(BF)


def block_weights(rank, d, meta, rows):
    ids = [meta[8 * rank + 1 + h, d] for h in range(4)]
    return ids, spread_weights(rows[4 * rank : 4 * rank + 3], meta[8 * rank, d], ids)


def spread_one(rank, d, meta, rows, block, acc):
    ids, weights = block_weights(rank, d, meta, rows)
    tile = dot_nt(block, weights)
    for h in range(4):
        acc[ids[h]] = acc[ids[h]] + tile[:, 128 * h : 128 * h + 128]


def quarter(source, target, sems, i):
    return pltpu.make_async_copy(
        source.at[pl.ds(32 * i, 32)], target.at[pl.ds(32 * i, 32)], sems.at[i]
    )


def encode_body(slots, got_at, eye, z_table, weights_at, grid_at, aux, meta_out, weights, *rest):
    *sends, modes, grid, acc, got, wide, meta, got_sems, grid_sems, sems = rest
    first = pltpu.make_async_copy(got_at.at[:, pl.ds(128, 8), :], aux, sems.at[0])
    first.start()
    for i in range(4):
        quarter(got_at, got, got_sems, i).start()
    fetch = pltpu.make_async_copy(weights_at.at[pl.ds(0, 64)], weights, sems.at[1])
    fetch.start()
    first.wait()
    wide[...] = aux[...].astype(F32).reshape(8 * DEV, 128)
    for rank in range(2):
        numbers = wide[pl.ds(4 * rank + 3, DEV, stride=8), :].T
        meta_out[8 * rank : 8 * rank + 8, :] = numbers[0:8].astype(jnp.int32)
    to_scalar = pltpu.make_async_copy(meta_out, meta, sems.at[2])
    to_scalar.start()

    def clear(b, _):
        acc[b] = jnp.zeros((64, 128), F32)
        return 0

    lax.fori_loop(0, 128, clear, 0, unroll=4)

    to_scalar.wait()

    def part(i, _):
        quarter(got_at, got, got_sems, i).wait()

        def one(k, _):
            d = 32 * i + k
            rows = aux[d].astype(F32)
            for rank in range(2):
                spread_one(rank, d, meta, rows, got[d, 64 * rank : 64 * rank + 64, :], acc)
            return 0

        return lax.fori_loop(0, 32, one, 0, unroll=16)

    lax.fori_loop(0, 4, part, 0)
    eye128 = eye[0:128, 0:128]
    stores = []
    for by in range(4):
        for bz in range(8):
            bricks = jnp.concatenate([acc[(bx * 4 + by) * 8 + bz] for bx in range(4)], 0)
            cells = dot_nt(eye128, bricks.astype(BF)).astype(BF)
            for xy in range(8):
                grid[by, xy, 16 * bz : 16 * bz + 16, :] = cells[16 * xy : 16 * xy + 16]
        stores.append(pltpu.make_async_copy(grid.at[by], grid_at.at[by], grid_sems.at[by]))
        stores[-1].start()
        third_forward(by, lambda xy: grid[by, xy], z_table[...], modes)
    to_relative(slots, modes, sends)
    for store in stores:
        store.wait()
    fetch.wait()


def encode(slots, got, weights, t):
    out = call(
        encode_body,
        [
            pltpu.HBM((4, 8, 128, 256), BF),
            shaped((DEV, 8, 128)),
            shaped((16, DEV), jnp.int32),
            shaped((64, 256, 128)),
        ]
        + [shaped((256, 256))] * 8,
        slots, in_hbm(got), t["eye"], t["z_forward"], weights,
        scratch=(
            pltpu.VMEM((8, 256, 256), BF),
            pltpu.VMEM((4, 8, 128, 256), BF),
            pltpu.VMEM((128, 64, 128), F32),
            pltpu.VMEM((DEV, 136, 128), BF),
            pltpu.VMEM((8 * DEV, 128), F32),
            pltpu.SMEM((16, DEV), jnp.int32),
            pltpu.SemaphoreType.DMA((4,)),
            pltpu.SemaphoreType.DMA((4,)),
            pltpu.SemaphoreType.DMA((3,)),
        ),
        specs=[SM, HB, VM, VM, HB],
        out_specs=[HB] + [VM] * 11,
        limit=24,
    )
    return in_hbm(out[0]), out[1], out[2], out[3], out[4:]


def second_body(me, *refs):
    *gots, table, order, send, got = refs
    from_relative(me, gots, got)
    rows = []
    for x2 in range(2):
        data = jnp.concatenate(
            [
                got[py, by * 64 + x2 * 32 : by * 64 + x2 * 32 + 32, :]
                for py in range(8)
                for by in range(4)
            ],
            0,
        )
        both = dot(table[...], data)
        out = both[:256] + both[256:]
        for bx in range(4):
            rows.append(
                jnp.concatenate(
                    [out[64 * k : 64 * k + 64, 64 * bx : 64 * bx + 64] for k in range(4)], 1
                ).astype(BF)
            )
    send[...] = dot(order[...], jnp.concatenate(rows, 0)).astype(BF)


def mix_body(got, weights, forward, back, repeat, send, product):
    both = dot(forward[...], got[...])
    modes = (both[:128] + both[128:]).astype(BF)
    spread = dot(repeat[...], modes)
    row = lax.broadcasted_iota(jnp.int32, (512, 256), 0)
    col = lax.broadcasted_iota(jnp.int32, (512, 256), 1)
    spread = jnp.where(col // 64 == (row % 8) // 2, spread, 0.0)
    for m in range(64):
        product[8 * m : 8 * m + 8, :] = dot(spread[8 * m : 8 * m + 8].astype(BF), weights[m])
    real, imag = [], []
    for kz in range(4):
        from_real = product[pl.ds(2 * kz, 64, stride=8), :]
        from_imag = product[pl.ds(2 * kz + 1, 64, stride=8), :]
        real.append(from_real[:, :64] - from_imag[:, 64:])
        imag.append(from_real[:, 64:] + from_imag[:, :64])
    mixed = jnp.concatenate([jnp.concatenate(real, 1), jnp.concatenate(imag, 1)], 0)
    high = mixed.astype(BF)
    low = (mixed - high.astype(F32)).astype(BF)
    send[...] = dot(back[...], jnp.concatenate([high, high, low], 0)).astype(BF)


def second_back_body(me, got, table, order, *rest):
    *sends, send = rest
    ordered = dot(order[...], got[...])
    for x2 in range(2):
        parts = []
        for k in range(4):
            parts.append(
                jnp.concatenate(
                    [
                        ordered[
                            (x2 * 4 + bx) * 64 : (x2 * 4 + bx) * 64 + 64, 64 * k : 64 * k + 64
                        ]
                        for bx in range(4)
                    ],
                    1,
                ).astype(BF)
            )
        data = jnp.concatenate(parts, 0)
        out = dot(table[...], jnp.concatenate([data, data], 0)).astype(BF)
        for py in range(8):
            for by in range(4):
                at = py * 128 + by * 32
                send[py, by * 64 + x2 * 32 : by * 64 + x2 * 32 + 32, :] = out[at : at + 32]
    to_relative(me, send, sends)


def layer_values(by, j, got, skipped, z_back):
    at = by * 64 + j * 16
    data = jnp.concatenate([got[kg, at : at + 16, :] for kg in range(8)], 0)
    total = dot(z_back, jnp.concatenate([data, data], 0))
    total = total + skipped[by, 2 * j : 2 * j + 2].reshape(256, 256)
    result = 0.5 * total * (1.0 + lax.erf(total * math.sqrt(0.5)))
    return result.astype(BF)


def load_grid(grid_at, grid, sems):
    copies = [
        pltpu.make_async_copy(grid_at.at[by], grid.at[by], sems.at[by]) for by in range(4)
    ]
    for copy in copies:
        copy.start()
    return copies


def four_fold(layer, skip, bias):
    wide = jnp.concatenate([skip[layer].astype(F32)] * 4, 1)
    tall = jnp.concatenate([wide] * 4, 0)
    row = lax.broadcasted_iota(jnp.int32, (256, 256), 0)
    col = lax.broadcasted_iota(jnp.int32, (256, 256), 1)
    matrix = jnp.where(row // 64 == col // 64, tall, 0.0).astype(BF)
    return matrix, jnp.concatenate([bias[layer : layer + 1, :]] * 4, 1)


def skip_body(layer, anchor, grid_at, skip, bias, out_at, grid, out, sems, out_sems):
    copies = load_grid(grid_at, grid, sems)
    skip, bias = four_fold(layer, skip, bias)
    stores = []
    for by in range(4):
        copies[by].wait()
        product = dot(grid[by].reshape(1024, 256), skip) + bias
        out[by] = product.reshape(8, 128, 256)
        stores.append(pltpu.make_async_copy(out.at[by], out_at.at[by], out_sems.at[by]))
        stores[-1].start()
    for store in stores:
        store.wait()


def inner_layer_body(layer, me, *refs):
    *gots, grid_at, z_back, z_table, weights_at, new_grid_at, weights = refs[:14]
    *sends, got, grid, new_grid, modes, sems, out_sems, sem = refs[14:]
    copies = load_grid(grid_at, grid, sems)
    fetch = pltpu.make_async_copy(weights_at.at[pl.ds(layer * 64 + 64, 64)], weights, sem)
    fetch.start()
    from_relative(me, gots, got)
    stores = []
    for by in range(4):
        copies[by].wait()
        for j in range(4):
            values = layer_values(by, j, got, grid, z_back[...])
            new_grid[by, 2 * j] = values[:128]
            new_grid[by, 2 * j + 1] = values[128:]
        stores.append(
            pltpu.make_async_copy(new_grid.at[by], new_grid_at.at[by], out_sems.at[by])
        )
        stores[-1].start()
        third_forward(by, lambda xy: new_grid[by, xy], z_table[...], modes)
    to_relative(me, modes, sends)
    for store in stores:
        store.wait()
    fetch.wait()


def last_layer_body(me, *refs):
    *gots, grid_at, z_back, eye, bricks, got, grid, sems = refs
    copies = load_grid(grid_at, grid, sems)
    from_relative(me, gots, got)
    for by in range(4):
        copies[by].wait()
        values = [
            layer_values(by, j, got, grid, z_back[...]) for j in range(4)
        ]
        for bz in range(8):
            cells = jnp.concatenate(
                [
                    values[xy // 2][(xy % 2) * 128 + 16 * bz : (xy % 2) * 128 + 16 * bz + 16]
                    for xy in range(8)
                ],
                0,
            )
            turned = dot_nt(eye[...], cells).astype(BF)
            for bx in range(4):
                bricks[(bx * 4 + by) * 8 + bz] = turned[64 * bx : 64 * bx + 64]


def decode_body(meta, aux, bricks, reply):
    def one(d, _):
        rows = aux[d].astype(F32)
        near, weights = [], []
        for rank in range(2):
            ids, kernel = block_weights(rank, d, meta, rows)
            weights.append(kernel)
            near.append(jnp.concatenate([bricks[i] for i in ids], 1))
        both = DECODE_SCALE * dot(jnp.concatenate(near, 0), jnp.concatenate(weights, 1))
        reply[d, 0:64, :] = both[:64, :128].astype(BF)
        reply[d, 64:128, :] = both[64:, 128:].astype(BF)
        return 0

    lax.fori_loop(0, DEV, one, 0, unroll=16)


def pick_body(slots, got, out_at, out, sems):
    def part(i, _):
        def one(k, _):
            b = 32 * i + k
            out[b] = got[slots[b]]
            return 0

        lax.fori_loop(0, 32, one, 0, unroll=8)
        quarter(out, out_at, sems, i).start()
        return 0

    lax.fori_loop(0, 4, part, 0)
    for i in range(4):
        quarter(out, out_at, sems, i).wait()


def exchange(x, axis):
    return lax.all_to_all(x, axis, split_axis=0, concat_axis=0, tiled=True)


def exchange_lines(chunks):
    got = [chunks[0]]
    for j in range(1, 8):
        got.append(lax.ppermute(chunks[j], "py", [(i, (i + j) % 8) for i in range(8)]))
    return got


def per_device(values, offsets, counts, bricks, spectral_weights, skip_weights, skip_bias):
    t = {name: jnp.asarray(table) for name, table in tables().items()}
    me = lax.axis_index("py").astype(jnp.int32).reshape(1)
    weights = in_hbm(spectral_weights.reshape(LAYERS * 64, 256, 128))
    send, slots = pack(me, values, offsets, counts, bricks)
    got = exchange(send, ("px", "py"))
    grid, aux, meta, kept, modes = encode(slots, got, weights, t)
    chunks = pltpu.VMEM((8, 256, 256), BF)
    grid_scratch = pltpu.VMEM((4, 8, 128, 256), BF)
    skip_scratch = pltpu.VMEM((4, 8, 128, 256), F32)
    four = pltpu.SemaphoreType.DMA((4,))
    piece = shaped((256, 256))
    for layer in range(LAYERS):
        columns = exchange_lines(modes)
        second = call(
            second_body,
            shaped((512, 256)),
            slots, *columns, t["y_forward"], t["to_send"],
            scratch=(chunks,),
            specs=[SM] + [VM] * 10,
            limit=24,
        )
        lines = exchange(second.reshape(16, 32, 256), "px").reshape(512, 256)
        back = call(
            mix_body,
            shaped((512, 256)),
            lines, kept, t["x_forward"], t["x_back"], t["repeat"],
            scratch=(pltpu.VMEM((512, 128), F32),),
            limit=24,
        )
        lines = exchange(back.reshape(16, 32, 256), "px").reshape(512, 256)
        columns = call(
            second_back_body,
            [piece] * 8,
            slots, lines, t["y_back"], t["from_send"],
            scratch=(chunks,),
            specs=[SM, VM, VM, VM],
            limit=24,
        )
        skipped = in_hbm(
            call(
                functools.partial(skip_body, layer),
                pltpu.HBM((4, 8, 128, 256), F32),
                columns[0], grid, skip_weights, skip_bias,
                scratch=(grid_scratch, skip_scratch, four, four),
                specs=[VM, HB, VM, VM],
                out_specs=HB,
                limit=24,
                flops=2 * 4096 * 256 * 256,
            )
        )
        columns = exchange_lines(columns)
        if layer + 1 < LAYERS:
            grid, kept, *modes = call(
                functools.partial(inner_layer_body, layer),
                [pltpu.HBM((4, 8, 128, 256), BF), shaped((64, 256, 128))] + [piece] * 8,
                slots, *columns, skipped, t["z_back"], t["z_forward"],
                weights,
                scratch=(
                    chunks, skip_scratch, grid_scratch, chunks, four, four,
                    pltpu.SemaphoreType.DMA,
                ),
                specs=[SM] + [VM] * 8 + [HB] + [VM] * 2 + [HB],
                out_specs=[HB] + [VM] * 9,
                limit=32,
            )
            grid = in_hbm(grid)
        else:
            final = call(
                last_layer_body,
                shaped((128, 64, 128)),
                slots, *columns, skipped, t["z_back"], t["eye"],
                scratch=(chunks, skip_scratch, four),
                specs=[SM] + [VM] * 8 + [HB] + [VM] * 2,
                limit=32,
            )
    reply = call(
        decode_body, shaped((DEV, 128, 128)), meta, aux, final, specs=[SM, VM, VM], limit=24
    )
    returned = exchange(reply, ("px", "py"))
    return call(
        pick_body,
        shaped((DEV, 64, 128)),
        slots, returned.reshape(2 * DEV, 64, 128),
        scratch=(pltpu.VMEM((DEV, 64, 128), BF), pltpu.SemaphoreType.DMA((4,))),
        specs=[SM, VM],
        out_specs=HB,
        limit=24,
    )


def solution(mesh):
    return jax.shard_map(
        per_device,
        mesh=mesh,
        in_specs=(
            P(("px", "py"), None, None),
            P(("px", "py"), None, None),
            P(("px", "py")),
            P(("px", "py"), None),
            P(None, None, "px", "py", None, None),
            P(),
            P(),
        ),
        out_specs=P(("px", "py"), None, None),
        check_vma=False,
    )
```

```python
import functools
import math

import jax
import jax.numpy as jnp
import numpy as np
from jax import lax
from jax.experimental import pallas as pl
from jax.experimental.pallas import tpu as pltpu
from jax.sharding import PartitionSpec as P

CH = 64
MODES = 32
LAYERS = 2
DEV = 128
AMPLITUDE = 0.25
SPREAD = 4.5
DECODE_SCALE = 0.1
BF = jnp.bfloat16
F32 = jnp.float32
MIB = 1024 * 1024
EARLY = 40
NT = (((1,), (1,)), ((), ()))
UNIT = math.sqrt(math.log2(math.e) / SPREAD)


def halves(table):
    high = np.asarray(table, np.float32).astype(BF)
    low = (np.asarray(table, np.float64) - high.astype(np.float64)).astype(np.float32).astype(BF)
    return high, low


def waves():
    j = np.arange(MODES)
    return np.where(j < MODES // 2, j, j - MODES)


def turn(frequency, place):
    return 2.0 * math.pi / 128 * ((frequency * place) % 128)


def forward_pair(angle):
    c, s = np.cos(angle) / math.sqrt(128), np.sin(angle) / math.sqrt(128)
    return np.array([[c, s], [-s, c]])


def backward_pair(angle):
    c, s = np.cos(angle) / math.sqrt(128), np.sin(angle) / math.sqrt(128)
    return np.array([[c, -s], [s, c]])


@functools.lru_cache(None)
def tables():
    k = np.arange(MODES)
    z = np.arange(128)
    angle = turn(k[:, None], z[None, :])
    mz = np.stack([np.cos(angle), -np.sin(angle)], 1).reshape(64, 128) / math.sqrt(128)
    mz_high, mz_low = halves(mz)
    z_forward = np.concatenate([mz_high, mz_low], 0)
    weight = np.where(k == 0, 1.0, 2.0)[:, None, None]
    inv = np.stack([np.cos(angle), -np.sin(angle)], 1) / math.sqrt(128) * weight
    inv = inv.reshape(8, 8, 128)
    zi = np.zeros((2, 128, 8, 2, 8))
    for y2 in range(2):
        zi[y2, :, :, y2, :] = inv.transpose(2, 0, 1)
    z_back = np.concatenate(halves(zi.reshape(256, 128)), 1)
    f = waves()
    y = np.arange(128)
    pair = forward_pair(turn(f[:, None], y[None, :])).reshape(2, 2, 16, 2, 32, 4)
    ty = np.zeros((4, 16, 2, 2, 32, 4, 4, 2))
    for k4 in range(4):
        ty[k4, :, :, :, :, :, k4, :] = pair.transpose(2, 3, 0, 4, 5, 1)
    y_forward = np.concatenate(halves(ty.reshape(256, 1024)), 0)
    pair = backward_pair(turn(f[:, None], y[None, :])).reshape(2, 2, 16, 2, 32, 4)
    ti = np.zeros((32, 4, 4, 2, 4, 16, 2, 2))
    for k4 in range(4):
        ti[:, :, k4, :, k4, :, :, :] = pair.transpose(4, 5, 0, 2, 3, 1)
    y_back = np.concatenate(halves(ti.reshape(1024, 256)), 1)
    x = np.arange(128)
    pair = forward_pair(turn(f[:, None], x[None, :])).reshape(2, 2, 32, 16, 4, 2)
    tx = np.zeros((32, 2, 2, 16, 2, 4, 2, 2))
    for ky in range(2):
        tx[:, ky, :, :, :, :, ky, :] = pair.transpose(2, 0, 3, 5, 4, 1)
    x_forward = np.concatenate(halves(tx.reshape(128, 512)), 0)
    pair = backward_pair(turn(f[:, None], x[None, :])).reshape(2, 2, 32, 16, 4, 2)
    txi = np.zeros((16, 2, 4, 2, 2, 2, 32, 2))
    for ky in range(2):
        txi[:, :, :, ky, :, :, :, ky] = pair.transpose(3, 5, 4, 0, 1, 2)
    high, low = halves(txi.reshape(512, 128))
    x_back = np.concatenate([high, low, high], 1)
    order = np.arange(512).reshape(8, 16, 4).transpose(1, 0, 2).reshape(-1)
    to_send = np.eye(512)[order].astype(BF)
    from_send = np.ascontiguousarray(np.eye(512)[order].T).astype(BF)
    row = np.arange(512)
    repeat = np.eye(128)[(row // 8) * 2 + row % 2].astype(BF)
    return dict(
        z_forward=z_forward, z_back=z_back, y_forward=y_forward, y_back=y_back,
        x_forward=x_forward, x_back=x_back, to_send=to_send, from_send=from_send,
        repeat=repeat, eye=np.eye(256).astype(BF),
    )


def dot(a, b):
    return jnp.dot(a, b, preferred_element_type=F32)


def dot_nt(a, b):
    return lax.dot_general(a, b, NT, preferred_element_type=F32)


def call(
    body, out_shape, *args, scratch=(), specs=None, out_specs=None, limit=40, flops=None
):
    vm = pl.BlockSpec(memory_space=pltpu.VMEM)
    single = not isinstance(out_shape, (tuple, list))
    if specs is None:
        specs = [vm] * len(args)
    if out_specs is None:
        out_specs = vm if single else [vm] * len(out_shape)
    return pl.pallas_call(
        body,
        out_shape=out_shape,
        in_specs=specs,
        out_specs=out_specs,
        scratch_shapes=list(scratch),
        cost_estimate=flops and pl.CostEstimate(
            flops=flops, bytes_accessed=flops // 100, transcendentals=0
        ),
        compiler_params=pltpu.CompilerParams(vmem_limit_bytes=limit * MIB),
    )(*args)


VM = pl.BlockSpec(memory_space=pltpu.VMEM)
SM = pl.BlockSpec(memory_space=pltpu.SMEM)
HB = pl.BlockSpec(memory_space=pltpu.HBM)


def in_hbm(x):
    return pltpu.with_memory_space_constraint(x, pltpu.HBM)


def shaped(shape, dtype=BF):
    return jax.ShapeDtypeStruct(shape, dtype)


def pack_body(
    me, bricks_at, counts_at, values_at, offsets_at, send, slots,
    seen, aux, bricks, counts, offsets_in, offsets, values, sems,
):
    loads = [
        pltpu.make_async_copy(
            values_at.at[pl.ds(32 * i, 32)], values.at[pl.ds(32 * i, 32)], sems.at[i]
        )
        for i in range(4)
    ]
    for load in loads:
        load.start()
    small = [
        pltpu.make_async_copy(source, target, sems.at[4 + i])
        for i, (source, target) in enumerate(
            [(bricks_at, bricks), (counts_at, counts), (offsets_at, offsets_in)]
        )
    ]
    for load in small:
        load.start()
    slots[DEV] = me[0]

    def clear(d, _):
        send[d] = jnp.zeros((136, 128), BF)
        aux[d] = jnp.zeros((8, 128), F32)
        seen[d] = 0
        return 0

    lax.fori_loop(0, DEV, clear, 0, unroll=4)
    lane = lax.broadcasted_iota(jnp.int32, (1, 128), 1)
    for load in small:
        load.wait()
    offsets[...] = offsets_in[...].astype(F32)
    for load in loads:
        load.wait()

    def one(b, _):
        head = bricks[0, b]
        owner = head >> 7
        rank = seen[owner]
        seen[owner] = rank + 1
        slots[b] = owner * 2 + rank

        send[owner, pl.ds(pl.multiple_of(rank * 64, 64), 64), :] = values[b]
        meta = jnp.where(lane == 0, counts[b], 0)
        for h in range(4):
            meta = jnp.where(lane == 1 + h, bricks[h, b] & 127, meta)
        rows = [offsets[k, pl.ds(b, 1), :] for k in range(3)] + [meta.astype(F32)]
        aux[owner, pl.ds(pl.multiple_of(4 * rank, 4), 4), :] = jnp.concatenate(rows, 0)
        return 0

    lax.fori_loop(0, DEV, one, 0, unroll=8)

    def finish(d, _):
        send[d, 128:136, :] = aux[d].astype(BF)
        return 0

    lax.fori_loop(0, DEV, finish, 0, unroll=4)


def pack(me, values, offsets, counts, bricks):
    return call(
        pack_body,
        (shaped((DEV, 136, 128)), shaped((DEV + 8,), jnp.int32)),
        me, in_hbm(bricks.T), in_hbm(counts), in_hbm(values), in_hbm(offsets.transpose(1, 0, 2)),
        scratch=(
            pltpu.SMEM((DEV,), jnp.int32),
            pltpu.VMEM((DEV, 8, 128), F32),
            pltpu.SMEM((4, DEV), jnp.int32),
            pltpu.SMEM((DEV,), jnp.int32),
            pltpu.VMEM((3, 128, 128), BF),
            pltpu.VMEM((3, 128, 128), F32),
            pltpu.VMEM((DEV, 64, 128), BF),
            pltpu.SemaphoreType.DMA((7,)),
        ),
        specs=[SM, HB, HB, HB, HB],
        out_specs=[VM, SM],
        limit=24,
    )


def spread_weights(place, count, ids):
    lane = lax.broadcasted_iota(jnp.int32, (1, 128), 1)
    sub = lax.broadcasted_iota(jnp.int32, (8, 128), 0)
    xs = ((sub // 4).astype(F32) + 0.5) * UNIT
    ys = ((sub % 4).astype(F32) + 0.5) * UNIT
    zs = (lax.broadcasted_iota(jnp.int32, (16, 128), 0).astype(F32) + 0.5) * UNIT
    place = place * UNIT
    px = jnp.where(lane < count, place[0:1], 1.0e4) - xs
    py = place[1:2] - ys
    pz = place[2:3] - zs
    grid_at = [(i >> 5, (i >> 3) & 3, i & 7) for i in ids]
    parts = []
    for h in range(4):
        shift = [(a - b).astype(F32) for a, b in zip(grid_at[h], grid_at[0])]
        dx = px - shift[0] * (2 * UNIT)
        dy = py - shift[1] * (4 * UNIT)
        dz = pz - shift[2] * (16 * UNIT)
        xy = jnp.exp2(math.log2(AMPLITUDE) - dx * dx - dy * dy)
        zz = jnp.exp2(-(dz * dz))
        for i in range(8):
            parts.append((xy[i : i + 1] * zz).astype(BF))
    return jnp.concatenate(parts, 0)


def to_relative(slots, chunks, sends):
    for j in range(8):
        sends[j][...] = chunks[(slots[DEV] + j) & 7]


def from_relative(slots, gots, chunks):
    for j in range(8):
        chunks[(slots[DEV] - j) & 7] = gots[j][...]


def third_forward(by, grid_at, table, out):
    for j in range(4):
        modes = []
        for half in range(2):
            both = dot(table, grid_at(2 * j + half))
            modes.append(both[:64] + both[64:])
        for kg in range(8):
            piece = jnp.concatenate([m[8 * kg : 8 * kg + 8] for m in modes], 0)
            at = by * 64 + j * 16
            out[kg, at : at + 16, :] = piece.astype(BF)


def block_weights(rank, d, meta, rows):
    ids = [meta[8 * rank + 1 + h, d] for h in range(4)]
    return ids, spread_weights(rows[4 * rank : 4 * rank + 3], meta[8 * rank, d], ids)


def spread_one(rank, d, meta, rows, block, acc):
    ids, weights = block_weights(rank, d, meta, rows)
    tile = dot_nt(block, weights)
    for h in range(4):
        acc[ids[h]] = acc[ids[h]] + tile[:, 128 * h : 128 * h + 128]


def quarter(source, target, sems, i):
    return pltpu.make_async_copy(
        source.at[pl.ds(32 * i, 32)], target.at[pl.ds(32 * i, 32)], sems.at[i]
    )


def encode_body(slots, got_at, eye, z_table, weights_at, grid_at, aux, meta_out, weights, *rest):
    *sends, modes, grid, acc, got, wide, meta, got_sems, grid_sems, sems = rest
    first = pltpu.make_async_copy(got_at.at[:, pl.ds(128, 8), :], aux, sems.at[0])
    first.start()
    for i in range(4):
        quarter(got_at, got, got_sems, i).start()
    fetch = pltpu.make_async_copy(weights_at.at[pl.ds(0, 64)], weights, sems.at[1])
    fetch.start()
    first.wait()
    wide[...] = aux[...].astype(F32).reshape(8 * DEV, 128)
    for rank in range(2):
        numbers = wide[pl.ds(4 * rank + 3, DEV, stride=8), :].T
        meta_out[8 * rank : 8 * rank + 8, :] = numbers[0:8].astype(jnp.int32)
    to_scalar = pltpu.make_async_copy(meta_out, meta, sems.at[2])
    to_scalar.start()

    def clear(b, _):
        acc[b] = jnp.zeros((64, 128), F32)
        return 0

    lax.fori_loop(0, 128, clear, 0, unroll=4)

    to_scalar.wait()

    def part(i, _):
        quarter(got_at, got, got_sems, i).wait()

        def one(k, _):
            d = 32 * i + k
            rows = aux[d].astype(F32)
            for rank in range(2):
                spread_one(rank, d, meta, rows, got[d, 64 * rank : 64 * rank + 64, :], acc)
            return 0

        return lax.fori_loop(0, 32, one, 0, unroll=16)

    lax.fori_loop(0, 4, part, 0)
    eye128 = eye[0:128, 0:128]
    stores = []
    for by in range(4):
        for bz in range(8):
            bricks = jnp.concatenate([acc[(bx * 4 + by) * 8 + bz] for bx in range(4)], 0)
            cells = dot_nt(eye128, bricks.astype(BF)).astype(BF)
            for xy in range(8):
                grid[by, xy, 16 * bz : 16 * bz + 16, :] = cells[16 * xy : 16 * xy + 16]
        stores.append(pltpu.make_async_copy(grid.at[by], grid_at.at[by], grid_sems.at[by]))
        stores[-1].start()
        third_forward(by, lambda xy: grid[by, xy], z_table[...], modes)
    to_relative(slots, modes, sends)
    for store in stores:
        store.wait()
    fetch.wait()


def encode(slots, got, weights, t):
    out = call(
        encode_body,
        [
            pltpu.HBM((4, 8, 128, 256), BF),
            shaped((DEV, 8, 128)),
            shaped((16, DEV), jnp.int32),
            shaped((64, 256, 128)),
        ]
        + [shaped((256, 256))] * 8,
        slots, in_hbm(got), t["eye"], t["z_forward"], weights,
        scratch=(
            pltpu.VMEM((8, 256, 256), BF),
            pltpu.VMEM((4, 8, 128, 256), BF),
            pltpu.VMEM((128, 64, 128), F32),
            pltpu.VMEM((DEV, 136, 128), BF),
            pltpu.VMEM((8 * DEV, 128), F32),
            pltpu.SMEM((16, DEV), jnp.int32),
            pltpu.SemaphoreType.DMA((4,)),
            pltpu.SemaphoreType.DMA((4,)),
            pltpu.SemaphoreType.DMA((3,)),
        ),
        specs=[SM, HB, VM, VM, HB],
        out_specs=[HB] + [VM] * 11,
        limit=24,
    )
    return in_hbm(out[0]), out[1], out[2], out[3], out[4:]


def second_body(me, token, *refs):
    *gots, table, order, send, got = refs
    from_relative(me, gots, got)
    rows = []
    for x2 in range(2):
        data = jnp.concatenate(
            [
                got[py, by * 64 + x2 * 32 : by * 64 + x2 * 32 + 32, :]
                for py in range(8)
                for by in range(4)
            ],
            0,
        )
        both = dot(table[...], data)
        out = both[:256] + both[256:]
        for bx in range(4):
            rows.append(
                jnp.concatenate(
                    [out[64 * k : 64 * k + 64, 64 * bx : 64 * bx + 64] for k in range(4)], 1
                ).astype(BF)
            )
    send[...] = dot(order[...], jnp.concatenate(rows, 0)).astype(BF)


def mix_body(got, weights, forward, back, repeat, send, product):
    both = dot(forward[...], got[...])
    modes = (both[:128] + both[128:]).astype(BF)
    spread = dot(repeat[...], modes)
    row = lax.broadcasted_iota(jnp.int32, (512, 256), 0)
    col = lax.broadcasted_iota(jnp.int32, (512, 256), 1)
    spread = jnp.where(col // 64 == (row % 8) // 2, spread, 0.0)
    for m in range(64):
        product[8 * m : 8 * m + 8, :] = dot(spread[8 * m : 8 * m + 8].astype(BF), weights[m])
    real, imag = [], []
    for kz in range(4):
        from_real = product[pl.ds(2 * kz, 64, stride=8), :]
        from_imag = product[pl.ds(2 * kz + 1, 64, stride=8), :]
        real.append(from_real[:, :64] - from_imag[:, 64:])
        imag.append(from_real[:, 64:] + from_imag[:, :64])
    mixed = jnp.concatenate([jnp.concatenate(real, 1), jnp.concatenate(imag, 1)], 0)
    high = mixed.astype(BF)
    low = (mixed - high.astype(F32)).astype(BF)
    send[...] = dot(back[...], jnp.concatenate([high, high, low], 0)).astype(BF)


def second_back_body(me, got, table, order, *rest):
    *sends, send = rest
    ordered = dot(order[...], got[...])
    for x2 in range(2):
        parts = []
        for k in range(4):
            parts.append(
                jnp.concatenate(
                    [
                        ordered[
                            (x2 * 4 + bx) * 64 : (x2 * 4 + bx) * 64 + 64, 64 * k : 64 * k + 64
                        ]
                        for bx in range(4)
                    ],
                    1,
                ).astype(BF)
            )
        data = jnp.concatenate(parts, 0)
        out = dot(table[...], jnp.concatenate([data, data], 0)).astype(BF)
        for py in range(8):
            for by in range(4):
                at = py * 128 + by * 32
                send[py, by * 64 + x2 * 32 : by * 64 + x2 * 32 + 32, :] = out[at : at + 32]
    to_relative(me, send, sends)


def layer_values(by, j, got, skipped, z_back):
    at = by * 64 + j * 16
    data = jnp.concatenate([got[kg, at : at + 16, :] for kg in range(8)], 0)
    total = dot(z_back, jnp.concatenate([data, data], 0))
    total = total + skipped[by, 2 * j : 2 * j + 2].reshape(256, 256)
    result = 0.5 * total * (1.0 + lax.erf(total * math.sqrt(0.5)))
    return result.astype(BF)


def load_grid(grid_at, grid, sems):
    copies = [
        pltpu.make_async_copy(grid_at.at[by], grid.at[by], sems.at[by]) for by in range(4)
    ]
    for copy in copies:
        copy.start()
    return copies


def four_fold(layer, skip, bias):
    wide = jnp.concatenate([skip[layer].astype(F32)] * 4, 1)
    tall = jnp.concatenate([wide] * 4, 0)
    row = lax.broadcasted_iota(jnp.int32, (256, 256), 0)
    col = lax.broadcasted_iota(jnp.int32, (256, 256), 1)
    matrix = jnp.where(row // 64 == col // 64, tall, 0.0).astype(BF)
    return matrix, jnp.concatenate([bias[layer : layer + 1, :]] * 4, 1)


def skip_body(layer, anchor, grid_at, skip, bias, out, grid, sems):
    copies = load_grid(grid_at, grid, sems)
    skip, bias = four_fold(layer, skip, bias)
    for by in range(4):
        copies[by].wait()
        product = dot(grid[by].reshape(1024, 256), skip) + bias
        out[by] = product.reshape(8, 128, 256)


def inner_layer_body(layer, me, *refs):
    *gots, skipped, z_back, z_table, weights_at, new_grid_at, weights = refs[:14]
    *sends, got, new_grid, modes, out_sems, sem = refs[14:]
    fetch = pltpu.make_async_copy(weights_at.at[pl.ds(layer * 64 + 64, 64)], weights, sem)
    fetch.start()
    from_relative(me, gots, got)
    stores = []
    for by in range(4):
        for j in range(4):
            values = layer_values(by, j, got, skipped, z_back[...])
            new_grid[by, 2 * j] = values[:128]
            new_grid[by, 2 * j + 1] = values[128:]
        stores.append(
            pltpu.make_async_copy(new_grid.at[by], new_grid_at.at[by], out_sems.at[by])
        )
        stores[-1].start()
        third_forward(by, lambda xy: new_grid[by, xy], z_table[...], modes)
    to_relative(me, modes, sends)
    for store in stores:
        store.wait()
    fetch.wait()


def last_layer_body(me, *refs):
    *gots, skipped, z_back, eye, bricks, got = refs
    from_relative(me, gots, got)
    for by in range(4):
        values = [
            layer_values(by, j, got, skipped, z_back[...]) for j in range(4)
        ]
        for bz in range(8):
            cells = jnp.concatenate(
                [
                    values[xy // 2][(xy % 2) * 128 + 16 * bz : (xy % 2) * 128 + 16 * bz + 16]
                    for xy in range(8)
                ],
                0,
            )
            turned = dot_nt(eye[...], cells).astype(BF)
            for bx in range(4):
                bricks[(bx * 4 + by) * 8 + bz] = turned[64 * bx : 64 * bx + 64]


def early_body(start, meta, aux, anchor, out, token):
    def one(k, _):
        d = start + 8 * pl.program_id(0) + k
        rows = aux[d].astype(F32)
        for rank in range(2):
            out[2 * k + rank] = block_weights(rank, d, meta, rows)[1]
        return 0

    lax.fori_loop(0, 8, one, 0, unroll=8)
    token[...] = jnp.zeros((8, 128), F32)


def early_weights(start, count, meta, aux, anchor):
    whole = pl.BlockSpec(memory_space=pltpu.VMEM)
    weights, token = pl.pallas_call(
        functools.partial(early_body, start),
        grid=(count // 8,),
        out_shape=[pltpu.HBM((2 * count, 512, 128), BF), shaped((8, 128), F32)],
        in_specs=[SM, whole, whole],
        out_specs=[pl.BlockSpec((16, 512, 128), lambda i: (i, 0, 0)), whole],
        compiler_params=pltpu.CompilerParams(vmem_limit_bytes=16 * MIB),
        cost_estimate=pl.CostEstimate(
            flops=count * 10**7, bytes_accessed=count * 2**18, transcendentals=0
        ),
    )(meta, aux, anchor)
    return in_hbm(weights), token


def decode_body(meta, aux, bricks, *refs):
    *stored_at, reply, stored, sems = refs
    loads = []
    for w in range(2):
        for i in range(EARLY // 8):
            loads.append(
                pltpu.make_async_copy(
                    stored_at[w].at[pl.ds(16 * i, 16)],
                    stored.at[pl.ds(2 * EARLY * w + 16 * i, 16)],
                    sems.at[len(loads)],
                )
            )
            loads[-1].start()

    def write(d, near, weights):
        both = DECODE_SCALE * dot(jnp.concatenate(near, 0), jnp.concatenate(weights, 1))
        reply[d, 0:64, :] = both[:64, :128].astype(BF)
        reply[d, 64:128, :] = both[64:, 128:].astype(BF)

    def fresh(k, _):
        d = 2 * EARLY + k
        rows = aux[d].astype(F32)
        near, weights = [], []
        for rank in range(2):
            ids, kernel = block_weights(rank, d, meta, rows)
            weights.append(kernel)
            near.append(jnp.concatenate([bricks[i] for i in ids], 1))
        write(d, near, weights)
        return 0

    lax.fori_loop(0, DEV - 2 * EARLY, fresh, 0, unroll=16)
    for load in loads:
        load.wait()

    def early(d, _):
        near = []
        for rank in range(2):
            ids = [meta[8 * rank + 1 + h, d] for h in range(4)]
            near.append(jnp.concatenate([bricks[i] for i in ids], 1))
        write(d, near, [stored[2 * d], stored[2 * d + 1]])
        return 0

    lax.fori_loop(0, 2 * EARLY, early, 0, unroll=16)


def pick_body(slots, got, out_at, out, sems):
    def part(i, _):
        def one(k, _):
            b = 32 * i + k
            out[b] = got[slots[b]]
            return 0

        lax.fori_loop(0, 32, one, 0, unroll=8)
        quarter(out, out_at, sems, i).start()
        return 0

    lax.fori_loop(0, 4, part, 0)
    for i in range(4):
        quarter(out, out_at, sems, i).wait()


def exchange(x, axis):
    return lax.all_to_all(x, axis, split_axis=0, concat_axis=0, tiled=True)


def exchange_lines(chunks):
    got = [chunks[0]]
    for j in range(1, 8):
        got.append(lax.ppermute(chunks[j], "py", [(i, (i + j) % 8) for i in range(8)]))
    return got


def per_device(values, offsets, counts, bricks, spectral_weights, skip_weights, skip_bias):
    t = {name: jnp.asarray(table) for name, table in tables().items()}
    me = lax.axis_index("py").astype(jnp.int32).reshape(1)
    weights = in_hbm(spectral_weights.reshape(LAYERS * 64, 256, 128))
    send, slots = pack(me, values, offsets, counts, bricks)
    got = exchange(send, ("px", "py"))
    grid, aux, meta, kept, modes = encode(slots, got, weights, t)
    chunks = pltpu.VMEM((8, 256, 256), BF)
    grid_scratch = pltpu.VMEM((4, 8, 128, 256), BF)
    four = pltpu.SemaphoreType.DMA((4,))
    piece = shaped((256, 256))
    stored = []
    for layer in range(LAYERS):
        kernel, token = early_weights(EARLY * layer, EARLY, meta, aux, modes[0])
        stored.append(kernel)
        columns = exchange_lines(modes)
        second = call(
            second_body,
            shaped((512, 256)),
            slots, token, *columns, t["y_forward"], t["to_send"],
            scratch=(chunks,),
            specs=[SM] + [VM] * 11,
            limit=24,
        )
        lines = exchange(second.reshape(16, 32, 256), "px").reshape(512, 256)
        back = call(
            mix_body,
            shaped((512, 256)),
            lines, kept, t["x_forward"], t["x_back"], t["repeat"],
            scratch=(pltpu.VMEM((512, 128), F32),),
            limit=24,
        )
        lines = exchange(back.reshape(16, 32, 256), "px").reshape(512, 256)
        columns = call(
            second_back_body,
            [piece] * 8,
            slots, lines, t["y_back"], t["from_send"],
            scratch=(chunks,),
            specs=[SM, VM, VM, VM],
            limit=24,
        )
        skipped = call(
            functools.partial(skip_body, layer),
            shaped((4, 8, 128, 256), F32),
            columns[0], grid, skip_weights, skip_bias,
            scratch=(grid_scratch, four),
            specs=[VM, HB, VM, VM],
            limit=24,
            flops=2 * 4096 * 256 * 256,
        )
        columns = exchange_lines(columns)
        if layer + 1 < LAYERS:
            grid, kept, *modes = call(
                functools.partial(inner_layer_body, layer),
                [pltpu.HBM((4, 8, 128, 256), BF), shaped((64, 256, 128))] + [piece] * 8,
                slots, *columns, skipped, t["z_back"], t["z_forward"],
                weights,
                scratch=(
                    chunks, grid_scratch, chunks, four,
                    pltpu.SemaphoreType.DMA,
                ),
                specs=[SM] + [VM] * 11 + [HB],
                out_specs=[HB] + [VM] * 9,
                limit=32,
            )
            grid = in_hbm(grid)
        else:
            final = call(
                last_layer_body,
                shaped((128, 64, 128)),
                slots, *columns, skipped, t["z_back"], t["eye"],
                scratch=(chunks,),
                specs=[SM] + [VM] * 11,
                limit=32,
            )
    reply = call(
        decode_body,
        shaped((DEV, 128, 128)),
        meta, aux, final, *stored,
        scratch=(
            pltpu.VMEM((4 * EARLY, 512, 128), BF),
            pltpu.SemaphoreType.DMA((EARLY // 4,)),
        ),
        specs=[SM, VM, VM, HB, HB],
        limit=40,
    )
    returned = exchange(reply, ("px", "py"))
    return call(
        pick_body,
        shaped((DEV, 64, 128)),
        slots, returned.reshape(2 * DEV, 64, 128),
        scratch=(pltpu.VMEM((DEV, 64, 128), BF), pltpu.SemaphoreType.DMA((4,))),
        specs=[SM, VM],
        out_specs=HB,
        limit=24,
    )


def solution(mesh):
    return jax.shard_map(
        per_device,
        mesh=mesh,
        in_specs=(
            P(("px", "py"), None, None),
            P(("px", "py"), None, None),
            P(("px", "py")),
            P(("px", "py"), None),
            P(None, None, "px", "py", None, None),
            P(),
            P(),
        ),
        out_specs=P(("px", "py"), None, None),
        check_vma=False,
    )
```

```python
import functools
import math

import jax
import jax.numpy as jnp
import numpy as np
from jax import lax
from jax.experimental import pallas as pl
from jax.experimental.pallas import tpu as pltpu
from jax.sharding import PartitionSpec as P

CH = 64
MODES = 32
LAYERS = 2
DEV = 128
AMPLITUDE = 0.25
SPREAD = 4.5
DECODE_SCALE = 0.1
BF = jnp.bfloat16
F32 = jnp.float32
MIB = 1024 * 1024
EARLY = 24
NT = (((1,), (1,)), ((), ()))
UNIT = math.sqrt(math.log2(math.e) / SPREAD)


def halves(table):
    high = np.asarray(table, np.float32).astype(BF)
    low = (np.asarray(table, np.float64) - high.astype(np.float64)).astype(np.float32).astype(BF)
    return high, low


def waves():
    j = np.arange(MODES)
    return np.where(j < MODES // 2, j, j - MODES)


def turn(frequency, place):
    return 2.0 * math.pi / 128 * ((frequency * place) % 128)


def forward_pair(angle):
    c, s = np.cos(angle) / math.sqrt(128), np.sin(angle) / math.sqrt(128)
    return np.array([[c, s], [-s, c]])


def backward_pair(angle):
    c, s = np.cos(angle) / math.sqrt(128), np.sin(angle) / math.sqrt(128)
    return np.array([[c, -s], [s, c]])


@functools.lru_cache(None)
def tables():
    k = np.arange(MODES)
    z = np.arange(128)
    angle = turn(k[:, None], z[None, :])
    mz = np.stack([np.cos(angle), -np.sin(angle)], 1).reshape(64, 128) / math.sqrt(128)
    mz_high, mz_low = halves(mz)
    z_forward = np.concatenate([mz_high, mz_low], 0)
    weight = np.where(k == 0, 1.0, 2.0)[:, None, None]
    inv = np.stack([np.cos(angle), -np.sin(angle)], 1) / math.sqrt(128) * weight
    inv = inv.reshape(8, 8, 128)
    zi = np.zeros((2, 128, 8, 2, 8))
    for y2 in range(2):
        zi[y2, :, :, y2, :] = inv.transpose(2, 0, 1)
    z_back = np.concatenate(halves(zi.reshape(256, 128)), 1)
    f = waves()
    y = np.arange(128)
    pair = forward_pair(turn(f[:, None], y[None, :])).reshape(2, 2, 16, 2, 32, 4)
    ty = np.zeros((4, 16, 2, 2, 32, 4, 4, 2))
    for k4 in range(4):
        ty[k4, :, :, :, :, :, k4, :] = pair.transpose(2, 3, 0, 4, 5, 1)
    y_forward = halves(ty.reshape(256, 1024))[0]
    pair = backward_pair(turn(f[:, None], y[None, :])).reshape(2, 2, 16, 2, 32, 4)
    ti = np.zeros((32, 4, 4, 2, 4, 16, 2, 2))
    for k4 in range(4):
        ti[:, :, k4, :, k4, :, :, :] = pair.transpose(4, 5, 0, 2, 3, 1)
    y_back = halves(ti.reshape(1024, 256))[0]
    x = np.arange(128)
    pair = forward_pair(turn(f[:, None], x[None, :])).reshape(2, 2, 32, 16, 4, 2)
    tx = np.zeros((32, 2, 2, 16, 2, 4, 2, 2))
    for ky in range(2):
        tx[:, ky, :, :, :, :, ky, :] = pair.transpose(2, 0, 3, 5, 4, 1)
    x_forward = np.concatenate(halves(tx.reshape(128, 512)), 0)
    pair = backward_pair(turn(f[:, None], x[None, :])).reshape(2, 2, 32, 16, 4, 2)
    txi = np.zeros((16, 2, 4, 2, 2, 2, 32, 2))
    for ky in range(2):
        txi[:, :, :, ky, :, :, :, ky] = pair.transpose(3, 5, 4, 0, 1, 2)
    high, low = halves(txi.reshape(512, 128))
    x_back = np.concatenate([high, low, high], 1)
    order = np.arange(512).reshape(8, 16, 4).transpose(1, 0, 2).reshape(-1)
    to_send = np.eye(512)[order].astype(BF)
    from_send = np.ascontiguousarray(np.eye(512)[order].T).astype(BF)
    row = np.arange(512)
    repeat = np.eye(128)[(row // 8) * 2 + row % 2].astype(BF)
    return dict(
        z_forward=z_forward, z_back=z_back, y_forward=y_forward, y_back=y_back,
        x_forward=x_forward, x_back=x_back, to_send=to_send, from_send=from_send,
        repeat=repeat, eye=np.eye(256).astype(BF),
    )


def dot(a, b):
    return jnp.dot(a, b, preferred_element_type=F32)


def dot_nt(a, b):
    return lax.dot_general(a, b, NT, preferred_element_type=F32)


def call(
    body, out_shape, *args, scratch=(), specs=None, out_specs=None, limit=40, flops=None
):
    vm = pl.BlockSpec(memory_space=pltpu.VMEM)
    single = not isinstance(out_shape, (tuple, list))
    if specs is None:
        specs = [vm] * len(args)
    if out_specs is None:
        out_specs = vm if single else [vm] * len(out_shape)
    return pl.pallas_call(
        body,
        out_shape=out_shape,
        in_specs=specs,
        out_specs=out_specs,
        scratch_shapes=list(scratch),
        cost_estimate=flops and pl.CostEstimate(
            flops=flops, bytes_accessed=flops // 100, transcendentals=0
        ),
        compiler_params=pltpu.CompilerParams(vmem_limit_bytes=limit * MIB),
    )(*args)


VM = pl.BlockSpec(memory_space=pltpu.VMEM)
SM = pl.BlockSpec(memory_space=pltpu.SMEM)
HB = pl.BlockSpec(memory_space=pltpu.HBM)


def in_hbm(x):
    return pltpu.with_memory_space_constraint(x, pltpu.HBM)


def shaped(shape, dtype=BF):
    return jax.ShapeDtypeStruct(shape, dtype)


def pack_body(
    me, bricks_at, counts_at, values_at, offsets_at, send, slots,
    seen, aux, bricks, counts, offsets_in, offsets, values, sems,
):
    loads = [
        pltpu.make_async_copy(
            values_at.at[pl.ds(32 * i, 32)], values.at[pl.ds(32 * i, 32)], sems.at[i]
        )
        for i in range(4)
    ]
    for load in loads:
        load.start()
    small = [
        pltpu.make_async_copy(source, target, sems.at[4 + i])
        for i, (source, target) in enumerate(
            [(bricks_at, bricks), (counts_at, counts), (offsets_at, offsets_in)]
        )
    ]
    for load in small:
        load.start()
    slots[DEV] = me[0]

    def clear(d, _):
        send[d] = jnp.zeros((136, 128), BF)
        aux[d] = jnp.zeros((8, 128), F32)
        seen[d] = 0
        return 0

    lax.fori_loop(0, DEV, clear, 0, unroll=4)
    lane = lax.broadcasted_iota(jnp.int32, (1, 128), 1)
    for load in small:
        load.wait()
    offsets[...] = offsets_in[...].astype(F32)
    for load in loads:
        load.wait()

    def one(b, _):
        head = bricks[0, b]
        owner = head >> 7
        rank = seen[owner]
        seen[owner] = rank + 1
        slots[b] = owner * 2 + rank

        send[owner, pl.ds(pl.multiple_of(rank * 64, 64), 64), :] = values[b]
        meta = jnp.where(lane == 0, counts[b], 0)
        for h in range(4):
            meta = jnp.where(lane == 1 + h, bricks[h, b] & 127, meta)
        rows = [offsets[k, pl.ds(b, 1), :] for k in range(3)] + [meta.astype(F32)]
        aux[owner, pl.ds(pl.multiple_of(4 * rank, 4), 4), :] = jnp.concatenate(rows, 0)
        return 0

    lax.fori_loop(0, DEV, one, 0, unroll=8)

    def finish(d, _):
        send[d, 128:136, :] = aux[d].astype(BF)
        return 0

    lax.fori_loop(0, DEV, finish, 0, unroll=4)


def pack(me, values, offsets, counts, bricks):
    return call(
        pack_body,
        (shaped((DEV, 136, 128)), shaped((DEV + 8,), jnp.int32)),
        me, in_hbm(bricks.T), in_hbm(counts), in_hbm(values), in_hbm(offsets.transpose(1, 0, 2)),
        scratch=(
            pltpu.SMEM((DEV,), jnp.int32),
            pltpu.VMEM((DEV, 8, 128), F32),
            pltpu.SMEM((4, DEV), jnp.int32),
            pltpu.SMEM((DEV,), jnp.int32),
            pltpu.VMEM((3, 128, 128), BF),
            pltpu.VMEM((3, 128, 128), F32),
            pltpu.VMEM((DEV, 64, 128), BF),
            pltpu.SemaphoreType.DMA((7,)),
        ),
        specs=[SM, HB, HB, HB, HB],
        out_specs=[VM, SM],
        limit=24,
    )


def spread_weights(place, count, ids):
    lane = lax.broadcasted_iota(jnp.int32, (1, 128), 1)
    sub = lax.broadcasted_iota(jnp.int32, (8, 128), 0)
    xs = ((sub // 4).astype(F32) + 0.5) * UNIT
    ys = ((sub % 4).astype(F32) + 0.5) * UNIT
    zs = (lax.broadcasted_iota(jnp.int32, (16, 128), 0).astype(F32) + 0.5) * UNIT
    place = place * UNIT
    px = jnp.where(lane < count, place[0:1], 1.0e4) - xs
    py = place[1:2] - ys
    pz = place[2:3] - zs
    grid_at = [(i >> 5, (i >> 3) & 3, i & 7) for i in ids]
    parts = []
    for h in range(4):
        shift = [(a - b).astype(F32) for a, b in zip(grid_at[h], grid_at[0])]
        dx = px - shift[0] * (2 * UNIT)
        dy = py - shift[1] * (4 * UNIT)
        dz = pz - shift[2] * (16 * UNIT)
        xy = jnp.exp2(math.log2(AMPLITUDE) - dx * dx - dy * dy)
        zz = jnp.exp2(-(dz * dz))
        for i in range(8):
            parts.append((xy[i : i + 1] * zz).astype(BF))
    return jnp.concatenate(parts, 0)


def to_relative(slots, chunks, sends):
    for j in range(8):
        sends[j][...] = chunks[(slots[DEV] + j) & 7]


def from_relative(slots, gots, chunks):
    for j in range(8):
        chunks[(slots[DEV] - j) & 7] = gots[j][...]


def third_forward(by, grid_at, table, out):
    for j in range(4):
        modes = []
        for half in range(2):
            both = dot(table, grid_at(2 * j + half))
            modes.append(both[:64] + both[64:])
        for kg in range(8):
            piece = jnp.concatenate([m[8 * kg : 8 * kg + 8] for m in modes], 0)
            at = by * 64 + j * 16
            out[kg, at : at + 16, :] = piece.astype(BF)


def block_weights(rank, d, meta, rows):
    ids = [meta[8 * rank + 1 + h, d] for h in range(4)]
    return ids, spread_weights(rows[4 * rank : 4 * rank + 3], meta[8 * rank, d], ids)


def spread_one(rank, d, meta, rows, block, acc):
    ids, weights = block_weights(rank, d, meta, rows)
    tile = dot_nt(block, weights)
    for h in range(4):
        acc[ids[h]] = acc[ids[h]] + tile[:, 128 * h : 128 * h + 128]


def quarter(source, target, sems, i):
    return pltpu.make_async_copy(
        source.at[pl.ds(32 * i, 32)], target.at[pl.ds(32 * i, 32)], sems.at[i]
    )


def encode_body(slots, got_at, eye, z_table, weights_at, grid_at, aux, meta_out, weights, *rest):
    *sends, modes, grid, acc, got, wide, meta, got_sems, grid_sems, sems = rest
    first = pltpu.make_async_copy(got_at.at[:, pl.ds(128, 8), :], aux, sems.at[0])
    first.start()
    for i in range(4):
        quarter(got_at, got, got_sems, i).start()
    fetch = pltpu.make_async_copy(weights_at.at[pl.ds(0, 64)], weights, sems.at[1])
    fetch.start()

    def clear(b, _):
        acc[b] = jnp.zeros((64, 128), F32)
        return 0

    lax.fori_loop(0, 128, clear, 0, unroll=4)
    first.wait()
    wide[...] = aux[...].astype(F32).reshape(8 * DEV, 128)
    for rank in range(2):
        numbers = wide[pl.ds(4 * rank + 3, DEV, stride=8), :].T
        meta_out[8 * rank : 8 * rank + 8, :] = numbers[0:8].astype(jnp.int32)
    to_scalar = pltpu.make_async_copy(meta_out, meta, sems.at[2])
    to_scalar.start()


    to_scalar.wait()

    def part(i, _):
        quarter(got_at, got, got_sems, i).wait()

        def one(k, _):
            d = 32 * i + k
            rows = aux[d].astype(F32)
            for rank in range(2):
                spread_one(rank, d, meta, rows, got[d, 64 * rank : 64 * rank + 64, :], acc)
            return 0

        return lax.fori_loop(0, 32, one, 0, unroll=16)

    lax.fori_loop(0, 4, part, 0)
    eye128 = eye[0:128, 0:128]
    stores = []
    for by in range(4):
        for bz in range(8):
            bricks = jnp.concatenate([acc[(bx * 4 + by) * 8 + bz] for bx in range(4)], 0)
            cells = dot_nt(eye128, bricks.astype(BF)).astype(BF)
            for xy in range(8):
                grid[by, xy, 16 * bz : 16 * bz + 16, :] = cells[16 * xy : 16 * xy + 16]
        stores.append(pltpu.make_async_copy(grid.at[by], grid_at.at[by], grid_sems.at[by]))
        stores[-1].start()
        third_forward(by, lambda xy: grid[by, xy], z_table[...], modes)
    to_relative(slots, modes, sends)
    for store in stores:
        store.wait()
    fetch.wait()


def encode(slots, got, weights, t):
    out = call(
        encode_body,
        [
            pltpu.HBM((4, 8, 128, 256), BF),
            shaped((DEV, 8, 128)),
            shaped((16, DEV), jnp.int32),
            shaped((64, 256, 128)),
        ]
        + [shaped((256, 256))] * 8,
        slots, in_hbm(got), t["eye"], t["z_forward"], weights,
        scratch=(
            pltpu.VMEM((8, 256, 256), BF),
            pltpu.VMEM((4, 8, 128, 256), BF),
            pltpu.VMEM((128, 64, 128), F32),
            pltpu.VMEM((DEV, 136, 128), BF),
            pltpu.VMEM((8 * DEV, 128), F32),
            pltpu.SMEM((16, DEV), jnp.int32),
            pltpu.SemaphoreType.DMA((4,)),
            pltpu.SemaphoreType.DMA((4,)),
            pltpu.SemaphoreType.DMA((3,)),
        ),
        specs=[SM, HB, VM, VM, HB],
        out_specs=[HB] + [VM] * 11,
        limit=24,
    )
    return in_hbm(out[0]), out[1], out[2], out[3], out[4:]


def second_body(me, token, *refs):
    *gots, table, order, send, got = refs
    from_relative(me, gots, got)
    rows = []
    for x2 in range(2):
        data = jnp.concatenate(
            [
                got[py, by * 64 + x2 * 32 : by * 64 + x2 * 32 + 32, :]
                for py in range(8)
                for by in range(4)
            ],
            0,
        )
        out = dot(table[...], data)
        for bx in range(4):
            rows.append(
                jnp.concatenate(
                    [out[64 * k : 64 * k + 64, 64 * bx : 64 * bx + 64] for k in range(4)], 1
                ).astype(BF)
            )
    send[...] = dot(order[...], jnp.concatenate(rows, 0)).astype(BF)


def mix_body(got, weights, forward, back, repeat, send, product):
    both = dot(forward[...], got[...])
    modes = (both[:128] + both[128:]).astype(BF)
    spread = dot(repeat[...], modes)
    row = lax.broadcasted_iota(jnp.int32, (512, 256), 0)
    col = lax.broadcasted_iota(jnp.int32, (512, 256), 1)
    spread = jnp.where(col // 64 == (row % 8) // 2, spread, 0.0)
    for m in range(64):
        product[8 * m : 8 * m + 8, :] = dot(spread[8 * m : 8 * m + 8].astype(BF), weights[m])
    real, imag = [], []
    for kz in range(4):
        from_real = product[pl.ds(2 * kz, 64, stride=8), :]
        from_imag = product[pl.ds(2 * kz + 1, 64, stride=8), :]
        real.append(from_real[:, :64] - from_imag[:, 64:])
        imag.append(from_real[:, 64:] + from_imag[:, :64])
    mixed = jnp.concatenate([jnp.concatenate(real, 1), jnp.concatenate(imag, 1)], 0)
    high = mixed.astype(BF)
    low = (mixed - high.astype(F32)).astype(BF)
    send[...] = dot(back[...], jnp.concatenate([high, high, low], 0)).astype(BF)


def second_back_body(me, got, table, order, *rest):
    *sends, send = rest
    ordered = dot(order[...], got[...])
    for x2 in range(2):
        parts = []
        for k in range(4):
            parts.append(
                jnp.concatenate(
                    [
                        ordered[
                            (x2 * 4 + bx) * 64 : (x2 * 4 + bx) * 64 + 64, 64 * k : 64 * k + 64
                        ]
                        for bx in range(4)
                    ],
                    1,
                ).astype(BF)
            )
        out = dot(table[...], jnp.concatenate(parts, 0)).astype(BF)
        for py in range(8):
            for by in range(4):
                at = py * 128 + by * 32
                send[py, by * 64 + x2 * 32 : by * 64 + x2 * 32 + 32, :] = out[at : at + 32]
    to_relative(me, send, sends)


def layer_values(by, j, got, skipped, z_back):
    at = by * 64 + j * 16
    data = jnp.concatenate([got[kg, at : at + 16, :] for kg in range(8)], 0)
    total = dot(z_back, jnp.concatenate([data, data], 0))
    total = total + skipped[by, 2 * j : 2 * j + 2].reshape(256, 256)
    result = 0.5 * total * (1.0 + lax.erf(total * math.sqrt(0.5)))
    return result.astype(BF)


def load_grid(grid_at, grid, sems):
    copies = [
        pltpu.make_async_copy(grid_at.at[by], grid.at[by], sems.at[by]) for by in range(4)
    ]
    for copy in copies:
        copy.start()
    return copies


def four_fold(layer, skip, bias):
    wide = jnp.concatenate([skip[layer].astype(F32)] * 4, 1)
    tall = jnp.concatenate([wide] * 4, 0)
    row = lax.broadcasted_iota(jnp.int32, (256, 256), 0)
    col = lax.broadcasted_iota(jnp.int32, (256, 256), 1)
    matrix = jnp.where(row // 64 == col // 64, tall, 0.0).astype(BF)
    return matrix, jnp.concatenate([bias[layer : layer + 1, :]] * 4, 1)


def skip_body(layer, anchor, grid_at, skip, bias, out, grid, sems):
    copies = load_grid(grid_at, grid, sems)
    skip, bias = four_fold(layer, skip, bias)
    for by in range(4):
        copies[by].wait()
        product = dot(grid[by].reshape(1024, 256), skip) + bias
        out[by] = product.reshape(8, 128, 256)


def inner_layer_body(layer, me, *refs):
    *gots, skipped, z_back, z_table, weights_at, new_grid_at, weights = refs[:14]
    *sends, got, new_grid, modes, out_sems, sem = refs[14:]
    fetch = pltpu.make_async_copy(weights_at.at[pl.ds(layer * 64 + 64, 64)], weights, sem)
    fetch.start()
    from_relative(me, gots, got)
    stores = []
    for by in range(4):
        for j in range(4):
            values = layer_values(by, j, got, skipped, z_back[...])
            new_grid[by, 2 * j] = values[:128]
            new_grid[by, 2 * j + 1] = values[128:]
        stores.append(
            pltpu.make_async_copy(new_grid.at[by], new_grid_at.at[by], out_sems.at[by])
        )
        stores[-1].start()
        third_forward(by, lambda xy: new_grid[by, xy], z_table[...], modes)
    to_relative(me, modes, sends)
    for store in stores:
        store.wait()
    fetch.wait()


def last_layer_body(me, *refs):
    *gots, skipped, z_back, eye, bricks, got = refs
    from_relative(me, gots, got)
    for by in range(4):
        values = [
            layer_values(by, j, got, skipped, z_back[...]) for j in range(4)
        ]
        for bz in range(8):
            cells = jnp.concatenate(
                [
                    values[xy // 2][(xy % 2) * 128 + 16 * bz : (xy % 2) * 128 + 16 * bz + 16]
                    for xy in range(8)
                ],
                0,
            )
            turned = dot_nt(eye[...], cells).astype(BF)
            for bx in range(4):
                bricks[(bx * 4 + by) * 8 + bz] = turned[64 * bx : 64 * bx + 64]


def early_body(start, meta, aux, anchor, out, token):
    def one(k, _):
        d = start + 8 * pl.program_id(0) + k
        rows = aux[d].astype(F32)
        for rank in range(2):
            out[2 * k + rank] = block_weights(rank, d, meta, rows)[1]
        return 0

    lax.fori_loop(0, 8, one, 0, unroll=8)
    token[...] = jnp.zeros((8, 128), F32)


def early_weights(start, count, meta, aux, anchor):
    whole = pl.BlockSpec(memory_space=pltpu.VMEM)
    weights, token = pl.pallas_call(
        functools.partial(early_body, start),
        grid=(count // 8,),
        out_shape=[pltpu.HBM((2 * count, 512, 128), BF), shaped((8, 128), F32)],
        in_specs=[SM, whole, whole],
        out_specs=[pl.BlockSpec((16, 512, 128), lambda i: (i, 0, 0)), whole],
        compiler_params=pltpu.CompilerParams(vmem_limit_bytes=16 * MIB),
        cost_estimate=pl.CostEstimate(
            flops=count * 10**7, bytes_accessed=count * 2**18, transcendentals=0
        ),
    )(meta, aux, anchor)
    return in_hbm(weights), token


def decode_body(meta, aux, bricks, *refs):
    *stored_at, reply, stored, sems = refs
    loads = []
    for w in range(2):
        for i in range(EARLY // 8):
            loads.append(
                pltpu.make_async_copy(
                    stored_at[w].at[pl.ds(16 * i, 16)],
                    stored.at[pl.ds(2 * EARLY * w + 16 * i, 16)],
                    sems.at[len(loads)],
                )
            )
            loads[-1].start()

    def write(d, near, weights):
        both = DECODE_SCALE * dot(jnp.concatenate(near, 0), jnp.concatenate(weights, 1))
        reply[d, 0:64, :] = both[:64, :128].astype(BF)
        reply[d, 64:128, :] = both[64:, 128:].astype(BF)

    def fresh(k, _):
        d = 2 * EARLY + k
        rows = aux[d].astype(F32)
        near, weights = [], []
        for rank in range(2):
            ids, kernel = block_weights(rank, d, meta, rows)
            weights.append(kernel)
            near.append(jnp.concatenate([bricks[i] for i in ids], 1))
        write(d, near, weights)
        return 0

    lax.fori_loop(0, DEV - 2 * EARLY, fresh, 0, unroll=16)
    for load in loads:
        load.wait()

    def early(d, _):
        near = []
        for rank in range(2):
            ids = [meta[8 * rank + 1 + h, d] for h in range(4)]
            near.append(jnp.concatenate([bricks[i] for i in ids], 1))
        write(d, near, [stored[2 * d], stored[2 * d + 1]])
        return 0

    lax.fori_loop(0, 2 * EARLY, early, 0, unroll=16)


def pick_body(slots, got, out_at, out, sems):
    def part(i, _):
        def one(k, _):
            b = 32 * i + k
            out[b] = got[slots[b]]
            return 0

        lax.fori_loop(0, 32, one, 0, unroll=8)
        quarter(out, out_at, sems, i).start()
        return 0

    lax.fori_loop(0, 4, part, 0)
    for i in range(4):
        quarter(out, out_at, sems, i).wait()


def exchange(x, axis):
    return lax.all_to_all(x, axis, split_axis=0, concat_axis=0, tiled=True)


def exchange_lines(chunks):
    got = [chunks[0]]
    for j in range(1, 8):
        got.append(lax.ppermute(chunks[j], "py", [(i, (i + j) % 8) for i in range(8)]))
    return got


def per_device(values, offsets, counts, bricks, spectral_weights, skip_weights, skip_bias):
    t = {name: jnp.asarray(table) for name, table in tables().items()}
    me = lax.axis_index("py").astype(jnp.int32).reshape(1)
    weights = in_hbm(spectral_weights.reshape(LAYERS * 64, 256, 128))
    send, slots = pack(me, values, offsets, counts, bricks)
    got = exchange(send, ("px", "py"))
    grid, aux, meta, kept, modes = encode(slots, got, weights, t)
    chunks = pltpu.VMEM((8, 256, 256), BF)
    grid_scratch = pltpu.VMEM((4, 8, 128, 256), BF)
    four = pltpu.SemaphoreType.DMA((4,))
    piece = shaped((256, 256))
    stored = []
    for layer in range(LAYERS):
        kernel, token = early_weights(EARLY * layer, EARLY, meta, aux, modes[0])
        stored.append(kernel)
        columns = exchange_lines(modes)
        second = call(
            second_body,
            shaped((512, 256)),
            slots, token, *columns, t["y_forward"], t["to_send"],
            scratch=(chunks,),
            specs=[SM] + [VM] * 11,
            limit=24,
        )
        lines = exchange(second.reshape(16, 32, 256), "px").reshape(512, 256)
        back = call(
            mix_body,
            shaped((512, 256)),
            lines, kept, t["x_forward"], t["x_back"], t["repeat"],
            scratch=(pltpu.VMEM((512, 128), F32),),
            limit=24,
        )
        lines = exchange(back.reshape(16, 32, 256), "px").reshape(512, 256)
        columns = call(
            second_back_body,
            [piece] * 8,
            slots, lines, t["y_back"], t["from_send"],
            scratch=(chunks,),
            specs=[SM, VM, VM, VM],
            limit=24,
        )
        skipped = call(
            functools.partial(skip_body, layer),
            shaped((4, 8, 128, 256), F32),
            columns[0], grid, skip_weights, skip_bias,
            scratch=(grid_scratch, four),
            specs=[VM, HB, VM, VM],
            limit=24,
            flops=2 * 4096 * 256 * 256,
        )
        columns = exchange_lines(columns)
        if layer + 1 < LAYERS:
            grid, kept, *modes = call(
                functools.partial(inner_layer_body, layer),
                [pltpu.HBM((4, 8, 128, 256), BF), shaped((64, 256, 128))] + [piece] * 8,
                slots, *columns, skipped, t["z_back"], t["z_forward"],
                weights,
                scratch=(
                    chunks, grid_scratch, chunks, four,
                    pltpu.SemaphoreType.DMA,
                ),
                specs=[SM] + [VM] * 11 + [HB],
                out_specs=[HB] + [VM] * 9,
                limit=32,
            )
            grid = in_hbm(grid)
        else:
            final = call(
                last_layer_body,
                shaped((128, 64, 128)),
                slots, *columns, skipped, t["z_back"], t["eye"],
                scratch=(chunks,),
                specs=[SM] + [VM] * 11,
                limit=32,
            )
    reply = call(
        decode_body,
        shaped((DEV, 128, 128)),
        meta, aux, final, *stored,
        scratch=(
            pltpu.VMEM((4 * EARLY, 512, 128), BF),
            pltpu.SemaphoreType.DMA((EARLY // 4,)),
        ),
        specs=[SM, VM, VM, HB, HB],
        limit=40,
    )
    returned = exchange(reply, ("px", "py"))
    return call(
        pick_body,
        shaped((DEV, 64, 128)),
        slots, returned.reshape(2 * DEV, 64, 128),
        scratch=(pltpu.VMEM((DEV, 64, 128), BF), pltpu.SemaphoreType.DMA((4,))),
        specs=[SM, VM],
        out_specs=HB,
        limit=24,
    )


def solution(mesh):
    return jax.shard_map(
        per_device,
        mesh=mesh,
        in_specs=(
            P(("px", "py"), None, None),
            P(("px", "py"), None, None),
            P(("px", "py")),
            P(("px", "py"), None),
            P(None, None, "px", "py", None, None),
            P(),
            P(),
        ),
        out_specs=P(("px", "py"), None, None),
        check_vma=False,
    )
```

```python
import functools
import math

import jax
import jax.numpy as jnp
import numpy as np
from jax import lax
from jax.experimental import pallas as pl
from jax.experimental.pallas import tpu as pltpu
from jax.sharding import PartitionSpec as P

CH = 64
MODES = 32
LAYERS = 2
DEV = 128
AMPLITUDE = 0.25
SPREAD = 4.5
DECODE_SCALE = 0.1
BF = jnp.bfloat16
F32 = jnp.float32
MIB = 1024 * 1024
EARLY = 32
NT = (((1,), (1,)), ((), ()))
UNIT = math.sqrt(math.log2(math.e) / SPREAD)


def halves(table):
    high = np.asarray(table, np.float32).astype(BF)
    low = (np.asarray(table, np.float64) - high.astype(np.float64)).astype(np.float32).astype(BF)
    return high, low


def waves():
    j = np.arange(MODES)
    return np.where(j < MODES // 2, j, j - MODES)


def turn(frequency, place):
    return 2.0 * math.pi / 128 * ((frequency * place) % 128)


def forward_pair(angle):
    c, s = np.cos(angle) / math.sqrt(128), np.sin(angle) / math.sqrt(128)
    return np.array([[c, s], [-s, c]])


def backward_pair(angle):
    c, s = np.cos(angle) / math.sqrt(128), np.sin(angle) / math.sqrt(128)
    return np.array([[c, -s], [s, c]])


@functools.lru_cache(None)
def tables():
    k = np.arange(MODES)
    z = np.arange(128)
    angle = turn(k[:, None], z[None, :])
    mz = np.stack([np.cos(angle), -np.sin(angle)], 1).reshape(64, 128) / math.sqrt(128)
    z_forward = halves(mz)[0]
    weight = np.where(k == 0, 1.0, 2.0)[:, None, None]
    inv = np.stack([np.cos(angle), -np.sin(angle)], 1) / math.sqrt(128) * weight
    inv = inv.reshape(8, 8, 128)
    zi = np.zeros((2, 128, 8, 2, 8))
    for y2 in range(2):
        zi[y2, :, :, y2, :] = inv.transpose(2, 0, 1)
    z_back = halves(zi.reshape(256, 128))[0]
    f = waves()
    y = np.arange(128)
    pair = forward_pair(turn(f[:, None], y[None, :])).reshape(2, 2, 16, 2, 32, 4)
    ty = np.zeros((4, 16, 2, 2, 32, 4, 4, 2))
    for k4 in range(4):
        ty[k4, :, :, :, :, :, k4, :] = pair.transpose(2, 3, 0, 4, 5, 1)
    y_forward = halves(ty.reshape(256, 1024))[0]
    pair = backward_pair(turn(f[:, None], y[None, :])).reshape(2, 2, 16, 2, 32, 4)
    ti = np.zeros((32, 4, 4, 2, 4, 16, 2, 2))
    for k4 in range(4):
        ti[:, :, k4, :, k4, :, :, :] = pair.transpose(4, 5, 0, 2, 3, 1)
    y_back = halves(ti.reshape(1024, 256))[0]
    x = np.arange(128)
    pair = forward_pair(turn(f[:, None], x[None, :])).reshape(2, 2, 32, 16, 4, 2)
    tx = np.zeros((32, 2, 2, 16, 2, 4, 2, 2))
    for ky in range(2):
        tx[:, ky, :, :, :, :, ky, :] = pair.transpose(2, 0, 3, 5, 4, 1)
    x_forward = np.concatenate(halves(tx.reshape(128, 512)), 0)
    pair = backward_pair(turn(f[:, None], x[None, :])).reshape(2, 2, 32, 16, 4, 2)
    txi = np.zeros((16, 2, 4, 2, 2, 2, 32, 2))
    for ky in range(2):
        txi[:, :, :, ky, :, :, :, ky] = pair.transpose(3, 5, 4, 0, 1, 2)
    high, low = halves(txi.reshape(512, 128))
    x_back = np.concatenate([high, low, high], 1)
    order = np.arange(512).reshape(8, 16, 4).transpose(1, 0, 2).reshape(-1)
    to_send = np.eye(512)[order].astype(BF)
    from_send = np.ascontiguousarray(np.eye(512)[order].T).astype(BF)
    row = np.arange(512)
    repeat = np.eye(128)[(row // 8) * 2 + row % 2].astype(BF)
    return dict(
        z_forward=z_forward, z_back=z_back, y_forward=y_forward, y_back=y_back,
        x_forward=x_forward, x_back=x_back, to_send=to_send, from_send=from_send,
        repeat=repeat, eye=np.eye(256).astype(BF),
    )


def dot(a, b):
    return jnp.dot(a, b, preferred_element_type=F32)


def dot_nt(a, b):
    return lax.dot_general(a, b, NT, preferred_element_type=F32)


def call(
    body, out_shape, *args, scratch=(), specs=None, out_specs=None, limit=40, flops=None
):
    vm = pl.BlockSpec(memory_space=pltpu.VMEM)
    single = not isinstance(out_shape, (tuple, list))
    if specs is None:
        specs = [vm] * len(args)
    if out_specs is None:
        out_specs = vm if single else [vm] * len(out_shape)
    return pl.pallas_call(
        body,
        out_shape=out_shape,
        in_specs=specs,
        out_specs=out_specs,
        scratch_shapes=list(scratch),
        cost_estimate=flops and pl.CostEstimate(
            flops=flops, bytes_accessed=flops // 100, transcendentals=0
        ),
        compiler_params=pltpu.CompilerParams(vmem_limit_bytes=limit * MIB),
    )(*args)


VM = pl.BlockSpec(memory_space=pltpu.VMEM)
SM = pl.BlockSpec(memory_space=pltpu.SMEM)
HB = pl.BlockSpec(memory_space=pltpu.HBM)


def in_hbm(x):
    return pltpu.with_memory_space_constraint(x, pltpu.HBM)


def shaped(shape, dtype=BF):
    return jax.ShapeDtypeStruct(shape, dtype)


def pack_body(
    me, bricks_at, counts_at, values_at, offsets_at, send, slots,
    seen, aux, bricks, counts, offsets_in, offsets, values, sems,
):
    loads = [
        pltpu.make_async_copy(
            values_at.at[pl.ds(32 * i, 32)], values.at[pl.ds(32 * i, 32)], sems.at[i]
        )
        for i in range(4)
    ]
    for load in loads:
        load.start()
    small = [
        pltpu.make_async_copy(source, target, sems.at[4 + i])
        for i, (source, target) in enumerate(
            [(bricks_at, bricks), (counts_at, counts), (offsets_at, offsets_in)]
        )
    ]
    for load in small:
        load.start()
    slots[DEV] = me[0]

    def clear(d, _):
        send[d] = jnp.zeros((136, 128), BF)
        aux[d] = jnp.zeros((8, 128), F32)
        seen[d] = 0
        return 0

    lax.fori_loop(0, DEV, clear, 0, unroll=4)
    lane = lax.broadcasted_iota(jnp.int32, (1, 128), 1)
    for load in small:
        load.wait()
    offsets[...] = offsets_in[...].astype(F32)
    for load in loads:
        load.wait()

    def one(b, _):
        head = bricks[0, b]
        owner = head >> 7
        rank = seen[owner]
        seen[owner] = rank + 1
        slots[b] = owner * 2 + rank

        send[owner, pl.ds(pl.multiple_of(rank * 64, 64), 64), :] = values[b]
        meta = jnp.where(lane == 0, counts[b], 0)
        for h in range(4):
            meta = jnp.where(lane == 1 + h, bricks[h, b] & 127, meta)
        rows = [offsets[k, pl.ds(b, 1), :] for k in range(3)] + [meta.astype(F32)]
        aux[owner, pl.ds(pl.multiple_of(4 * rank, 4), 4), :] = jnp.concatenate(rows, 0)
        return 0

    lax.fori_loop(0, DEV, one, 0, unroll=8)

    def finish(d, _):
        send[d, 128:136, :] = aux[d].astype(BF)
        return 0

    lax.fori_loop(0, DEV, finish, 0, unroll=4)


def pack(me, values, offsets, counts, bricks):
    return call(
        pack_body,
        (shaped((DEV, 136, 128)), shaped((DEV + 8,), jnp.int32)),
        me, in_hbm(bricks.T), in_hbm(counts), in_hbm(values), in_hbm(offsets.transpose(1, 0, 2)),
        scratch=(
            pltpu.SMEM((DEV,), jnp.int32),
            pltpu.VMEM((DEV, 8, 128), F32),
            pltpu.SMEM((4, DEV), jnp.int32),
            pltpu.SMEM((DEV,), jnp.int32),
            pltpu.VMEM((3, 128, 128), BF),
            pltpu.VMEM((3, 128, 128), F32),
            pltpu.VMEM((DEV, 64, 128), BF),
            pltpu.SemaphoreType.DMA((7,)),
        ),
        specs=[SM, HB, HB, HB, HB],
        out_specs=[VM, SM],
        limit=24,
    )


def spread_weights(place, count, ids):
    lane = lax.broadcasted_iota(jnp.int32, (1, 128), 1)
    sub = lax.broadcasted_iota(jnp.int32, (8, 128), 0)
    xs = ((sub // 4).astype(F32) + 0.5) * UNIT
    ys = ((sub % 4).astype(F32) + 0.5) * UNIT
    zs = (lax.broadcasted_iota(jnp.int32, (16, 128), 0).astype(F32) + 0.5) * UNIT
    place = place * UNIT
    px = jnp.where(lane < count, place[0:1], 1.0e4) - xs
    py = place[1:2] - ys
    pz = place[2:3] - zs
    grid_at = [(i >> 5, (i >> 3) & 3, i & 7) for i in ids]
    parts = []
    for h in range(4):
        shift = [(a - b).astype(F32) for a, b in zip(grid_at[h], grid_at[0])]
        dx = px - shift[0] * (2 * UNIT)
        dy = py - shift[1] * (4 * UNIT)
        dz = pz - shift[2] * (16 * UNIT)
        xy = jnp.exp2(math.log2(AMPLITUDE) - dx * dx - dy * dy)
        zz = jnp.exp2(-(dz * dz))
        for i in range(8):
            parts.append((xy[i : i + 1] * zz).astype(BF))
    return jnp.concatenate(parts, 0)


def to_relative(slots, chunks, sends):
    for j in range(8):
        sends[j][...] = chunks[(slots[DEV] + j) & 7]


def from_relative(slots, gots, chunks):
    for j in range(8):
        chunks[(slots[DEV] - j) & 7] = gots[j][...]


def third_forward(by, grid_at, table, out):
    for j in range(4):
        modes = []
        for half in range(2):
            modes.append(dot(table, grid_at(2 * j + half)))
        for kg in range(8):
            piece = jnp.concatenate([m[8 * kg : 8 * kg + 8] for m in modes], 0)
            at = by * 64 + j * 16
            out[kg, at : at + 16, :] = piece.astype(BF)


def block_weights(rank, d, meta, rows):
    ids = [meta[8 * rank + 1 + h, d] for h in range(4)]
    return ids, spread_weights(rows[4 * rank : 4 * rank + 3], meta[8 * rank, d], ids)


def spread_one(rank, d, meta, rows, block, acc):
    ids, weights = block_weights(rank, d, meta, rows)
    tile = dot_nt(block, weights)
    for h in range(4):
        acc[ids[h]] = acc[ids[h]] + tile[:, 128 * h : 128 * h + 128]


def quarter(source, target, sems, i):
    return pltpu.make_async_copy(
        source.at[pl.ds(32 * i, 32)], target.at[pl.ds(32 * i, 32)], sems.at[i]
    )


def encode_body(slots, got_at, eye, z_table, weights_at, grid_at, aux, meta_out, weights, *rest):
    *sends, modes, grid, acc, got, wide, meta, got_sems, grid_sems, sems = rest
    first = pltpu.make_async_copy(got_at.at[:, pl.ds(128, 8), :], aux, sems.at[0])
    first.start()
    for i in range(4):
        quarter(got_at, got, got_sems, i).start()
    fetch = pltpu.make_async_copy(weights_at.at[pl.ds(0, 64)], weights, sems.at[1])
    fetch.start()

    def clear(b, _):
        acc[b] = jnp.zeros((64, 128), F32)
        return 0

    lax.fori_loop(0, 128, clear, 0, unroll=4)
    first.wait()
    wide[...] = aux[...].astype(F32).reshape(8 * DEV, 128)
    for rank in range(2):
        numbers = wide[pl.ds(4 * rank + 3, DEV, stride=8), :].T
        meta_out[8 * rank : 8 * rank + 8, :] = numbers[0:8].astype(jnp.int32)
    to_scalar = pltpu.make_async_copy(meta_out, meta, sems.at[2])
    to_scalar.start()


    to_scalar.wait()

    def part(i, _):
        quarter(got_at, got, got_sems, i).wait()

        def one(k, _):
            d = 32 * i + k
            rows = aux[d].astype(F32)
            for rank in range(2):
                spread_one(rank, d, meta, rows, got[d, 64 * rank : 64 * rank + 64, :], acc)
            return 0

        return lax.fori_loop(0, 32, one, 0, unroll=16)

    lax.fori_loop(0, 4, part, 0)
    eye128 = eye[0:128, 0:128]
    stores = []
    for by in range(4):
        for bz in range(8):
            bricks = jnp.concatenate([acc[(bx * 4 + by) * 8 + bz] for bx in range(4)], 0)
            cells = dot_nt(eye128, bricks.astype(BF)).astype(BF)
            for xy in range(8):
                grid[by, xy, 16 * bz : 16 * bz + 16, :] = cells[16 * xy : 16 * xy + 16]
        stores.append(pltpu.make_async_copy(grid.at[by], grid_at.at[by], grid_sems.at[by]))
        stores[-1].start()
        third_forward(by, lambda xy: grid[by, xy], z_table[...], modes)
    to_relative(slots, modes, sends)
    for store in stores:
        store.wait()
    fetch.wait()


def encode(slots, got, weights, t):
    out = call(
        encode_body,
        [
            pltpu.HBM((4, 8, 128, 256), BF),
            shaped((DEV, 8, 128)),
            shaped((16, DEV), jnp.int32),
            shaped((64, 256, 128)),
        ]
        + [shaped((256, 256))] * 8,
        slots, in_hbm(got), t["eye"], t["z_forward"], weights,
        scratch=(
            pltpu.VMEM((8, 256, 256), BF),
            pltpu.VMEM((4, 8, 128, 256), BF),
            pltpu.VMEM((128, 64, 128), F32),
            pltpu.VMEM((DEV, 136, 128), BF),
            pltpu.VMEM((8 * DEV, 128), F32),
            pltpu.SMEM((16, DEV), jnp.int32),
            pltpu.SemaphoreType.DMA((4,)),
            pltpu.SemaphoreType.DMA((4,)),
            pltpu.SemaphoreType.DMA((3,)),
        ),
        specs=[SM, HB, VM, VM, HB],
        out_specs=[HB] + [VM] * 11,
        limit=24,
    )
    return in_hbm(out[0]), out[1], out[2], out[3], out[4:]


def second_body(me, token, *refs):
    *gots, table, order, send, got = refs
    from_relative(me, gots, got)
    rows = []
    for x2 in range(2):
        data = jnp.concatenate(
            [
                got[py, by * 64 + x2 * 32 : by * 64 + x2 * 32 + 32, :]
                for py in range(8)
                for by in range(4)
            ],
            0,
        )
        out = dot(table[...], data)
        for bx in range(4):
            rows.append(
                jnp.concatenate(
                    [out[64 * k : 64 * k + 64, 64 * bx : 64 * bx + 64] for k in range(4)], 1
                ).astype(BF)
            )
    send[...] = dot(order[...], jnp.concatenate(rows, 0)).astype(BF)


def mix_body(got, weights, forward, back, repeat, send, product):
    both = dot(forward[...], got[...])
    modes = (both[:128] + both[128:]).astype(BF)
    spread = dot(repeat[...], modes)
    row = lax.broadcasted_iota(jnp.int32, (512, 256), 0)
    col = lax.broadcasted_iota(jnp.int32, (512, 256), 1)
    spread = jnp.where(col // 64 == (row % 8) // 2, spread, 0.0)
    for m in range(64):
        product[8 * m : 8 * m + 8, :] = dot(spread[8 * m : 8 * m + 8].astype(BF), weights[m])
    real, imag = [], []
    for kz in range(4):
        from_real = product[pl.ds(2 * kz, 64, stride=8), :]
        from_imag = product[pl.ds(2 * kz + 1, 64, stride=8), :]
        real.append(from_real[:, :64] - from_imag[:, 64:])
        imag.append(from_real[:, 64:] + from_imag[:, :64])
    mixed = jnp.concatenate([jnp.concatenate(real, 1), jnp.concatenate(imag, 1)], 0)
    high = mixed.astype(BF)
    low = (mixed - high.astype(F32)).astype(BF)
    send[...] = dot(back[...], jnp.concatenate([high, high, low], 0)).astype(BF)


def second_back_body(me, got, table, order, *rest):
    *sends, send = rest
    ordered = dot(order[...], got[...])
    for x2 in range(2):
        parts = []
        for k in range(4):
            parts.append(
                jnp.concatenate(
                    [
                        ordered[
                            (x2 * 4 + bx) * 64 : (x2 * 4 + bx) * 64 + 64, 64 * k : 64 * k + 64
                        ]
                        for bx in range(4)
                    ],
                    1,
                ).astype(BF)
            )
        out = dot(table[...], jnp.concatenate(parts, 0)).astype(BF)
        for py in range(8):
            for by in range(4):
                at = py * 128 + by * 32
                send[py, by * 64 + x2 * 32 : by * 64 + x2 * 32 + 32, :] = out[at : at + 32]
    to_relative(me, send, sends)


def layer_values(by, j, got, skipped, z_back):
    at = by * 64 + j * 16
    data = jnp.concatenate([got[kg, at : at + 16, :] for kg in range(8)], 0)
    total = dot(z_back, data)
    total = total + skipped[by, 2 * j : 2 * j + 2].reshape(256, 256)
    result = 0.5 * total * (1.0 + lax.erf(total * math.sqrt(0.5)))
    return result.astype(BF)


def load_grid(grid_at, grid, sems):
    copies = [
        pltpu.make_async_copy(grid_at.at[by], grid.at[by], sems.at[by]) for by in range(4)
    ]
    for copy in copies:
        copy.start()
    return copies


def four_fold(layer, skip, bias):
    wide = jnp.concatenate([skip[layer].astype(F32)] * 4, 1)
    tall = jnp.concatenate([wide] * 4, 0)
    row = lax.broadcasted_iota(jnp.int32, (256, 256), 0)
    col = lax.broadcasted_iota(jnp.int32, (256, 256), 1)
    matrix = jnp.where(row // 64 == col // 64, tall, 0.0).astype(BF)
    return matrix, jnp.concatenate([bias[layer : layer + 1, :]] * 4, 1)


def skip_body(layer, anchor, grid_at, skip, bias, out, grid, sems):
    copies = load_grid(grid_at, grid, sems)
    skip, bias = four_fold(layer, skip, bias)
    for by in range(4):
        copies[by].wait()
        product = dot(grid[by].reshape(1024, 256), skip) + bias
        out[by] = product.reshape(8, 128, 256)


def inner_layer_body(layer, me, *refs):
    *gots, skipped, z_back, z_table, weights_at, new_grid_at, weights = refs[:14]
    *sends, got, new_grid, modes, out_sems, sem = refs[14:]
    fetch = pltpu.make_async_copy(weights_at.at[pl.ds(layer * 64 + 64, 64)], weights, sem)
    fetch.start()
    from_relative(me, gots, got)
    stores = []
    for by in range(4):
        for j in range(4):
            values = layer_values(by, j, got, skipped, z_back[...])
            new_grid[by, 2 * j] = values[:128]
            new_grid[by, 2 * j + 1] = values[128:]
        stores.append(
            pltpu.make_async_copy(new_grid.at[by], new_grid_at.at[by], out_sems.at[by])
        )
        stores[-1].start()
        third_forward(by, lambda xy: new_grid[by, xy], z_table[...], modes)
    to_relative(me, modes, sends)
    for store in stores:
        store.wait()
    fetch.wait()


def last_layer_body(me, *refs):
    *gots, skipped, z_back, eye, bricks, got = refs
    from_relative(me, gots, got)
    for by in range(4):
        values = [
            layer_values(by, j, got, skipped, z_back[...]) for j in range(4)
        ]
        for bz in range(8):
            cells = jnp.concatenate(
                [
                    values[xy // 2][(xy % 2) * 128 + 16 * bz : (xy % 2) * 128 + 16 * bz + 16]
                    for xy in range(8)
                ],
                0,
            )
            turned = dot_nt(eye[...], cells).astype(BF)
            for bx in range(4):
                bricks[(bx * 4 + by) * 8 + bz] = turned[64 * bx : 64 * bx + 64]


def early_body(start, meta, aux, anchor, out, token):
    def one(k, _):
        d = start + 8 * pl.program_id(0) + k
        rows = aux[d].astype(F32)
        for rank in range(2):
            out[2 * k + rank] = block_weights(rank, d, meta, rows)[1]
        return 0

    lax.fori_loop(0, 8, one, 0, unroll=8)
    token[...] = jnp.zeros((8, 128), F32)


def early_weights(start, count, meta, aux, anchor):
    whole = pl.BlockSpec(memory_space=pltpu.VMEM)
    weights, token = pl.pallas_call(
        functools.partial(early_body, start),
        grid=(count // 8,),
        out_shape=[pltpu.HBM((2 * count, 512, 128), BF), shaped((8, 128), F32)],
        in_specs=[SM, whole, whole],
        out_specs=[pl.BlockSpec((16, 512, 128), lambda i: (i, 0, 0)), whole],
        compiler_params=pltpu.CompilerParams(vmem_limit_bytes=16 * MIB),
        cost_estimate=pl.CostEstimate(
            flops=count * 10**7, bytes_accessed=count * 2**18, transcendentals=0
        ),
    )(meta, aux, anchor)
    return in_hbm(weights), token


def decode_body(meta, aux, bricks, *refs):
    *stored_at, reply, stored, sems = refs
    loads = []
    for w in range(2):
        for i in range(EARLY // 8):
            loads.append(
                pltpu.make_async_copy(
                    stored_at[w].at[pl.ds(16 * i, 16)],
                    stored.at[pl.ds(2 * EARLY * w + 16 * i, 16)],
                    sems.at[len(loads)],
                )
            )
            loads[-1].start()

    def write(d, near, weights):
        both = DECODE_SCALE * dot(jnp.concatenate(near, 0), jnp.concatenate(weights, 1))
        reply[d, 0:64, :] = both[:64, :128].astype(BF)
        reply[d, 64:128, :] = both[64:, 128:].astype(BF)

    def fresh(k, _):
        d = 2 * EARLY + k
        rows = aux[d].astype(F32)
        near, weights = [], []
        for rank in range(2):
            ids, kernel = block_weights(rank, d, meta, rows)
            weights.append(kernel)
            near.append(jnp.concatenate([bricks[i] for i in ids], 1))
        write(d, near, weights)
        return 0

    lax.fori_loop(0, DEV - 2 * EARLY, fresh, 0, unroll=16)
    for load in loads:
        load.wait()

    def early(d, _):
        near = []
        for rank in range(2):
            ids = [meta[8 * rank + 1 + h, d] for h in range(4)]
            near.append(jnp.concatenate([bricks[i] for i in ids], 1))
        write(d, near, [stored[2 * d], stored[2 * d + 1]])
        return 0

    lax.fori_loop(0, 2 * EARLY, early, 0, unroll=16)


def pick_body(slots, got, out_at, out, sems):
    def part(i, _):
        def one(k, _):
            b = 32 * i + k
            out[b] = got[slots[b]]
            return 0

        lax.fori_loop(0, 32, one, 0, unroll=8)
        quarter(out, out_at, sems, i).start()
        return 0

    lax.fori_loop(0, 4, part, 0)
    for i in range(4):
        quarter(out, out_at, sems, i).wait()


def exchange(x, axis):
    return lax.all_to_all(x, axis, split_axis=0, concat_axis=0, tiled=True)


def exchange_lines(chunks):
    got = [chunks[0]]
    for j in range(1, 8):
        got.append(lax.ppermute(chunks[j], "py", [(i, (i + j) % 8) for i in range(8)]))
    return got


def per_device(values, offsets, counts, bricks, spectral_weights, skip_weights, skip_bias):
    t = {name: jnp.asarray(table) for name, table in tables().items()}
    me = lax.axis_index("py").astype(jnp.int32).reshape(1)
    weights = in_hbm(spectral_weights.reshape(LAYERS * 64, 256, 128))
    send, slots = pack(me, values, offsets, counts, bricks)
    got = exchange(send, ("px", "py"))
    grid, aux, meta, kept, modes = encode(slots, got, weights, t)
    chunks = pltpu.VMEM((8, 256, 256), BF)
    grid_scratch = pltpu.VMEM((4, 8, 128, 256), BF)
    four = pltpu.SemaphoreType.DMA((4,))
    piece = shaped((256, 256))
    stored = []
    for layer in range(LAYERS):
        kernel, token = early_weights(EARLY * layer, EARLY, meta, aux, modes[0])
        stored.append(kernel)
        columns = exchange_lines(modes)
        second = call(
            second_body,
            shaped((512, 256)),
            slots, token, *columns, t["y_forward"], t["to_send"],
            scratch=(chunks,),
            specs=[SM] + [VM] * 11,
            limit=24,
        )
        lines = exchange(second.reshape(16, 32, 256), "px").reshape(512, 256)
        back = call(
            mix_body,
            shaped((512, 256)),
            lines, kept, t["x_forward"], t["x_back"], t["repeat"],
            scratch=(pltpu.VMEM((512, 128), F32),),
            limit=24,
        )
        lines = exchange(back.reshape(16, 32, 256), "px").reshape(512, 256)
        columns = call(
            second_back_body,
            [piece] * 8,
            slots, lines, t["y_back"], t["from_send"],
            scratch=(chunks,),
            specs=[SM, VM, VM, VM],
            limit=24,
        )
        skipped = call(
            functools.partial(skip_body, layer),
            shaped((4, 8, 128, 256), F32),
            columns[0], grid, skip_weights, skip_bias,
            scratch=(grid_scratch, four),
            specs=[VM, HB, VM, VM],
            limit=24,
            flops=2 * 4096 * 256 * 256,
        )
        columns = exchange_lines(columns)
        if layer + 1 < LAYERS:
            grid, kept, *modes = call(
                functools.partial(inner_layer_body, layer),
                [pltpu.HBM((4, 8, 128, 256), BF), shaped((64, 256, 128))] + [piece] * 8,
                slots, *columns, skipped, t["z_back"], t["z_forward"],
                weights,
                scratch=(
                    chunks, grid_scratch, chunks, four,
                    pltpu.SemaphoreType.DMA,
                ),
                specs=[SM] + [VM] * 11 + [HB],
                out_specs=[HB] + [VM] * 9,
                limit=32,
            )
            grid = in_hbm(grid)
        else:
            final = call(
                last_layer_body,
                shaped((128, 64, 128)),
                slots, *columns, skipped, t["z_back"], t["eye"],
                scratch=(chunks,),
                specs=[SM] + [VM] * 11,
                limit=32,
            )
    reply = call(
        decode_body,
        shaped((DEV, 128, 128)),
        meta, aux, final, *stored,
        scratch=(
            pltpu.VMEM((4 * EARLY, 512, 128), BF),
            pltpu.SemaphoreType.DMA((EARLY // 4,)),
        ),
        specs=[SM, VM, VM, HB, HB],
        limit=40,
    )
    returned = exchange(reply, ("px", "py"))
    return call(
        pick_body,
        shaped((DEV, 64, 128)),
        slots, returned.reshape(2 * DEV, 64, 128),
        scratch=(pltpu.VMEM((DEV, 64, 128), BF), pltpu.SemaphoreType.DMA((4,))),
        specs=[SM, VM],
        out_specs=HB,
        limit=24,
    )


def solution(mesh):
    return jax.shard_map(
        per_device,
        mesh=mesh,
        in_specs=(
            P(("px", "py"), None, None),
            P(("px", "py"), None, None),
            P(("px", "py")),
            P(("px", "py"), None),
            P(None, None, "px", "py", None, None),
            P(),
            P(),
        ),
        out_specs=P(("px", "py"), None, None),
        check_vma=False,
    )
```

```python
import functools
import math

import jax
import jax.numpy as jnp
import numpy as np
from jax import lax
from jax.experimental import pallas as pl
from jax.experimental.pallas import tpu as pltpu
from jax.sharding import PartitionSpec as P

CH = 64
MODES = 32
LAYERS = 2
DEV = 128
AMPLITUDE = 0.25
SPREAD = 4.5
DECODE_SCALE = 0.1
BF = jnp.bfloat16
F32 = jnp.float32
MIB = 1024 * 1024
EARLY = 32
NT = (((1,), (1,)), ((), ()))
UNIT = math.sqrt(math.log2(math.e) / SPREAD)


def halves(table):
    high = np.asarray(table, np.float32).astype(BF)
    low = (np.asarray(table, np.float64) - high.astype(np.float64)).astype(np.float32).astype(BF)
    return high, low


def waves():
    j = np.arange(MODES)
    return np.where(j < MODES // 2, j, j - MODES)


def turn(frequency, place):
    return 2.0 * math.pi / 128 * ((frequency * place) % 128)


def forward_pair(angle):
    c, s = np.cos(angle) / math.sqrt(128), np.sin(angle) / math.sqrt(128)
    return np.array([[c, s], [-s, c]])


def backward_pair(angle):
    c, s = np.cos(angle) / math.sqrt(128), np.sin(angle) / math.sqrt(128)
    return np.array([[c, -s], [s, c]])


@functools.lru_cache(None)
def tables():
    k = np.arange(MODES)
    z = np.arange(128)
    angle = turn(k[:, None], z[None, :])
    mz = np.stack([np.cos(angle), -np.sin(angle)], 1).reshape(64, 128) / math.sqrt(128)
    z_forward = np.concatenate(halves(mz), 0)
    weight = np.where(k == 0, 1.0, 2.0)[:, None, None]
    inv = np.stack([np.cos(angle), -np.sin(angle)], 1) / math.sqrt(128) * weight
    inv = inv.reshape(8, 8, 128)
    zi = np.zeros((2, 128, 8, 2, 8))
    for y2 in range(2):
        zi[y2, :, :, y2, :] = inv.transpose(2, 0, 1)
    z_back = np.concatenate(halves(zi.reshape(256, 128)), 1)
    f = waves()
    y = np.arange(128)
    pair = forward_pair(turn(f[:, None], y[None, :])).reshape(2, 2, 16, 2, 32, 4)
    ty = np.zeros((4, 16, 2, 2, 32, 4, 4, 2))
    for k4 in range(4):
        ty[k4, :, :, :, :, :, k4, :] = pair.transpose(2, 3, 0, 4, 5, 1)
    y_forward = halves(ty.reshape(256, 1024))[0]
    pair = backward_pair(turn(f[:, None], y[None, :])).reshape(2, 2, 16, 2, 32, 4)
    ti = np.zeros((32, 4, 4, 2, 4, 16, 2, 2))
    for k4 in range(4):
        ti[:, :, k4, :, k4, :, :, :] = pair.transpose(4, 5, 0, 2, 3, 1)
    y_back = halves(ti.reshape(1024, 256))[0]
    x = np.arange(128)
    pair = forward_pair(turn(f[:, None], x[None, :])).reshape(2, 2, 32, 16, 4, 2)
    tx = np.zeros((32, 2, 2, 16, 2, 4, 2, 2))
    for ky in range(2):
        tx[:, ky, :, :, :, :, ky, :] = pair.transpose(2, 0, 3, 5, 4, 1)
    x_forward = np.concatenate(halves(tx.reshape(128, 512)), 0)
    pair = backward_pair(turn(f[:, None], x[None, :])).reshape(2, 2, 32, 16, 4, 2)
    txi = np.zeros((16, 2, 4, 2, 2, 2, 32, 2))
    for ky in range(2):
        txi[:, :, :, ky, :, :, :, ky] = pair.transpose(3, 5, 4, 0, 1, 2)
    high, low = halves(txi.reshape(512, 128))
    x_back = np.concatenate([high, low, high], 1)
    order = np.arange(512).reshape(8, 16, 4).transpose(1, 0, 2).reshape(-1)
    to_send = np.eye(512)[order].astype(BF)
    from_send = np.ascontiguousarray(np.eye(512)[order].T).astype(BF)
    row = np.arange(512)
    repeat = np.eye(128)[(row // 8) * 2 + row % 2].astype(BF)
    return dict(
        z_forward=z_forward, z_back=z_back, y_forward=y_forward, y_back=y_back,
        x_forward=x_forward, x_back=x_back, to_send=to_send, from_send=from_send,
        repeat=repeat, eye=np.eye(256).astype(BF),
    )


def dot(a, b):
    return jnp.dot(a, b, preferred_element_type=F32)


def dot_nt(a, b):
    return lax.dot_general(a, b, NT, preferred_element_type=F32)


def call(
    body, out_shape, *args, scratch=(), specs=None, out_specs=None, limit=40, flops=None
):
    vm = pl.BlockSpec(memory_space=pltpu.VMEM)
    single = not isinstance(out_shape, (tuple, list))
    if specs is None:
        specs = [vm] * len(args)
    if out_specs is None:
        out_specs = vm if single else [vm] * len(out_shape)
    return pl.pallas_call(
        body,
        out_shape=out_shape,
        in_specs=specs,
        out_specs=out_specs,
        scratch_shapes=list(scratch),
        cost_estimate=flops and pl.CostEstimate(
            flops=flops, bytes_accessed=flops // 100, transcendentals=0
        ),
        compiler_params=pltpu.CompilerParams(vmem_limit_bytes=limit * MIB),
    )(*args)


VM = pl.BlockSpec(memory_space=pltpu.VMEM)
SM = pl.BlockSpec(memory_space=pltpu.SMEM)
HB = pl.BlockSpec(memory_space=pltpu.HBM)


def in_hbm(x):
    return pltpu.with_memory_space_constraint(x, pltpu.HBM)


def shaped(shape, dtype=BF):
    return jax.ShapeDtypeStruct(shape, dtype)


def pack_body(
    me, bricks_at, counts_at, values_at, offsets_at, send, slots,
    seen, aux, bricks, counts, offsets_in, offsets, values, sems,
):
    loads = [
        pltpu.make_async_copy(
            values_at.at[pl.ds(32 * i, 32)], values.at[pl.ds(32 * i, 32)], sems.at[i]
        )
        for i in range(4)
    ]
    for load in loads:
        load.start()
    small = [
        pltpu.make_async_copy(source, target, sems.at[4 + i])
        for i, (source, target) in enumerate(
            [(bricks_at, bricks), (counts_at, counts), (offsets_at, offsets_in)]
        )
    ]
    for load in small:
        load.start()
    slots[DEV] = me[0]

    def clear(d, _):
        send[d] = jnp.zeros((136, 128), BF)
        aux[d] = jnp.zeros((8, 128), F32)
        seen[d] = 0
        return 0

    lax.fori_loop(0, DEV, clear, 0, unroll=4)
    lane = lax.broadcasted_iota(jnp.int32, (1, 128), 1)
    for load in small:
        load.wait()
    offsets[...] = offsets_in[...].astype(F32)
    for load in loads:
        load.wait()

    def one(b, _):
        head = bricks[0, b]
        owner = head >> 7
        rank = seen[owner]
        seen[owner] = rank + 1
        slots[b] = owner * 2 + rank

        send[owner, pl.ds(pl.multiple_of(rank * 64, 64), 64), :] = values[b]
        meta = jnp.where(lane == 0, counts[b], 0)
        for h in range(4):
            meta = jnp.where(lane == 1 + h, bricks[h, b] & 127, meta)
        rows = [offsets[k, pl.ds(b, 1), :] for k in range(3)] + [meta.astype(F32)]
        aux[owner, pl.ds(pl.multiple_of(4 * rank, 4), 4), :] = jnp.concatenate(rows, 0)
        return 0

    lax.fori_loop(0, DEV, one, 0, unroll=8)

    def finish(d, _):
        send[d, 128:136, :] = aux[d].astype(BF)
        return 0

    lax.fori_loop(0, DEV, finish, 0, unroll=4)


def pack(me, values, offsets, counts, bricks):
    return call(
        pack_body,
        (shaped((DEV, 136, 128)), shaped((DEV + 8,), jnp.int32)),
        me, in_hbm(bricks.T), in_hbm(counts), in_hbm(values), in_hbm(offsets.transpose(1, 0, 2)),
        scratch=(
            pltpu.SMEM((DEV,), jnp.int32),
            pltpu.VMEM((DEV, 8, 128), F32),
            pltpu.SMEM((4, DEV), jnp.int32),
            pltpu.SMEM((DEV,), jnp.int32),
            pltpu.VMEM((3, 128, 128), BF),
            pltpu.VMEM((3, 128, 128), F32),
            pltpu.VMEM((DEV, 64, 128), BF),
            pltpu.SemaphoreType.DMA((7,)),
        ),
        specs=[SM, HB, HB, HB, HB],
        out_specs=[VM, SM],
        limit=24,
    )


def spread_weights(place, count, ids):
    lane = lax.broadcasted_iota(jnp.int32, (1, 128), 1)
    sub = lax.broadcasted_iota(jnp.int32, (8, 128), 0)
    xs = ((sub // 4).astype(F32) + 0.5) * UNIT
    ys = ((sub % 4).astype(F32) + 0.5) * UNIT
    zs = (lax.broadcasted_iota(jnp.int32, (16, 128), 0).astype(F32) + 0.5) * UNIT
    place = place * UNIT
    px = jnp.where(lane < count, place[0:1], 1.0e4) - xs
    py = place[1:2] - ys
    pz = place[2:3] - zs
    grid_at = [(i >> 5, (i >> 3) & 3, i & 7) for i in ids]
    parts = []
    for h in range(4):
        shift = [(a - b).astype(F32) for a, b in zip(grid_at[h], grid_at[0])]
        dx = px - shift[0] * (2 * UNIT)
        dy = py - shift[1] * (4 * UNIT)
        dz = pz - shift[2] * (16 * UNIT)
        xy = jnp.exp2(math.log2(AMPLITUDE) - dx * dx - dy * dy)
        zz = jnp.exp2(-(dz * dz))
        for i in range(8):
            parts.append((xy[i : i + 1] * zz).astype(BF))
    return jnp.concatenate(parts, 0)


def to_relative(slots, chunks, sends):
    for j in range(8):
        sends[j][...] = chunks[(slots[DEV] + j) & 7]


def from_relative(slots, gots, chunks):
    for j in range(8):
        chunks[(slots[DEV] - j) & 7] = gots[j][...]


def third_forward(by, grid_at, table, out):
    for j in range(4):
        modes = []
        for half in range(2):
            both = dot(table, grid_at(2 * j + half))
            modes.append(both[:64] + both[64:])
        for kg in range(8):
            piece = jnp.concatenate([m[8 * kg : 8 * kg + 8] for m in modes], 0)
            at = by * 64 + j * 16
            out[kg, at : at + 16, :] = piece.astype(BF)


def block_weights(rank, d, meta, rows):
    ids = [meta[8 * rank + 1 + h, d] for h in range(4)]
    return ids, spread_weights(rows[4 * rank : 4 * rank + 3], meta[8 * rank, d], ids)


def spread_one(rank, d, meta, rows, block, acc):
    ids, weights = block_weights(rank, d, meta, rows)
    tile = dot_nt(block, weights)
    for h in range(4):
        acc[ids[h]] = acc[ids[h]] + tile[:, 128 * h : 128 * h + 128]


def quarter(source, target, sems, i):
    return pltpu.make_async_copy(
        source.at[pl.ds(32 * i, 32)], target.at[pl.ds(32 * i, 32)], sems.at[i]
    )


def encode_body(slots, got_at, eye, z_table, grid_at, aux, meta_out, *rest):
    *sends, modes, grid, acc, got, wide, meta, got_sems, grid_sems, sems = rest
    first = pltpu.make_async_copy(got_at.at[:, pl.ds(128, 8), :], aux, sems.at[0])
    first.start()
    for i in range(4):
        quarter(got_at, got, got_sems, i).start()

    def clear(b, _):
        acc[b] = jnp.zeros((64, 128), F32)
        return 0

    lax.fori_loop(0, 128, clear, 0, unroll=4)
    first.wait()
    wide[...] = aux[...].astype(F32).reshape(8 * DEV, 128)
    for rank in range(2):
        numbers = wide[pl.ds(4 * rank + 3, DEV, stride=8), :].T
        meta_out[8 * rank : 8 * rank + 8, :] = numbers[0:8].astype(jnp.int32)
    to_scalar = pltpu.make_async_copy(meta_out, meta, sems.at[1])
    to_scalar.start()


    to_scalar.wait()

    def part(i, _):
        quarter(got_at, got, got_sems, i).wait()

        def one(k, _):
            d = 32 * i + k
            rows = aux[d].astype(F32)
            for rank in range(2):
                spread_one(rank, d, meta, rows, got[d, 64 * rank : 64 * rank + 64, :], acc)
            return 0

        return lax.fori_loop(0, 32, one, 0, unroll=16)

    lax.fori_loop(0, 4, part, 0)
    eye128 = eye[0:128, 0:128]
    stores = []
    for by in range(4):
        for bz in range(8):
            bricks = jnp.concatenate([acc[(bx * 4 + by) * 8 + bz] for bx in range(4)], 0)
            cells = dot_nt(eye128, bricks.astype(BF)).astype(BF)
            for xy in range(8):
                grid[by, xy, 16 * bz : 16 * bz + 16, :] = cells[16 * xy : 16 * xy + 16]
        stores.append(pltpu.make_async_copy(grid.at[by], grid_at.at[by], grid_sems.at[by]))
        stores[-1].start()
        third_forward(by, lambda xy: grid[by, xy], z_table[...], modes)
    to_relative(slots, modes, sends)
    for store in stores:
        store.wait()


def encode(slots, got, t):
    out = call(
        encode_body,
        [
            pltpu.HBM((4, 8, 128, 256), BF),
            shaped((DEV, 8, 128)),
            shaped((16, DEV), jnp.int32),
        ]
        + [shaped((256, 256))] * 8,
        slots, in_hbm(got), t["eye"], t["z_forward"],
        scratch=(
            pltpu.VMEM((8, 256, 256), BF),
            pltpu.VMEM((4, 8, 128, 256), BF),
            pltpu.VMEM((128, 64, 128), F32),
            pltpu.VMEM((DEV, 136, 128), BF),
            pltpu.VMEM((8 * DEV, 128), F32),
            pltpu.SMEM((16, DEV), jnp.int32),
            pltpu.SemaphoreType.DMA((4,)),
            pltpu.SemaphoreType.DMA((4,)),
            pltpu.SemaphoreType.DMA((2,)),
        ),
        specs=[SM, HB, VM, VM],
        out_specs=[HB] + [VM] * 10,
        limit=24,
    )
    return in_hbm(out[0]), out[1], out[2], out[3:]


def second_body(me, token, *refs):
    *gots, table, order, send, got = refs
    from_relative(me, gots, got)
    rows = []
    for x2 in range(2):
        data = jnp.concatenate(
            [
                got[py, by * 64 + x2 * 32 : by * 64 + x2 * 32 + 32, :]
                for py in range(8)
                for by in range(4)
            ],
            0,
        )
        out = dot(table[...], data)
        for bx in range(4):
            rows.append(
                jnp.concatenate(
                    [out[64 * k : 64 * k + 64, 64 * bx : 64 * bx + 64] for k in range(4)], 1
                ).astype(BF)
            )
    send[...] = dot(order[...], jnp.concatenate(rows, 0)).astype(BF)


def mix_body(got, weights, forward, back, repeat, send, product):
    both = dot(forward[...], got[...])
    modes = (both[:128] + both[128:]).astype(BF)
    spread = dot(repeat[...], modes)
    row = lax.broadcasted_iota(jnp.int32, (512, 256), 0)
    col = lax.broadcasted_iota(jnp.int32, (512, 256), 1)
    spread = jnp.where(col // 64 == (row % 8) // 2, spread, 0.0)
    for m in range(64):
        product[8 * m : 8 * m + 8, :] = dot(spread[8 * m : 8 * m + 8].astype(BF), weights[m])
    real, imag = [], []
    for kz in range(4):
        from_real = product[pl.ds(2 * kz, 64, stride=8), :]
        from_imag = product[pl.ds(2 * kz + 1, 64, stride=8), :]
        real.append(from_real[:, :64] - from_imag[:, 64:])
        imag.append(from_real[:, 64:] + from_imag[:, :64])
    mixed = jnp.concatenate([jnp.concatenate(real, 1), jnp.concatenate(imag, 1)], 0)
    high = mixed.astype(BF)
    low = (mixed - high.astype(F32)).astype(BF)
    send[...] = dot(back[...], jnp.concatenate([high, high, low], 0)).astype(BF)


def second_back_body(me, got, table, order, *rest):
    *sends, send = rest
    ordered = dot(order[...], got[...])
    for x2 in range(2):
        parts = []
        for k in range(4):
            parts.append(
                jnp.concatenate(
                    [
                        ordered[
                            (x2 * 4 + bx) * 64 : (x2 * 4 + bx) * 64 + 64, 64 * k : 64 * k + 64
                        ]
                        for bx in range(4)
                    ],
                    1,
                ).astype(BF)
            )
        out = dot(table[...], jnp.concatenate(parts, 0)).astype(BF)
        for py in range(8):
            for by in range(4):
                at = py * 128 + by * 32
                send[py, by * 64 + x2 * 32 : by * 64 + x2 * 32 + 32, :] = out[at : at + 32]
    to_relative(me, send, sends)


def layer_values(by, j, got, skipped, z_back):
    at = by * 64 + j * 16
    data = jnp.concatenate([got[kg, at : at + 16, :] for kg in range(8)], 0)
    total = dot(z_back, jnp.concatenate([data, data], 0))
    total = total + skipped[by, 2 * j : 2 * j + 2].reshape(256, 256)
    result = 0.5 * total * (1.0 + lax.erf(total * math.sqrt(0.5)))
    return result.astype(BF)


def load_grid(grid_at, grid, sems):
    copies = [
        pltpu.make_async_copy(grid_at.at[by], grid.at[by], sems.at[by]) for by in range(4)
    ]
    for copy in copies:
        copy.start()
    return copies


def four_fold(layer, skip, bias):
    wide = jnp.concatenate([skip[layer].astype(F32)] * 4, 1)
    tall = jnp.concatenate([wide] * 4, 0)
    row = lax.broadcasted_iota(jnp.int32, (256, 256), 0)
    col = lax.broadcasted_iota(jnp.int32, (256, 256), 1)
    matrix = jnp.where(row // 64 == col // 64, tall, 0.0).astype(BF)
    return matrix, jnp.concatenate([bias[layer : layer + 1, :]] * 4, 1)


def skip_body(layer, anchor, grid_at, skip, bias, out, grid, sems):
    copies = load_grid(grid_at, grid, sems)
    skip, bias = four_fold(layer, skip, bias)
    for by in range(4):
        copies[by].wait()
        product = dot(grid[by].reshape(1024, 256), skip) + bias
        out[by] = product.reshape(8, 128, 256)


def inner_layer_body(me, *refs):
    *gots, skipped, z_back, z_table, new_grid_at = refs[:12]
    *sends, got, new_grid, modes, out_sems = refs[12:]
    from_relative(me, gots, got)
    stores = []
    for by in range(4):
        for j in range(4):
            values = layer_values(by, j, got, skipped, z_back[...])
            new_grid[by, 2 * j] = values[:128]
            new_grid[by, 2 * j + 1] = values[128:]
        stores.append(
            pltpu.make_async_copy(new_grid.at[by], new_grid_at.at[by], out_sems.at[by])
        )
        stores[-1].start()
        third_forward(by, lambda xy: new_grid[by, xy], z_table[...], modes)
    to_relative(me, modes, sends)
    for store in stores:
        store.wait()


def last_layer_body(me, *refs):
    *gots, skipped, z_back, eye, bricks, got = refs
    from_relative(me, gots, got)
    for by in range(4):
        values = [
            layer_values(by, j, got, skipped, z_back[...]) for j in range(4)
        ]
        for bz in range(8):
            cells = jnp.concatenate(
                [
                    values[xy // 2][(xy % 2) * 128 + 16 * bz : (xy % 2) * 128 + 16 * bz + 16]
                    for xy in range(8)
                ],
                0,
            )
            turned = dot_nt(eye[...], cells).astype(BF)
            for bx in range(4):
                bricks[(bx * 4 + by) * 8 + bz] = turned[64 * bx : 64 * bx + 64]


def early_body(layer, meta, aux, anchor, weights_at, out, kept, token, sem):
    start = EARLY * layer
    fetch = pltpu.make_async_copy(weights_at.at[pl.ds(64 * layer, 64)], kept, sem)

    @pl.when(pl.program_id(0) == 0)
    def _():
        fetch.start()

    def one(k, _):
        d = start + 8 * pl.program_id(0) + k
        rows = aux[d].astype(F32)
        for rank in range(2):
            out[2 * k + rank] = block_weights(rank, d, meta, rows)[1]
        return 0

    lax.fori_loop(0, 8, one, 0, unroll=8)

    token[...] = jnp.zeros((8, 128), F32)

    @pl.when(pl.program_id(0) == EARLY // 8 - 1)
    def _():
        fetch.wait()


def early_weights(layer, meta, aux, anchor, weights):
    kernels, kept, token = pl.pallas_call(
        functools.partial(early_body, layer),
        grid=(EARLY // 8,),
        out_shape=[
            pltpu.HBM((2 * EARLY, 512, 128), BF), shaped((64, 256, 128)), shaped((8, 128), F32)
        ],
        in_specs=[SM, VM, VM, HB],
        out_specs=[pl.BlockSpec((16, 512, 128), lambda i: (i, 0, 0)), VM, VM],
        scratch_shapes=[pltpu.SemaphoreType.DMA],
        compiler_params=pltpu.CompilerParams(vmem_limit_bytes=16 * MIB),
        cost_estimate=pl.CostEstimate(
            flops=EARLY * 10**7, bytes_accessed=EARLY * 2**18, transcendentals=0
        ),
    )(meta, aux, anchor, weights)
    return in_hbm(kernels), kept, token


def decode_body(meta, aux, bricks, *refs):
    *stored_at, reply, stored, sems = refs
    loads = []
    for w in range(2):
        for i in range(EARLY // 8):
            loads.append(
                pltpu.make_async_copy(
                    stored_at[w].at[pl.ds(16 * i, 16)],
                    stored.at[pl.ds(2 * EARLY * w + 16 * i, 16)],
                    sems.at[len(loads)],
                )
            )
            loads[-1].start()

    def write(d, near, weights):
        both = DECODE_SCALE * dot(jnp.concatenate(near, 0), jnp.concatenate(weights, 1))
        reply[d, 0:64, :] = both[:64, :128].astype(BF)
        reply[d, 64:128, :] = both[64:, 128:].astype(BF)

    def fresh(k, _):
        d = 2 * EARLY + k
        rows = aux[d].astype(F32)
        near, weights = [], []
        for rank in range(2):
            ids, kernel = block_weights(rank, d, meta, rows)
            weights.append(kernel)
            near.append(jnp.concatenate([bricks[i] for i in ids], 1))
        write(d, near, weights)
        return 0

    lax.fori_loop(0, DEV - 2 * EARLY, fresh, 0, unroll=16)
    for load in loads:
        load.wait()

    def early(d, _):
        near = []
        for rank in range(2):
            ids = [meta[8 * rank + 1 + h, d] for h in range(4)]
            near.append(jnp.concatenate([bricks[i] for i in ids], 1))
        write(d, near, [stored[2 * d], stored[2 * d + 1]])
        return 0

    lax.fori_loop(0, 2 * EARLY, early, 0, unroll=16)


def pick_body(slots, got, out_at, out, sems):
    def part(i, _):
        def one(k, _):
            b = 32 * i + k
            out[b] = got[slots[b]]
            return 0

        lax.fori_loop(0, 32, one, 0, unroll=8)
        quarter(out, out_at, sems, i).start()
        return 0

    lax.fori_loop(0, 4, part, 0)
    for i in range(4):
        quarter(out, out_at, sems, i).wait()


def exchange(x, axis):
    return lax.all_to_all(x, axis, split_axis=0, concat_axis=0, tiled=True)


def exchange_lines(chunks):
    got = [chunks[0]]
    for j in range(1, 8):
        got.append(lax.ppermute(chunks[j], "py", [(i, (i + j) % 8) for i in range(8)]))
    return got


def per_device(values, offsets, counts, bricks, spectral_weights, skip_weights, skip_bias):
    t = {name: jnp.asarray(table) for name, table in tables().items()}
    me = lax.axis_index("py").astype(jnp.int32).reshape(1)
    weights = in_hbm(spectral_weights.reshape(LAYERS * 64, 256, 128))
    send, slots = pack(me, values, offsets, counts, bricks)
    got = exchange(send, ("px", "py"))
    grid, aux, meta, modes = encode(slots, got, t)
    chunks = pltpu.VMEM((8, 256, 256), BF)
    grid_scratch = pltpu.VMEM((4, 8, 128, 256), BF)
    four = pltpu.SemaphoreType.DMA((4,))
    piece = shaped((256, 256))
    stored = []
    for layer in range(LAYERS):
        kernel, kept, token = early_weights(layer, meta, aux, modes[0], weights)
        stored.append(kernel)
        columns = exchange_lines(modes)
        second = call(
            second_body,
            shaped((512, 256)),
            slots, token, *columns, t["y_forward"], t["to_send"],
            scratch=(chunks,),
            specs=[SM] + [VM] * 11,
            limit=24,
        )
        lines = exchange(second.reshape(16, 32, 256), "px").reshape(512, 256)
        back = call(
            mix_body,
            shaped((512, 256)),
            lines, kept, t["x_forward"], t["x_back"], t["repeat"],
            scratch=(pltpu.VMEM((512, 128), F32),),
            limit=24,
        )
        lines = exchange(back.reshape(16, 32, 256), "px").reshape(512, 256)
        columns = call(
            second_back_body,
            [piece] * 8,
            slots, lines, t["y_back"], t["from_send"],
            scratch=(chunks,),
            specs=[SM, VM, VM, VM],
            limit=24,
        )
        skipped = call(
            functools.partial(skip_body, layer),
            shaped((4, 8, 128, 256), F32),
            columns[0], grid, skip_weights, skip_bias,
            scratch=(grid_scratch, four),
            specs=[VM, HB, VM, VM],
            limit=24,
            flops=2 * 4096 * 256 * 256,
        )
        columns = exchange_lines(columns)
        if layer + 1 < LAYERS:
            grid, *modes = call(
                inner_layer_body,
                [pltpu.HBM((4, 8, 128, 256), BF)] + [piece] * 8,
                slots, *columns, skipped, t["z_back"], t["z_forward"],
                scratch=(
                    chunks, grid_scratch, chunks, four,
                ),
                specs=[SM] + [VM] * 11,
                out_specs=[HB] + [VM] * 8,
                limit=32,
            )
            grid = in_hbm(grid)
        else:
            final = call(
                last_layer_body,
                shaped((128, 64, 128)),
                slots, *columns, skipped, t["z_back"], t["eye"],
                scratch=(chunks,),
                specs=[SM] + [VM] * 11,
                limit=32,
            )
    reply = call(
        decode_body,
        shaped((DEV, 128, 128)),
        meta, aux, final, *stored,
        scratch=(
            pltpu.VMEM((4 * EARLY, 512, 128), BF),
            pltpu.SemaphoreType.DMA((EARLY // 4,)),
        ),
        specs=[SM, VM, VM, HB, HB],
        limit=40,
    )
    returned = exchange(reply, ("px", "py"))
    return call(
        pick_body,
        shaped((DEV, 64, 128)),
        slots, returned.reshape(2 * DEV, 64, 128),
        scratch=(pltpu.VMEM((DEV, 64, 128), BF), pltpu.SemaphoreType.DMA((4,))),
        specs=[SM, VM],
        out_specs=HB,
        limit=24,
    )


def solution(mesh):
    return jax.shard_map(
        per_device,
        mesh=mesh,
        in_specs=(
            P(("px", "py"), None, None),
            P(("px", "py"), None, None),
            P(("px", "py")),
            P(("px", "py"), None),
            P(None, None, "px", "py", None, None),
            P(),
            P(),
        ),
        out_specs=P(("px", "py"), None, None),
        check_vma=False,
    )
```
